32 devices in a mesh: rep: 1 (over z), row: 4 (over y), col: 4 (over x), core: 2 (over core).
Axes of the slice: x: 4, y: 4, z: 1, core: 2. Of those that a mesh axis runs over, the one named last changes fastest.
The devices are a block of a 4x4x8 slice.
Arguments:
- x: bfloat16 [2, 512, 1280], P(None, ('rep', 'row', 'col', 'core'))
- route_idx: int32 [2, 512, 6], P(None, ('rep', 'row', 'col', 'core'))
- gates: float32 [2, 512, 6], P(None, ('rep', 'row', 'col', 'core'))
- w_gate: bfloat16 [160, 1280, 384], P(('rep', 'row', 'col', 'core'))
- w_up: bfloat16 [160, 1280, 384], P(('rep', 'row', 'col', 'core'))
- w_down: bfloat16 [160, 384, 1280], P(('rep', 'row', 'col', 'core'))
- grad_y: bfloat16 [2, 512, 1280], P(None, ('rep', 'row', 'col', 'core'))
Outputs:
- output 1: bfloat16 [2, 512, 1280], P(None, ('rep', 'row', 'col', 'core'))
- output 2: bfloat16 [2, 512, 1280], P(None, ('rep', 'row', 'col', 'core'))
- output 3: float32 [2, 512, 6], P(None, ('rep', 'row', 'col', 'core'))
- output 4: float32 [160, 1280, 384], P(('rep', 'row', 'col', 'core'))
- output 5: float32 [160, 1280, 384], P(('rep', 'row', 'col', 'core'))
- output 6: float32 [160, 384, 1280], P(('rep', 'row', 'col', 'core'))
All inputs are finite; a program needn't handle non-finite values.
Results may differ from the reference program's by a relative error of at most 0.00984795.
Values are sent between devices in bfloat16 or wider.
A program may use at most 768 MiB of HBM per device.

```python
import jax
import jax.numpy as jnp
from jax import lax

D_MODEL = 1280
D_FF = 384
EXPERTS = 160
TOP_K = 6
TOK_DEV = 16
N_ROWS = 4
N_COLS = 4
N_CORES = 2

GROUP_SIZE = N_ROWS * N_COLS * N_CORES
TOKENS = GROUP_SIZE * TOK_DEV
CAPACITY = TOK_DEV // 2
CHIP_EXP = EXPERTS // (N_ROWS * N_COLS)
N_HOT = min(CHIP_EXP, TOP_K // 2)
N_COLD = EXPERTS - N_HOT
LOAD_MAX = GROUP_SIZE * CAPACITY


def draw_hot_chips(base_key):
    key_list = jax.random.split(base_key, 4)
    row_first = jax.random.randint(key_list[0], (), 0, N_ROWS)
    col_first = jax.random.randint(key_list[1], (), 0, N_COLS)
    row_second = (row_first + jax.random.randint(key_list[2], (), 1, N_ROWS)) % N_ROWS
    col_second = (col_first + jax.random.randint(key_list[3], (), 1, N_COLS)) % N_COLS
    return row_first * N_COLS + col_first, row_second * N_COLS + col_second


def draw_routing(base_key, hot_chip):
    key_list = jax.random.split(base_key, 4)
    slot_ids = jnp.arange(TOP_K)
    hot_ids = hot_chip * CHIP_EXP + jnp.arange(N_HOT) * (CHIP_EXP // N_HOT)
    sel_keys = jax.random.split(key_list[0], GROUP_SIZE * N_HOT)
    perm_rank = jax.vmap(lambda sub_key: jax.random.permutation(sub_key, TOK_DEV))(sel_keys)
    hot_mask = (perm_rank < CAPACITY).astype(jnp.int32).reshape(GROUP_SIZE, N_HOT, TOK_DEV)
    hot_mask = jnp.transpose(hot_mask, (0, 2, 1))
    hot_count = jnp.sum(hot_mask, axis=2)
    hot_rank = jnp.cumsum(hot_mask, axis=2) - hot_mask
    hot_pick = hot_mask[:, :, :, None] * (hot_rank[:, :, :, None] == slot_ids).astype(jnp.int32)
    hot_route = jnp.sum(hot_pick * hot_ids[None, None, :, None], axis=2)
    is_hot = jnp.zeros((EXPERTS,), jnp.int32).at[hot_ids].set(1)
    cold_sorted = jnp.argsort(is_hot * EXPERTS + jnp.arange(EXPERTS))[:N_COLD]
    cold_keys = jax.random.split(key_list[1], GROUP_SIZE)
    cold_perm = jax.vmap(lambda sub_key: jax.random.permutation(sub_key, cold_sorted))(cold_keys)
    win_start = jax.random.randint(key_list[2], (GROUP_SIZE, 1, 1), 0, N_COLD)
    cold_offset = slot_ids[None, None, :] - hot_count[:, :, None]
    cold_pos = (win_start + jnp.arange(TOK_DEV)[None, :, None] * TOP_K + cold_offset) % N_COLD
    cold_route = jnp.take_along_axis(cold_perm, cold_pos.reshape(GROUP_SIZE, TOK_DEV * TOP_K), axis=1)
    route_ids = jnp.where(cold_offset < 0, hot_route, cold_route.reshape(GROUP_SIZE, TOK_DEV, TOP_K))
    slot_rot = jax.random.randint(key_list[3], (GROUP_SIZE, TOK_DEV, 1), 0, TOP_K)
    route_ids = jnp.take_along_axis(route_ids, (slot_ids - slot_rot) % TOP_K, axis=2)
    return route_ids.reshape(TOKENS, TOP_K).astype(jnp.int32)


def setup_inputs(seed: int = 0, part: int = 0) -> dict:
    base_key = jax.random.fold_in(jax.random.key(seed), part)
    key_list = jax.random.split(base_key, 9)
    hot_first, hot_second = draw_hot_chips(key_list[0])
    route_idx = jnp.stack([draw_routing(key_list[1], hot_first), draw_routing(key_list[2], hot_second)])
    x = jax.random.normal(key_list[3], (2, TOKENS, D_MODEL), jnp.float32).astype(jnp.bfloat16)
    raw_gates = jax.random.uniform(key_list[4], (2, TOKENS, TOP_K), jnp.float32, 1.0, 2.0)
    gates = raw_gates / jnp.sum(raw_gates, axis=2, keepdims=True)
    w_gate = (jax.random.normal(key_list[5], (EXPERTS, D_MODEL, D_FF), jnp.float32) * D_MODEL ** -0.5).astype(jnp.bfloat16)
    w_up = (jax.random.normal(key_list[6], (EXPERTS, D_MODEL, D_FF), jnp.float32) * D_MODEL ** -0.5).astype(jnp.bfloat16)
    w_down = (jax.random.normal(key_list[7], (EXPERTS, D_FF, D_MODEL), jnp.float32) * D_FF ** -0.5).astype(jnp.bfloat16)
    grad_y = jax.random.normal(key_list[8], (2, TOKENS, D_MODEL), jnp.float32).astype(jnp.bfloat16)
    return {"x": x, "route_idx": route_idx, "gates": gates, "w_gate": w_gate, "w_up": w_up, "w_down": w_down, "grad_y": grad_y}


def swiglu_rows(x_rows, d_out, w_gate_e, w_up_e, w_down_e):
    gate_pre = jnp.dot(x_rows, w_gate_e, preferred_element_type=jnp.float32).astype(jnp.bfloat16)
    up_pre = jnp.dot(x_rows, w_up_e, preferred_element_type=jnp.float32).astype(jnp.bfloat16)
    gate_f = gate_pre.astype(jnp.float32)
    up_f = up_pre.astype(jnp.float32)
    sigmoid_g = jax.nn.sigmoid(gate_f)
    hidden = (gate_f * sigmoid_g * up_f).astype(jnp.bfloat16)
    exp_out = jnp.dot(hidden, w_down_e, preferred_element_type=jnp.float32).astype(jnp.bfloat16)
    d_act = jnp.dot(d_out, w_down_e.T, preferred_element_type=jnp.float32)
    d_up = (d_act * gate_f * sigmoid_g).astype(jnp.bfloat16)
    d_gate = (d_act * up_f * sigmoid_g * (1.0 + gate_f * (1.0 - sigmoid_g))).astype(jnp.bfloat16)
    d_in = (jnp.dot(d_gate, w_gate_e.T, preferred_element_type=jnp.float32) + jnp.dot(d_up, w_up_e.T, preferred_element_type=jnp.float32)).astype(jnp.bfloat16)
    g_gate = jnp.dot(x_rows.T, d_gate, preferred_element_type=jnp.float32)
    g_up = jnp.dot(x_rows.T, d_up, preferred_element_type=jnp.float32)
    g_down = jnp.dot(hidden.T, d_out, preferred_element_type=jnp.float32)
    return exp_out, d_in, g_gate, g_up, g_down


def microbatch(x, route_ids, gates, grad_y, w_gate, w_up, w_down):
    token_ids = jnp.arange(TOKENS)
    member = jnp.zeros((TOKENS, EXPERTS), jnp.int32).at[token_ids[:, None], route_ids].set(1)
    slot_rank = jnp.cumsum(member, axis=0) - member
    slot_pos = jnp.take_along_axis(slot_rank, route_ids, axis=1)
    slot_owner = jnp.full((EXPERTS * LOAD_MAX,), TOKENS * TOP_K, jnp.int32)
    slot_owner = slot_owner.at[(route_ids * LOAD_MAX + slot_pos).reshape(-1)].set(jnp.arange(TOKENS * TOP_K))
    slot_owner = slot_owner.reshape(EXPERTS, LOAD_MAX)
    x_pad = jnp.concatenate([x, jnp.zeros((1, D_MODEL), x.dtype)])
    dy_pad = jnp.concatenate([grad_y, jnp.zeros((1, D_MODEL), grad_y.dtype)])
    gate_pad = jnp.concatenate([gates.reshape(-1), jnp.zeros((1,), jnp.float32)])

    def one_expert(accums, per_expert):
        y_acc, dx_acc, dg_acc = accums
        slot_ids, w_gate_e, w_up_e, w_down_e = per_expert
        tok_rows = slot_ids // TOP_K
        row_gate = gate_pad[slot_ids]
        x_rows = x_pad[tok_rows]
        dy_rows = dy_pad[tok_rows].astype(jnp.float32)
        d_out = (row_gate[:, None] * dy_rows).astype(jnp.bfloat16)
        exp_out, d_in, g_gate, g_up, g_down = swiglu_rows(x_rows, d_out, w_gate_e, w_up_e, w_down_e)
        out_f = exp_out.astype(jnp.float32)
        y_acc = y_acc.at[tok_rows].add(row_gate[:, None] * out_f)
        dx_acc = dx_acc.at[tok_rows].add(d_in.astype(jnp.float32))
        dg_acc = dg_acc.at[slot_ids].add(jnp.sum(dy_rows * out_f, axis=1))
        return (y_acc, dx_acc, dg_acc), (g_gate, g_up, g_down)

    init_acc = (jnp.zeros((TOKENS + 1, D_MODEL), jnp.float32), jnp.zeros((TOKENS + 1, D_MODEL), jnp.float32), jnp.zeros((TOKENS * TOP_K + 1,), jnp.float32))
    final_acc, grads = lax.scan(one_expert, init_acc, (slot_owner, w_gate, w_up, w_down))
    y_acc, dx_acc, dg_acc = final_acc
    y_out = y_acc[:TOKENS].astype(jnp.bfloat16)
    dx_out = dx_acc[:TOKENS].astype(jnp.bfloat16)
    dg_out = dg_acc[:TOKENS * TOP_K].reshape(TOKENS, TOP_K)
    return y_out, dx_out, dg_out, grads[0], grads[1], grads[2]


def reference(x, route_idx, gates, w_gate, w_up, w_down, grad_y):
    mb_first = microbatch(x[0], route_idx[0], gates[0], grad_y[0], w_gate, w_up, w_down)
    mb_second = microbatch(x[1], route_idx[1], gates[1], grad_y[1], w_gate, w_up, w_down)
    return (jnp.stack([mb_first[0], mb_second[0]]), jnp.stack([mb_first[1], mb_second[1]]), jnp.stack([mb_first[2], mb_second[2]]), mb_first[3] + mb_second[3], mb_first[4] + mb_second[4], mb_first[5] + mb_second[5])
```

```python
import functools

import jax
import jax.numpy as jnp
from jax import lax
from jax.experimental import pallas as pl
from jax.experimental.pallas import tpu as pltpu
from jax.sharding import PartitionSpec as P

GROUP_AXES = ("row", "col", "core")
ALL_AXES = ("rep", "row", "col", "core")
F32 = jnp.float32
BF16 = jnp.bfloat16
LANES = 128
SMALL = 32


def dot_nn(a, b):
    return lax.dot_general(a, b, (((1,), (0,)), ((), ())), preferred_element_type=F32)


def dot_nt(a, b):
    return lax.dot_general(a, b, (((1,), (1,)), ((), ())), preferred_element_type=F32)


def dot_tn(a, b):
    return lax.dot_general(a, b, (((0,), (0,)), ((), ())), preferred_element_type=F32)


def split3(v):
    h1 = v.astype(BF16)
    r1 = v - h1.astype(F32)
    h2 = r1.astype(BF16)
    h3 = (r1 - h2.astype(F32)).astype(BF16)
    return h1, h2, h3


def col_blocks(width, step):
    return [(s, min(step, width - s)) for s in range(0, width, step)]


def expert_kernel(dims, xd_hbm, wg_hbm, wu_hbm, wd_hbm, part_hbm, gg_hbm, gu_hbm, gd_hbm,
                  xd_v, pt_v, gr_v, acc_v, wg_v, wu_v, wd_v, og_v, ou_v, od_v, pos_v,
                  xt_v, qt_v, a_v, duv_v, cnt_s, base_s, sem_x, sem_w, sem_o, sem_p):
    tokens, dm, ff, el, top_k, seg = dims
    n_row, n_col, n_core = lax.axis_size("row"), lax.axis_size("col"), lax.axis_size("core")
    me = (lax.axis_index("row") * n_col + lax.axis_index("col")) * n_core + lax.axis_index("core")
    width = 2 * dm + LANES

    def load_w(e, slot):
        return [pltpu.make_async_copy(h.at[e], v.at[slot], sem_w.at[slot, i])
                for i, (h, v) in enumerate(((wg_hbm, wg_v), (wu_hbm, wu_v), (wd_hbm, wd_v)))]

    def store_g(e, slot):
        return [pltpu.make_async_copy(v.at[slot], h.at[e], sem_o.at[slot, i])
                for i, (h, v) in enumerate(((gg_hbm, og_v), (gu_hbm, ou_v), (gd_hbm, od_v)))]

    loads_x = [pltpu.make_async_copy(xd_hbm.at[m], xd_v.at[m], sem_x.at[m]) for m in range(2)]
    for c in loads_x:
        c.start()
    for s in range(2):
        for c in load_w(s, s):
            c.start()

    row_i = lax.broadcasted_iota(jnp.int32, (tokens, tokens), 0)
    col_i = lax.broadcasted_iota(jnp.int32, (tokens, tokens), 1)
    tri = (row_i < col_i).astype(F32).astype(BF16)
    sub = lax.broadcasted_iota(jnp.int32, (8, tokens), 0)
    eids = jnp.where(sub < el, (me * el + sub), -1).astype(F32)

    def chunks(total):
        return jnp.maximum((total + (seg - 1)) // seg, 1)

    n_chunks = []
    for m in range(2):
        loads_x[m].wait()
        meta_t = xd_v[m, :, 2 * dm:].astype(F32).T
        hits = jnp.zeros((8, tokens), F32)
        for j in range(top_k):
            hits = hits + (meta_t[j:j + 1, :] == eids).astype(F32)
        rank = dot_nn(hits.astype(BF16), tri)
        total = jnp.int32(0)
        for e in range(el):
            cnt = jnp.sum(hits[e:e + 1, :]).astype(jnp.int32)
            cnt_s[m, e] = cnt
            base_s[m, e] = total
            pos_v[m, e:e + 1, :] = jnp.where(hits[e:e + 1, :] > 0, rank[e:e + 1, :] + total.astype(F32), -1.0)
            total = total + (cnt + 15) // 16 * 16
        n_ch = chunks(total)
        n_chunks.append(n_ch)

        def gather(c, carry, m=m):
            off = pl.multiple_of(c * seg, seg)
            rows = (lax.broadcasted_iota(jnp.int32, (seg, tokens), 0) + off).astype(F32)
            pick = rows == pos_v[m, 0:1, :]
            for e in range(1, el):
                pick = pick | (rows == pos_v[m, e:e + 1, :])
            pick_f = pick.astype(F32)
            pt_v[m, :, pl.ds(off, seg)] = pick_f.T.astype(BF16)
            pick_b = pick_f.astype(BF16)
            for s, w in col_blocks(width, 512):
                gr_v[m, pl.ds(off, seg), s:s + w] = dot_nn(pick_b, xd_v[m, :, s:s + w]).astype(BF16)
            return carry

        lax.fori_loop(0, n_ch, gather, 0)

    def tile(e, slot, ra, rb, m_a, n_a, n_b, first):
        rows = ra + rb
        base_a = pl.multiple_of(base_s[m_a, e], 16)
        base_b = pl.multiple_of(base_s[1 - m_a, e], 16)
        it = lax.broadcasted_iota(jnp.int32, (rows, 1), 0)
        valid = ((it < ra) & (it < n_a)) | ((it >= ra) & (it - ra < n_b))

        def read(s, w):
            return jnp.concatenate([gr_v[m_a, pl.ds(base_a, ra), s:s + w],
                                    gr_v[1 - m_a, pl.ds(base_b, rb), s:s + w]], axis=0)

        def write(s, w, val):
            merged = jnp.where(valid, val.astype(F32), read(s, w).astype(F32)).astype(BF16)
            gr_v[m_a, pl.ds(base_a, ra), s:s + w] = merged[:ra]

            @pl.when(n_b > 0)
            def _():
                gr_v[1 - m_a, pl.ds(base_b, rb), s:s + w] = merged[ra:]

        lane = lax.broadcasted_iota(jnp.int32, (rows, LANES), 1)
        meta = jnp.where(valid, read(2 * dm, LANES).astype(F32), 0.0)
        eid = (me * el + e).astype(F32)
        mine = ((meta == eid) & (lane < top_k)).astype(F32)
        sel = pltpu.roll(mine, 8, 1) + pltpu.roll(mine, 16, 1) + pltpu.roll(mine, 24, 1)
        gate = jnp.where(valid, jnp.sum(meta * sel, axis=1, keepdims=True), 0.0)
        for s, w in col_blocks(dm, 256):
            xt_v[:rows, s:s + w] = jnp.where(valid, read(s, w).astype(F32), 0.0).astype(BF16)
            dy = jnp.where(valid, read(dm + s, w).astype(F32), 0.0)
            qt_v[:rows, s:s + w] = (gate * dy).astype(BF16)
        xt = xt_v[:rows, :]
        u = dot_nn(xt, wg_v[slot]).astype(BF16).astype(F32)
        v = dot_nn(xt, wu_v[slot]).astype(BF16).astype(F32)
        r = dot_nt(qt_v[:rows, :], wd_v[slot])
        s_g = jax.nn.sigmoid(u)
        a_v[:rows, :] = (u * s_g * v).astype(BF16)
        duv_v[:rows, :ff] = (r * v * s_g * (1.0 + u * (1.0 - s_g))).astype(BF16)
        duv_v[:rows, ff:] = (r * u * s_g).astype(BF16)
        a = a_v[:rows, :]
        du = duv_v[:rows, :ff]
        dv = duv_v[:rows, ff:]
        dots = jnp.zeros((rows, 1), F32)
        for s, w in col_blocks(dm, 256):
            o = dot_nn(a, wd_v[slot, :, s:s + w]).astype(BF16)
            dy = jnp.where(valid, read(dm + s, w).astype(F32), 0.0)
            dots = dots + jnp.sum(dy * o.astype(F32), axis=1, keepdims=True)
            write(s, w, o)
        for s, w in col_blocks(dm, 256):
            p = dot_nt(du, wg_v[slot, s:s + w, :]) + dot_nt(dv, wu_v[slot, s:s + w, :])
            write(dm + s, w, p.astype(BF16))
        d1, d2, d3 = split3(dots)
        g1, g2, g3 = split3(gate)
        new_meta = jnp.zeros((rows, LANES), F32)
        for at, val in ((e, d1), (8 + e, d2), (16 + e, d3), (32, g1), (33, g2), (34, g3)):
            new_meta = jnp.where(lane == at, val.astype(F32), new_meta)
        write(2 * dm, LANES, new_meta)

        def put(ref, idx, val):
            if first is None:
                ref[idx] = val
            else:
                ref[idx] = jnp.where(first, 0.0, ref[idx]) + val

        duv = duv_v[:rows, :]
        for s, w in col_blocks(dm, 256):
            g_in = dot_tn(xt_v[:rows, s:s + w], duv)
            put(og_v, (slot, slice(s, s + w)), g_in[:, :ff])
            put(ou_v, (slot, slice(s, s + w)), g_in[:, ff:])
        for s, w in col_blocks(dm, 256):
            put(od_v, (slot, slice(None), slice(s, s + w)), dot_tn(a, qt_v[:rows, s:s + w]))

    def expert(e, carry):
        slot = lax.rem(e, 2)
        for c in load_w(e, slot):
            c.wait()

        @pl.when(e >= 2)
        def _():
            for c in store_g(e - 2, slot):
                c.wait()

        n0, n1 = cnt_s[0, e], cnt_s[1, e]
        big0, big1 = n0 > SMALL, n1 > SMALL

        @pl.when(jnp.logical_not(big0 | big1))
        def _():
            tile(e, slot, SMALL, SMALL, 0, n0, n1, None)

        @pl.when(big0 | big1)
        def _():
            both = big0 & big1

            def one(i, inner):
                m_a = jnp.where(both, i, jnp.where(big0, 0, 1))
                n_a = jnp.where(m_a == 0, n0, n1)
                n_b = jnp.where(both, 0, jnp.where(m_a == 0, n1, n0))
                tile(e, slot, seg, SMALL, m_a, n_a, n_b, i == 0)
                return inner

            lax.fori_loop(0, jnp.where(both, 2, 1), one, 0)

        for c in store_g(e, slot):
            c.start()

        @pl.when(e + 2 < el)
        def _():
            for c in load_w(e + 2, slot):
                c.start()

        return carry

    lax.fori_loop(0, el, expert, 0)

    for m in range(2):
        def scatter(c, carry, m=m):
            off = pl.multiple_of(c * seg, seg)
            rows = pl.ds(off, seg)
            first = c == 0
            pt = pt_v[m, :, rows]
            gp = gr_v[m, rows, 2 * dm:].astype(F32)
            gate = gp[:, 32:33] + gp[:, 33:34] + gp[:, 34:35]
            for s, w in col_blocks(dm, 256):
                h1, h2, h3 = split3(gate * gr_v[m, rows, s:s + w].astype(F32))
                add = dot_nn(pt, h1) + dot_nn(pt, h2) + dot_nn(pt, h3)
                acc_v[m, :, s:s + w] = jnp.where(first, 0.0, acc_v[m, :, s:s + w]) + add
            for s, w in col_blocks(dm + LANES, 256):
                lo = dm + s
                add = dot_nn(pt, gr_v[m, rows, lo:lo + w])
                acc_v[m, :, lo:lo + w] = jnp.where(first, 0.0, acc_v[m, :, lo:lo + w]) + add
            return carry

        lax.fori_loop(0, n_chunks[m], scatter, 0)
        lane = lax.broadcasted_iota(jnp.int32, (tokens, LANES), 1)
        ids = jnp.where(lane < top_k, xd_v[m, :, 2 * dm:].astype(F32), -1.0)
        raw = acc_v[m, :, 2 * dm:]
        out = jnp.zeros((tokens, LANES), F32)
        for e in range(el):
            val = raw[:, e:e + 1] + raw[:, 8 + e:9 + e] + raw[:, 16 + e:17 + e]
            out = jnp.where(ids == (me * el + e).astype(F32), val, out)
        acc_v[m, :, 2 * dm:] = out
        pltpu.make_async_copy(acc_v.at[m], part_hbm.at[m], sem_p.at[m]).start()

    for e in range(el - 2, el):
        for c in store_g(e, e % 2):
            c.wait()
    for m in range(2):
        pltpu.make_async_copy(acc_v.at[m], part_hbm.at[m], sem_p.at[m]).wait()


def expert_stage(xd, w_gate, w_up, w_down, top_k, seg):
    _, tokens, width = xd.shape
    el, dm, ff = w_gate.shape
    any_spec = pl.BlockSpec(memory_space=pl.ANY)
    rows_max = el * seg
    tile_rows = seg + SMALL
    dims = (tokens, dm, ff, el, top_k, seg)
    return pl.pallas_call(
        functools.partial(expert_kernel, dims),
        out_shape=(
            jax.ShapeDtypeStruct((2, tokens, width), F32),
            jax.ShapeDtypeStruct((el, dm, ff), F32),
            jax.ShapeDtypeStruct((el, dm, ff), F32),
            jax.ShapeDtypeStruct((el, ff, dm), F32),
        ),
        in_specs=[any_spec] * 4,
        out_specs=[any_spec] * 4,
        scratch_shapes=[
            pltpu.VMEM((2, tokens, width), BF16),
            pltpu.VMEM((2, tokens, rows_max), BF16),
            pltpu.VMEM((2, rows_max, width), BF16),
            pltpu.VMEM((2, tokens, width), F32),
            pltpu.VMEM((2, dm, ff), BF16),
            pltpu.VMEM((2, dm, ff), BF16),
            pltpu.VMEM((2, ff, dm), BF16),
            pltpu.VMEM((2, dm, ff), F32),
            pltpu.VMEM((2, dm, ff), F32),
            pltpu.VMEM((2, ff, dm), F32),
            pltpu.VMEM((2, 8, tokens), F32),
            pltpu.VMEM((tile_rows, dm), BF16),
            pltpu.VMEM((tile_rows, dm), BF16),
            pltpu.VMEM((tile_rows, ff), BF16),
            pltpu.VMEM((tile_rows, 2 * ff), BF16),
            pltpu.SMEM((2, 8), jnp.int32),
            pltpu.SMEM((2, 8), jnp.int32),
            pltpu.SemaphoreType.DMA((2,)),
            pltpu.SemaphoreType.DMA((2, 3)),
            pltpu.SemaphoreType.DMA((2, 3)),
            pltpu.SemaphoreType.DMA((2,)),
        ],
        compiler_params=pltpu.CompilerParams(vmem_limit_bytes=66_000_000),
        name="experts",
    )(xd, w_gate, w_up, w_down)


def pack_tokens(x, route_idx, gates, grad_y):
    def piece(v):
        return lax.reduce_precision(v, 8, 7)

    g1 = piece(gates)
    g2 = piece(gates - g1)
    g3 = piece(gates - g1 - g2)

    def pad(v):
        return jnp.pad(v.astype(BF16), ((0, 0), (0, 0), (0, 8 - v.shape[2])))

    ids = route_idx.astype(F32)
    meta = jnp.concatenate([pad(ids), pad(g1), pad(g2), pad(g3)], axis=2)
    meta = jnp.pad(meta, ((0, 0), (0, 0), (0, LANES - meta.shape[2])))
    return jnp.concatenate([x, grad_y, meta], axis=2)


def solution(mesh):
    group = mesh.shape["row"] * mesh.shape["col"] * mesh.shape["core"]
    tok_spec = P(None, ALL_AXES, None)
    w_spec = P(ALL_AXES, None, None)

    def moe_layer(x, route_idx, gates, w_gate, w_up, w_down, grad_y):
        _, tok_dev, dm = x.shape
        top_k = route_idx.shape[2]
        packed = pack_tokens(x, route_idx, gates, grad_y)
        xd = lax.all_gather(packed, GROUP_AXES, axis=1, tiled=True)
        part, g_gate, g_up, g_down = expert_stage(xd, w_gate, w_up, w_down, top_k, group * (tok_dev // 2))
        mine = lax.psum_scatter(part, GROUP_AXES, scatter_dimension=1, tiled=True)
        y = mine[:, :, :dm].astype(BF16)
        dx = mine[:, :, dm:2 * dm].astype(BF16)
        dg = mine[:, :, 2 * dm:2 * dm + top_k]
        return y, dx, dg, g_gate, g_up, g_down

    return jax.shard_map(moe_layer, mesh=mesh, in_specs=(tok_spec, tok_spec, tok_spec, w_spec, w_spec, w_spec, tok_spec), out_specs=(tok_spec, tok_spec, tok_spec, w_spec, w_spec, w_spec), check_vma=False)
```

```python
import functools

import jax
import jax.numpy as jnp
from jax import lax
from jax.experimental import pallas as pl
from jax.experimental.pallas import tpu as pltpu
from jax.sharding import PartitionSpec as P

GROUP_AXES = ("row", "col", "core")
ALL_AXES = ("rep", "row", "col", "core")
F32 = jnp.float32
BF16 = jnp.bfloat16
LANES = 128
SMALL = 32


def dot_nn(a, b):
    return lax.dot_general(a, b, (((1,), (0,)), ((), ())), preferred_element_type=F32)


def dot_nt(a, b):
    return lax.dot_general(a, b, (((1,), (1,)), ((), ())), preferred_element_type=F32)


def dot_tn(a, b):
    return lax.dot_general(a, b, (((0,), (0,)), ((), ())), preferred_element_type=F32)


def split3(v):
    h1 = v.astype(BF16)
    r1 = v - h1.astype(F32)
    h2 = r1.astype(BF16)
    h3 = (r1 - h2.astype(F32)).astype(BF16)
    return h1, h2, h3


def col_blocks(width, step):
    return [(s, min(step, width - s)) for s in range(0, width, step)]


def expert_kernel(dims, xd_hbm, wg_hbm, wu_hbm, wd_hbm, part_hbm, gg_hbm, gu_hbm, gd_hbm,
                  xd_v, pt_v, gr_v, acc_v, wg_v, wu_v, wd_v, og_v, ou_v, od_v, pos_v,
                  xt_v, qt_v, a_v, duv_v, cnt_s, base_s, sem_x, sem_w, sem_o, sem_p):
    tokens, dm, ff, el, top_k, seg = dims
    n_row, n_col, n_core = lax.axis_size("row"), lax.axis_size("col"), lax.axis_size("core")
    me = (lax.axis_index("row") * n_col + lax.axis_index("col")) * n_core + lax.axis_index("core")
    width = 2 * dm + LANES

    def load_w(e, slot):
        return [pltpu.make_async_copy(h.at[e], v.at[slot], sem_w.at[slot, i])
                for i, (h, v) in enumerate(((wg_hbm, wg_v), (wu_hbm, wu_v), (wd_hbm, wd_v)))]

    def store_g(e, slot):
        return [pltpu.make_async_copy(v.at[slot], h.at[e], sem_o.at[slot, i])
                for i, (h, v) in enumerate(((gg_hbm, og_v), (gu_hbm, ou_v), (gd_hbm, od_v)))]

    loads_x = [pltpu.make_async_copy(xd_hbm.at[m], xd_v.at[m], sem_x.at[m]) for m in range(2)]
    for c in loads_x:
        c.start()
    for s in range(2):
        for c in load_w(s, s):
            c.start()

    row_i = lax.broadcasted_iota(jnp.int32, (tokens, tokens), 0)
    col_i = lax.broadcasted_iota(jnp.int32, (tokens, tokens), 1)
    tri = (row_i < col_i).astype(F32).astype(BF16)
    sub = lax.broadcasted_iota(jnp.int32, (8, tokens), 0)
    eids = jnp.where(sub < el, (me * el + sub), -1).astype(F32)

    def chunks(total):
        return jnp.maximum((total + (seg - 1)) // seg, 1)

    n_chunks = []
    for m in range(2):
        loads_x[m].wait()
        meta_t = xd_v[m, :, 2 * dm:].astype(F32).T
        hits = jnp.zeros((8, tokens), F32)
        for j in range(top_k):
            hits = hits + (meta_t[j:j + 1, :] == eids).astype(F32)
        rank = dot_nn(hits.astype(BF16), tri)
        total = jnp.int32(0)
        for e in range(el):
            cnt = jnp.sum(hits[e:e + 1, :]).astype(jnp.int32)
            cnt_s[m, e] = cnt
            base_s[m, e] = total
            pos_v[m, e:e + 1, :] = jnp.where(hits[e:e + 1, :] > 0, rank[e:e + 1, :] + total.astype(F32), -1.0)
            total = total + (cnt + 15) // 16 * 16
        n_ch = chunks(total)
        n_chunks.append(n_ch)

        def gather(c, carry, m=m):
            off = pl.multiple_of(c * seg, seg)
            rows = (lax.broadcasted_iota(jnp.int32, (seg, tokens), 0) + off).astype(F32)
            pick = rows == pos_v[m, 0:1, :]
            for e in range(1, el):
                pick = pick | (rows == pos_v[m, e:e + 1, :])
            pick_f = pick.astype(F32)
            pt_v[m, :, pl.ds(off, seg)] = pick_f.T.astype(BF16)
            pick_b = pick_f.astype(BF16)
            for s, w in col_blocks(width, 512):
                gr_v[m, pl.ds(off, seg), s:s + w] = dot_nn(pick_b, xd_v[m, :, s:s + w]).astype(BF16)
            return carry

        lax.fori_loop(0, n_ch, gather, 0)

    def tile(e, slot, ra, rb, m_a, n_a, n_b, first):
        rows = ra + rb
        base_a = pl.multiple_of(base_s[m_a, e], 16)
        base_b = pl.multiple_of(base_s[1 - m_a, e], 16)
        it = lax.broadcasted_iota(jnp.int32, (rows, 1), 0)
        valid = ((it < ra) & (it < n_a)) | ((it >= ra) & (it - ra < n_b))

        def read(s, w):
            return jnp.concatenate([gr_v[m_a, pl.ds(base_a, ra), s:s + w],
                                    gr_v[1 - m_a, pl.ds(base_b, rb), s:s + w]], axis=0)

        def write(s, w, val):
            merged = jnp.where(valid, val.astype(F32), read(s, w).astype(F32)).astype(BF16)
            gr_v[m_a, pl.ds(base_a, ra), s:s + w] = merged[:ra]

            @pl.when(n_b > 0)
            def _():
                gr_v[1 - m_a, pl.ds(base_b, rb), s:s + w] = merged[ra:]

        lane = lax.broadcasted_iota(jnp.int32, (rows, LANES), 1)
        meta = jnp.where(valid, read(2 * dm, LANES).astype(F32), 0.0)
        eid = (me * el + e).astype(F32)
        mine = ((meta == eid) & (lane < top_k)).astype(F32)
        sel = pltpu.roll(mine, 8, 1) + pltpu.roll(mine, 16, 1) + pltpu.roll(mine, 24, 1)
        gate = jnp.where(valid, jnp.sum(meta * sel, axis=1, keepdims=True), 0.0)
        for s, w in col_blocks(dm, 256):
            xt_v[:rows, s:s + w] = jnp.where(valid, read(s, w).astype(F32), 0.0).astype(BF16)
            dy = jnp.where(valid, read(dm + s, w).astype(F32), 0.0)
            qt_v[:rows, s:s + w] = (gate * dy).astype(BF16)
        xt = xt_v[:rows, :]
        u = dot_nn(xt, wg_v[slot]).astype(BF16).astype(F32)
        v = dot_nn(xt, wu_v[slot]).astype(BF16).astype(F32)
        r = dot_nt(qt_v[:rows, :], wd_v[slot])
        s_g = jax.nn.sigmoid(u)
        a_v[:rows, :] = (u * s_g * v).astype(BF16)
        duv_v[:rows, :ff] = (r * v * s_g * (1.0 + u * (1.0 - s_g))).astype(BF16)
        duv_v[:rows, ff:] = (r * u * s_g).astype(BF16)
        a = a_v[:rows, :]
        du = duv_v[:rows, :ff]
        dv = duv_v[:rows, ff:]
        dots = jnp.zeros((rows, 1), F32)
        for s, w in col_blocks(dm, 256):
            o = dot_nn(a, wd_v[slot, :, s:s + w]).astype(BF16)
            dy = jnp.where(valid, read(dm + s, w).astype(F32), 0.0)
            dots = dots + jnp.sum(dy * o.astype(F32), axis=1, keepdims=True)
            write(s, w, o)
        for s, w in col_blocks(dm, 256):
            p = dot_nt(du, wg_v[slot, s:s + w, :]) + dot_nt(dv, wu_v[slot, s:s + w, :])
            write(dm + s, w, p.astype(BF16))
        d1, d2, d3 = split3(dots)
        g1, g2, g3 = split3(gate)
        new_meta = jnp.zeros((rows, LANES), F32)
        for at, val in ((e, d1), (8 + e, d2), (16 + e, d3), (32, g1), (33, g2), (34, g3)):
            new_meta = jnp.where(lane == at, val.astype(F32), new_meta)
        write(2 * dm, LANES, new_meta)

        def put(ref, idx, val):
            if first is None:
                ref[idx] = val
            else:
                ref[idx] = jnp.where(first, 0.0, ref[idx]) + val

        duv = duv_v[:rows, :]
        for s, w in col_blocks(dm, 256):
            g_in = dot_tn(xt_v[:rows, s:s + w], duv)
            put(og_v, (slot, slice(s, s + w)), g_in[:, :ff])
            put(ou_v, (slot, slice(s, s + w)), g_in[:, ff:])
        for s, w in col_blocks(dm, 256):
            put(od_v, (slot, slice(None), slice(s, s + w)), dot_tn(a, qt_v[:rows, s:s + w]))

    def expert(e, carry):
        slot = lax.rem(e, 2)
        for c in load_w(e, slot):
            c.wait()

        @pl.when(e >= 2)
        def _():
            for c in store_g(e - 2, slot):
                c.wait()

        n0, n1 = cnt_s[0, e], cnt_s[1, e]
        big0, big1 = n0 > SMALL, n1 > SMALL

        @pl.when(jnp.logical_not(big0 | big1))
        def _():
            tile(e, slot, SMALL, SMALL, 0, n0, n1, None)

        @pl.when(big0 | big1)
        def _():
            both = big0 & big1

            def one(i, inner):
                m_a = jnp.where(both, i, jnp.where(big0, 0, 1))
                n_a = jnp.where(m_a == 0, n0, n1)
                n_b = jnp.where(both, 0, jnp.where(m_a == 0, n1, n0))
                tile(e, slot, seg, SMALL, m_a, n_a, n_b, i == 0)
                return inner

            lax.fori_loop(0, jnp.where(both, 2, 1), one, 0)

        for c in store_g(e, slot):
            c.start()

        @pl.when(e + 2 < el)
        def _():
            for c in load_w(e + 2, slot):
                c.start()

        return carry

    lax.fori_loop(0, el, expert, 0)

    for m in range(2):
        def scatter(c, carry, m=m):
            off = pl.multiple_of(c * seg, seg)
            rows = pl.ds(off, seg)
            first = c == 0
            pt = pt_v[m, :, rows]
            gp = gr_v[m, rows, 2 * dm:].astype(F32)
            gate = gp[:, 32:33] + gp[:, 33:34] + gp[:, 34:35]
            for s, w in col_blocks(dm, 256):
                h1, h2, h3 = split3(gate * gr_v[m, rows, s:s + w].astype(F32))
                add = dot_nn(pt, h1) + dot_nn(pt, h2) + dot_nn(pt, h3)
                acc_v[m, :, s:s + w] = jnp.where(first, 0.0, acc_v[m, :, s:s + w]) + add
            for s, w in col_blocks(dm + LANES, 256):
                lo = dm + s
                add = dot_nn(pt, gr_v[m, rows, lo:lo + w])
                acc_v[m, :, lo:lo + w] = jnp.where(first, 0.0, acc_v[m, :, lo:lo + w]) + add
            return carry

        lax.fori_loop(0, n_chunks[m], scatter, 0)
        lane = lax.broadcasted_iota(jnp.int32, (tokens, LANES), 1)
        ids = jnp.where(lane < top_k, xd_v[m, :, 2 * dm:].astype(F32), -1.0)
        raw = acc_v[m, :, 2 * dm:]
        out = jnp.zeros((tokens, LANES), F32)
        for e in range(el):
            val = raw[:, e:e + 1] + raw[:, 8 + e:9 + e] + raw[:, 16 + e:17 + e]
            out = jnp.where(ids == (me * el + e).astype(F32), val, out)
        acc_v[m, :, 2 * dm:] = out
        pltpu.make_async_copy(acc_v.at[m], part_hbm.at[m], sem_p.at[m]).start()

    for e in range(el - 2, el):
        for c in store_g(e, e % 2):
            c.wait()
    for m in range(2):
        pltpu.make_async_copy(acc_v.at[m], part_hbm.at[m], sem_p.at[m]).wait()


def expert_stage(xd, w_gate, w_up, w_down, top_k, seg):
    _, tokens, width = xd.shape
    el, dm, ff = w_gate.shape
    any_spec = pl.BlockSpec(memory_space=pl.ANY)
    rows_max = el * seg
    tile_rows = seg + SMALL
    dims = (tokens, dm, ff, el, top_k, seg)
    return pl.pallas_call(
        functools.partial(expert_kernel, dims),
        out_shape=(
            jax.ShapeDtypeStruct((2, tokens, width), F32),
            jax.ShapeDtypeStruct((el, dm, ff), F32),
            jax.ShapeDtypeStruct((el, dm, ff), F32),
            jax.ShapeDtypeStruct((el, ff, dm), F32),
        ),
        in_specs=[any_spec] * 4,
        out_specs=[any_spec] * 4,
        scratch_shapes=[
            pltpu.VMEM((2, tokens, width), BF16),
            pltpu.VMEM((2, tokens, rows_max), BF16),
            pltpu.VMEM((2, rows_max, width), BF16),
            pltpu.VMEM((2, tokens, width), F32),
            pltpu.VMEM((2, dm, ff), BF16),
            pltpu.VMEM((2, dm, ff), BF16),
            pltpu.VMEM((2, ff, dm), BF16),
            pltpu.VMEM((2, dm, ff), F32),
            pltpu.VMEM((2, dm, ff), F32),
            pltpu.VMEM((2, ff, dm), F32),
            pltpu.VMEM((2, 8, tokens), F32),
            pltpu.VMEM((tile_rows, dm), BF16),
            pltpu.VMEM((tile_rows, dm), BF16),
            pltpu.VMEM((tile_rows, ff), BF16),
            pltpu.VMEM((tile_rows, 2 * ff), BF16),
            pltpu.SMEM((2, 8), jnp.int32),
            pltpu.SMEM((2, 8), jnp.int32),
            pltpu.SemaphoreType.DMA((2,)),
            pltpu.SemaphoreType.DMA((2, 3)),
            pltpu.SemaphoreType.DMA((2, 3)),
            pltpu.SemaphoreType.DMA((2,)),
        ],
        compiler_params=pltpu.CompilerParams(vmem_limit_bytes=66_000_000),
        name="experts",
    )(xd, w_gate, w_up, w_down)


RING = 4
NEAR = (0, -1, 1, 2)
FAR = (2, -1, 1, 0)


class Place:
    def __init__(self):
        self.at = {a: lax.axis_index(a) for a in GROUP_AXES}
        self.size = {a: lax.axis_size(a) for a in GROUP_AXES}

    def step(self, axis, d):
        n = self.size[axis]
        return lax.rem(self.at[axis] + (d + n), n)

    def axes(self, m):
        return ("col", "row") if m == 0 else ("row", "col")

    def block(self, m, d1, d2, other):
        ax1, ax2 = self.axes(m)
        pos = {ax1: self.step(ax1, d1), ax2: self.step(ax2, d2)}
        core = self.step("core", 1) if other else self.at["core"]
        return (pos["row"] * self.size["col"] + pos["col"]) * self.size["core"] + core

    def barrier(self):
        sem = pltpu.get_barrier_semaphore()
        peers = [{a: self.step(a, d)} for a in ("row", "col") for d in (-1, 1)] + [{"core": self.step("core", 1)}]
        for peer in peers:
            pl.semaphore_signal(sem, inc=1, device_id=peer, device_id_type=pl.DeviceIdType.MESH)
        pl.semaphore_wait(sem, len(peers))


def half_lanes(width):
    mid = (width // LANES + 1) // 2 * LANES
    return (pl.ds(0, mid), pl.ds(mid, width - mid))


def gather_kernel(src_hbm, out_hbm, buf, send_sem, recv_sem, load_sem, out_sem):
    here = Place()
    width = src_hbm.shape[2]
    halves = half_lanes(width)
    sent = []

    def move(m, idx, block, peer, lanes=None):
        ref = buf.at[m, block] if lanes is None else buf.at[m, block, :, lanes]
        return pltpu.make_async_remote_copy(src_ref=ref, dst_ref=ref, send_sem=send_sem.at[m, idx], recv_sem=recv_sem.at[m, idx],
                                            device_id=peer, device_id_type=pl.DeviceIdType.MESH)

    def send(m, idx, block, axis, d, lanes=None):
        c = move(m, idx, block, {axis: here.step(axis, d)}, lanes)
        c.start()
        sent.append(c)

    def arrive(m, idx, block, lanes=None):
        move(m, idx, block, {"core": here.at["core"]}, lanes).wait_recv()

    def keep(m, block):
        pltpu.make_async_copy(buf.at[m, block], out_hbm.at[m, block], out_sem.at[m]).start()

    def blk(m, i, d, other=False):
        return here.block(m, NEAR[i], NEAR[d], other)

    def have(m, i, d):
        b = blk(m, i, d)
        send(m, 20 + 4 * i + d, b, "core", 1)
        keep(m, b)

    def spread(m, i):
        b = blk(m, i, 0)
        ax2 = here.axes(m)[1]
        send(m, 4 + 4 * i, b, ax2, 1)
        send(m, 5 + 4 * i, b, ax2, -1)
        have(m, i, 0)

    loads = [pltpu.make_async_copy(src_hbm.at[m], buf.at[m, blk(m, 0, 0)], load_sem.at[m]) for m in range(2)]
    for c in loads:
        c.start()
    here.barrier()
    for m in range(2):
        loads[m].wait()
        ax1 = here.axes(m)[0]
        send(m, 0, blk(m, 0, 0), ax1, 1)
        send(m, 1, blk(m, 0, 0), ax1, -1)
        spread(m, 0)

    def first_axis(m):
        ax1 = here.axes(m)[0]
        arrive(m, 0, blk(m, 1, 0))
        send(m, 2, blk(m, 1, 0), ax1, 1, halves[0])
        spread(m, 1)
        arrive(m, 1, blk(m, 2, 0))
        send(m, 3, blk(m, 2, 0), ax1, -1, halves[1])
        spread(m, 2)

    def first_axis_far(m):
        arrive(m, 2, blk(m, 3, 0), halves[0])
        arrive(m, 3, blk(m, 3, 0), halves[1])
        spread(m, 3)

    def second_axis(m, i):
        ax2 = here.axes(m)[1]
        arrive(m, 4 + 4 * i, blk(m, i, 1))
        send(m, 6 + 4 * i, blk(m, i, 1), ax2, 1, halves[0])
        have(m, i, 1)
        arrive(m, 5 + 4 * i, blk(m, i, 2))
        send(m, 7 + 4 * i, blk(m, i, 2), ax2, -1, halves[1])
        have(m, i, 2)

    def second_axis_far(m, i):
        arrive(m, 6 + 4 * i, blk(m, i, 3), halves[0])
        arrive(m, 7 + 4 * i, blk(m, i, 3), halves[1])
        have(m, i, 3)

    for m in range(2):
        first_axis(m)
    for m in range(2):
        second_axis(m, 0)
    for m in range(2):
        first_axis_far(m)
    for m in range(2):
        second_axis(m, 1)
    for m in range(2):
        second_axis_far(m, 0)
        second_axis(m, 2)
    for m in range(2):
        second_axis_far(m, 1)
        second_axis(m, 3)
    for m in range(2):
        second_axis_far(m, 2)
    for m in range(2):
        second_axis_far(m, 3)
    for m in range(2):
        for i in range(RING):
            for d in range(RING):
                b = blk(m, i, d, True)
                arrive(m, 20 + 4 * i + d, b)
                keep(m, b)
    for c in sent:
        c.wait_send()
    for m in range(2):
        pltpu.make_async_copy(buf.at[m], out_hbm.at[m], out_sem.at[m]).wait()


def gather_tokens(packed, group):
    _, tok_dev, width = packed.shape
    full = (2, group, tok_dev, width)
    sems = pltpu.SemaphoreType.DMA((2, 36))
    return pl.pallas_call(
        gather_kernel,
        out_shape=jax.ShapeDtypeStruct(full, packed.dtype),
        in_specs=[pl.BlockSpec(memory_space=pl.ANY)],
        out_specs=pl.BlockSpec(memory_space=pl.ANY),
        scratch_shapes=[pltpu.VMEM(full, packed.dtype), sems, sems, pltpu.SemaphoreType.DMA((2,)), pltpu.SemaphoreType.DMA((2,))],
        compiler_params=pltpu.CompilerParams(collective_id=0, has_side_effects=True, vmem_limit_bytes=32_000_000),
        name="gather_tokens",
    )(packed)


def reduce_kernel(dm, top_k, part_hbm, y_ref, dx_ref, dg_ref, own, pair, full, half, load_sem, pair_send, pair_recv, ring_send, ring_recv):
    here = Place()
    width = part_hbm.shape[3]
    halves = half_lanes(width)
    sent = []

    def load(m, q):
        b = here.block(m, FAR[q // RING], FAR[q % RING], False)
        return pltpu.make_async_copy(part_hbm.at[m, b], own.at[m, q], load_sem.at[m, q])

    def swap(m, q):
        b = here.block(m, FAR[q // RING], FAR[q % RING], True)
        return pltpu.make_async_remote_copy(src_ref=part_hbm.at[m, b], dst_ref=pair.at[m, q], send_sem=pair_send.at[m, q],
                                            recv_sem=pair_recv.at[m, q], device_id={"core": here.step("core", 1)},
                                            device_id_type=pl.DeviceIdType.MESH)

    def ring(m, f, kind, q):
        axis = here.axes(m)[0 if f == RING else 1]
        d = 1 if kind % 2 == 0 else -1
        if kind < 2:
            src, dst = own.at[m, q, :, halves[kind]], half.at[m, f, :, halves[kind]]
        else:
            src, dst = own.at[m, q], full.at[m, f, kind - 2]
        return pltpu.make_async_remote_copy(src_ref=src, dst_ref=dst, send_sem=ring_send.at[m, f, kind], recv_sem=ring_recv.at[m, f, kind],
                                            device_id={axis: here.step(axis, d)}, device_id_type=pl.DeviceIdType.MESH)

    def go(m, f, kind, q):
        c = ring(m, f, kind, q)
        c.start()
        sent.append(c)

    def at(f, d):
        k = FAR.index(d)
        return k * RING + FAR.index(0) if f == RING else f * RING + k

    def add_pair(m, q):
        load(m, q).wait()
        swap(m, q).wait_recv()
        own[m, q] = own[m, q] + pair[m, q]

    def far(f, fresh):
        for m in range(2):
            if fresh:
                add_pair(m, at(f, 2))
        for m in range(2):
            go(m, f, 0, at(f, 2))
            go(m, f, 1, at(f, 2))

    def near(f, fresh):
        for m in range(2):
            for kind, d in ((0, 1), (1, -1)):
                q = at(f, d)
                if fresh:
                    add_pair(m, q)
                ring(m, f, kind, q).wait_recv()
                own[m, q, :, halves[kind]] = own[m, q, :, halves[kind]] + half[m, f, :, halves[kind]]
        for m in range(2):
            go(m, f, 2, at(f, 1))
            go(m, f, 3, at(f, -1))

    def done(f, fresh):
        for m in range(2):
            q = at(f, 0)
            if fresh:
                add_pair(m, q)
            ring(m, f, 2, q).wait_recv()
            ring(m, f, 3, q).wait_recv()
            own[m, q] = own[m, q] + full[m, f, 0] + full[m, f, 1]

    order = [at(0, 2), at(1, 2), at(0, 1), at(0, -1), at(2, 2), at(1, 1), at(1, -1), at(3, 2), at(2, 1), at(2, -1), at(0, 0),
             at(3, 1), at(3, -1), at(1, 0), at(2, 0), at(3, 0)]
    for q in order:
        for m in range(2):
            load(m, q).start()
    here.barrier()
    for q in order:
        for m in range(2):
            c = swap(m, q)
            c.start()
            sent.append(c)
    far(0, True)
    far(1, True)
    near(0, True)
    far(2, True)
    near(1, True)
    far(3, True)
    near(2, True)
    done(0, True)
    far(RING, False)
    near(3, True)
    done(1, True)
    done(2, True)
    near(RING, False)
    done(3, True)
    done(RING, False)
    q = at(RING, 0)
    for m in range(2):
        y_ref[m] = own[m, q, :, :dm].astype(BF16)
        dx_ref[m] = own[m, q, :, dm:2 * dm].astype(BF16)
        dg_ref[m] = own[m, q, :, 2 * dm:2 * dm + top_k]
    for c in sent:
        c.wait_send()


def reduce_tokens(part, dm, top_k):
    _, group, tok_dev, width = part.shape
    chips = RING * RING
    vmem = pl.BlockSpec(memory_space=pltpu.VMEM)
    return pl.pallas_call(
        functools.partial(reduce_kernel, dm, top_k),
        out_shape=(
            jax.ShapeDtypeStruct((2, tok_dev, dm), BF16),
            jax.ShapeDtypeStruct((2, tok_dev, dm), BF16),
            jax.ShapeDtypeStruct((2, tok_dev, top_k), F32),
        ),
        in_specs=[pl.BlockSpec(memory_space=pl.ANY)],
        out_specs=(vmem, vmem, vmem),
        scratch_shapes=[
            pltpu.VMEM((2, chips, tok_dev, width), F32),
            pltpu.VMEM((2, chips, tok_dev, width), F32),
            pltpu.VMEM((2, RING + 1, 2, tok_dev, width), F32),
            pltpu.VMEM((2, RING + 1, tok_dev, width), F32),
            pltpu.SemaphoreType.DMA((2, chips)),
            pltpu.SemaphoreType.DMA((2, chips)),
            pltpu.SemaphoreType.DMA((2, chips)),
            pltpu.SemaphoreType.DMA((2, RING + 1, 4)),
            pltpu.SemaphoreType.DMA((2, RING + 1, 4)),
        ],
        compiler_params=pltpu.CompilerParams(collective_id=1, has_side_effects=True, vmem_limit_bytes=40_000_000),
        name="reduce_tokens",
    )(part)


def pack_tokens(x, route_idx, gates, grad_y):
    def piece(v):
        return lax.reduce_precision(v, 8, 7)

    g1 = piece(gates)
    g2 = piece(gates - g1)
    g3 = piece(gates - g1 - g2)

    def pad(v):
        return jnp.pad(v.astype(BF16), ((0, 0), (0, 0), (0, 8 - v.shape[2])))

    ids = route_idx.astype(F32)
    meta = jnp.concatenate([pad(ids), pad(g1), pad(g2), pad(g3)], axis=2)
    meta = jnp.pad(meta, ((0, 0), (0, 0), (0, LANES - meta.shape[2])))
    return jnp.concatenate([x, grad_y, meta], axis=2)


def solution(mesh):
    group = mesh.shape["row"] * mesh.shape["col"] * mesh.shape["core"]
    tok_spec = P(None, ALL_AXES, None)
    w_spec = P(ALL_AXES, None, None)

    def moe_layer(x, route_idx, gates, w_gate, w_up, w_down, grad_y):
        _, tok_dev, dm = x.shape
        top_k = route_idx.shape[2]
        packed = pack_tokens(x, route_idx, gates, grad_y)
        xd = gather_tokens(packed, group).reshape(2, group * tok_dev, packed.shape[2])
        part, g_gate, g_up, g_down = expert_stage(xd, w_gate, w_up, w_down, top_k, group * (tok_dev // 2))
        y, dx, dg = reduce_tokens(part.reshape(2, group, tok_dev, packed.shape[2]), dm, top_k)
        return y, dx, dg, g_gate, g_up, g_down

    return jax.shard_map(moe_layer, mesh=mesh, in_specs=(tok_spec, tok_spec, tok_spec, w_spec, w_spec, w_spec, tok_spec), out_specs=(tok_spec, tok_spec, tok_spec, w_spec, w_spec, w_spec), check_vma=False)
```

```python
import functools

import jax
import jax.numpy as jnp
from jax import lax
from jax.experimental import pallas as pl
from jax.experimental.pallas import tpu as pltpu
from jax.sharding import PartitionSpec as P

GROUP_AXES = ("row", "col", "core")
ALL_AXES = ("rep", "row", "col", "core")
F32 = jnp.float32
BF16 = jnp.bfloat16
LANES = 128
SMALL = 32


def dot_nn(a, b):
    return lax.dot_general(a, b, (((1,), (0,)), ((), ())), preferred_element_type=F32)


def dot_nt(a, b):
    return lax.dot_general(a, b, (((1,), (1,)), ((), ())), preferred_element_type=F32)


def dot_tn(a, b):
    return lax.dot_general(a, b, (((0,), (0,)), ((), ())), preferred_element_type=F32)


def split3(v):
    h1 = v.astype(BF16)
    r1 = v - h1.astype(F32)
    h2 = r1.astype(BF16)
    h3 = (r1 - h2.astype(F32)).astype(BF16)
    return h1, h2, h3


def col_blocks(width, step):
    return [(s, min(step, width - s)) for s in range(0, width, step)]


def expert_kernel(dims, xd_hbm, wg_hbm, wu_hbm, wd_hbm, part_hbm, gg_hbm, gu_hbm, gd_hbm,
                  xd_v, pt_v, gr_v, acc_v, wg_v, wu_v, wd_v, og_v, ou_v, od_v, pos_v,
                  xt_v, qt_v, a_v, duv_v, cnt_s, base_s, sem_x, sem_w, sem_o, sem_p):
    tokens, dm, ff, el, top_k, seg = dims
    n_row, n_col, n_core = lax.axis_size("row"), lax.axis_size("col"), lax.axis_size("core")
    me = (lax.axis_index("row") * n_col + lax.axis_index("col")) * n_core + lax.axis_index("core")
    width = 2 * dm + LANES

    def load_w(e, slot):
        return [pltpu.make_async_copy(h.at[e], v.at[slot], sem_w.at[slot, i])
                for i, (h, v) in enumerate(((wg_hbm, wg_v), (wu_hbm, wu_v), (wd_hbm, wd_v)))]

    def store_g(e, slot):
        return [pltpu.make_async_copy(v.at[slot], h.at[e], sem_o.at[slot, i])
                for i, (h, v) in enumerate(((gg_hbm, og_v), (gu_hbm, ou_v), (gd_hbm, od_v)))]

    loads_x = [pltpu.make_async_copy(xd_hbm.at[m], xd_v.at[m], sem_x.at[m]) for m in range(2)]
    for c in loads_x:
        c.start()
    for s in range(2):
        for c in load_w(s, s):
            c.start()

    row_i = lax.broadcasted_iota(jnp.int32, (tokens, tokens), 0)
    col_i = lax.broadcasted_iota(jnp.int32, (tokens, tokens), 1)
    tri = (row_i < col_i).astype(F32).astype(BF16)
    sub = lax.broadcasted_iota(jnp.int32, (8, tokens), 0)
    eids = jnp.where(sub < el, (me * el + sub), -1).astype(F32)

    def chunks(total):
        return jnp.maximum((total + (seg - 1)) // seg, 1)

    n_chunks = []
    for m in range(2):
        loads_x[m].wait()
        meta_t = xd_v[m, :, 2 * dm:].astype(F32).T
        hits = jnp.zeros((8, tokens), F32)
        for j in range(top_k):
            hits = hits + (meta_t[j:j + 1, :] == eids).astype(F32)
        rank = dot_nn(hits.astype(BF16), tri)
        total = jnp.int32(0)
        for e in range(el):
            cnt = jnp.sum(hits[e:e + 1, :]).astype(jnp.int32)
            cnt_s[m, e] = cnt
            base_s[m, e] = total
            pos_v[m, e:e + 1, :] = jnp.where(hits[e:e + 1, :] > 0, rank[e:e + 1, :] + total.astype(F32), -1.0)
            total = total + (cnt + 15) // 16 * 16
        n_ch = chunks(total)
        n_chunks.append(n_ch)

        def gather(c, carry, m=m):
            off = pl.multiple_of(c * seg, seg)
            rows = (lax.broadcasted_iota(jnp.int32, (seg, tokens), 0) + off).astype(F32)
            pick = rows == pos_v[m, 0:1, :]
            for e in range(1, el):
                pick = pick | (rows == pos_v[m, e:e + 1, :])
            pick_f = pick.astype(F32)
            pt_v[m, :, pl.ds(off, seg)] = pick_f.T.astype(BF16)
            pick_b = pick_f.astype(BF16)
            for s, w in col_blocks(width, 512):
                gr_v[m, pl.ds(off, seg), s:s + w] = dot_nn(pick_b, xd_v[m, :, s:s + w]).astype(BF16)
            return carry

        lax.fori_loop(0, n_ch, gather, 0)

    def tile(e, slot, ra, rb, m_a, n_a, n_b, first):
        rows = ra + rb
        base_a = pl.multiple_of(base_s[m_a, e], 16)
        base_b = pl.multiple_of(base_s[1 - m_a, e], 16)
        it = lax.broadcasted_iota(jnp.int32, (rows, 1), 0)
        valid = ((it < ra) & (it < n_a)) | ((it >= ra) & (it - ra < n_b))

        def read(s, w):
            return jnp.concatenate([gr_v[m_a, pl.ds(base_a, ra), s:s + w],
                                    gr_v[1 - m_a, pl.ds(base_b, rb), s:s + w]], axis=0)

        def write(s, w, val):
            merged = jnp.where(valid, val.astype(F32), read(s, w).astype(F32)).astype(BF16)
            gr_v[m_a, pl.ds(base_a, ra), s:s + w] = merged[:ra]

            @pl.when(n_b > 0)
            def _():
                gr_v[1 - m_a, pl.ds(base_b, rb), s:s + w] = merged[ra:]

        lane = lax.broadcasted_iota(jnp.int32, (rows, LANES), 1)
        meta = jnp.where(valid, read(2 * dm, LANES).astype(F32), 0.0)
        eid = (me * el + e).astype(F32)
        mine = ((meta == eid) & (lane < top_k)).astype(F32)
        sel = pltpu.roll(mine, 8, 1) + pltpu.roll(mine, 16, 1) + pltpu.roll(mine, 24, 1)
        gate = jnp.where(valid, jnp.sum(meta * sel, axis=1, keepdims=True), 0.0)
        for s, w in col_blocks(dm, 256):
            xt_v[:rows, s:s + w] = jnp.where(valid, read(s, w).astype(F32), 0.0).astype(BF16)
            dy = jnp.where(valid, read(dm + s, w).astype(F32), 0.0)
            qt_v[:rows, s:s + w] = (gate * dy).astype(BF16)
        xt = xt_v[:rows, :]
        u = dot_nn(xt, wg_v[slot]).astype(BF16).astype(F32)
        v = dot_nn(xt, wu_v[slot]).astype(BF16).astype(F32)
        r = dot_nt(qt_v[:rows, :], wd_v[slot])
        s_g = jax.nn.sigmoid(u)
        a_v[:rows, :] = (u * s_g * v).astype(BF16)
        duv_v[:rows, :ff] = (r * v * s_g * (1.0 + u * (1.0 - s_g))).astype(BF16)
        duv_v[:rows, ff:] = (r * u * s_g).astype(BF16)
        a = a_v[:rows, :]
        du = duv_v[:rows, :ff]
        dv = duv_v[:rows, ff:]
        dots = jnp.zeros((rows, 1), F32)
        for s, w in col_blocks(dm, 256):
            o = dot_nn(a, wd_v[slot, :, s:s + w]).astype(BF16)
            dy = jnp.where(valid, read(dm + s, w).astype(F32), 0.0)
            dots = dots + jnp.sum(dy * o.astype(F32), axis=1, keepdims=True)
            write(s, w, o)
        for s, w in col_blocks(dm, 256):
            p = dot_nt(du, wg_v[slot, s:s + w, :]) + dot_nt(dv, wu_v[slot, s:s + w, :])
            write(dm + s, w, p.astype(BF16))
        d1, d2, d3 = split3(dots)
        g1, g2, g3 = split3(gate)
        new_meta = jnp.zeros((rows, LANES), F32)
        for at, val in ((e, d1), (8 + e, d2), (16 + e, d3), (32, g1), (33, g2), (34, g3)):
            new_meta = jnp.where(lane == at, val.astype(F32), new_meta)
        write(2 * dm, LANES, new_meta)

        def put(ref, idx, val):
            if first is None:
                ref[idx] = val
            else:
                ref[idx] = jnp.where(first, 0.0, ref[idx]) + val

        duv = duv_v[:rows, :]
        for s, w in col_blocks(dm, 256):
            g_in = dot_tn(xt_v[:rows, s:s + w], duv)
            put(og_v, (slot, slice(s, s + w)), g_in[:, :ff])
            put(ou_v, (slot, slice(s, s + w)), g_in[:, ff:])
        for s, w in col_blocks(dm, 256):
            put(od_v, (slot, slice(None), slice(s, s + w)), dot_tn(a, qt_v[:rows, s:s + w]))

    def expert(e, carry):
        slot = lax.rem(e, 2)
        for c in load_w(e, slot):
            c.wait()

        @pl.when(e >= 2)
        def _():
            for c in store_g(e - 2, slot):
                c.wait()

        n0, n1 = cnt_s[0, e], cnt_s[1, e]
        big0, big1 = n0 > SMALL, n1 > SMALL

        @pl.when(jnp.logical_not(big0 | big1))
        def _():
            tile(e, slot, SMALL, SMALL, 0, n0, n1, None)

        @pl.when(big0 | big1)
        def _():
            both = big0 & big1

            def one(i, inner):
                m_a = jnp.where(both, i, jnp.where(big0, 0, 1))
                n_a = jnp.where(m_a == 0, n0, n1)
                n_b = jnp.where(both, 0, jnp.where(m_a == 0, n1, n0))
                tile(e, slot, seg, SMALL, m_a, n_a, n_b, i == 0)
                return inner

            lax.fori_loop(0, jnp.where(both, 2, 1), one, 0)

        for c in store_g(e, slot):
            c.start()

        @pl.when(e + 2 < el)
        def _():
            for c in load_w(e + 2, slot):
                c.start()

        return carry

    lax.fori_loop(0, el, expert, 0)

    for m in range(2):
        def scatter(c, carry, m=m):
            off = pl.multiple_of(c * seg, seg)
            rows = pl.ds(off, seg)
            first = c == 0
            pt = pt_v[m, :, rows]
            gp = gr_v[m, rows, 2 * dm:].astype(F32)
            gate = gp[:, 32:33] + gp[:, 33:34] + gp[:, 34:35]
            for s, w in col_blocks(dm, 256):
                h1, h2, h3 = split3(gate * gr_v[m, rows, s:s + w].astype(F32))
                add = dot_nn(pt, h1) + dot_nn(pt, h2) + dot_nn(pt, h3)
                acc_v[m, :, s:s + w] = jnp.where(first, 0.0, acc_v[m, :, s:s + w]) + add
            for s, w in col_blocks(dm + LANES, 256):
                lo = dm + s
                add = dot_nn(pt, gr_v[m, rows, lo:lo + w])
                acc_v[m, :, lo:lo + w] = jnp.where(first, 0.0, acc_v[m, :, lo:lo + w]) + add
            return carry

        lax.fori_loop(0, n_chunks[m], scatter, 0)
        lane = lax.broadcasted_iota(jnp.int32, (tokens, LANES), 1)
        ids = jnp.where(lane < top_k, xd_v[m, :, 2 * dm:].astype(F32), -1.0)
        raw = acc_v[m, :, 2 * dm:]
        out = jnp.zeros((tokens, LANES), F32)
        for e in range(el):
            val = raw[:, e:e + 1] + raw[:, 8 + e:9 + e] + raw[:, 16 + e:17 + e]
            out = jnp.where(ids == (me * el + e).astype(F32), val, out)
        acc_v[m, :, 2 * dm:] = out
        pltpu.make_async_copy(acc_v.at[m], part_hbm.at[m], sem_p.at[m]).start()

    for e in range(el - 2, el):
        for c in store_g(e, e % 2):
            c.wait()
    for m in range(2):
        pltpu.make_async_copy(acc_v.at[m], part_hbm.at[m], sem_p.at[m]).wait()


def expert_stage(xd, w_gate, w_up, w_down, top_k, seg):
    _, tokens, width = xd.shape
    el, dm, ff = w_gate.shape
    any_spec = pl.BlockSpec(memory_space=pltpu.HBM)
    rows_max = el * seg
    tile_rows = seg + SMALL
    dims = (tokens, dm, ff, el, top_k, seg)
    return pl.pallas_call(
        functools.partial(expert_kernel, dims),
        out_shape=(
            jax.ShapeDtypeStruct((2, tokens, width), F32),
            jax.ShapeDtypeStruct((el, dm, ff), F32),
            jax.ShapeDtypeStruct((el, dm, ff), F32),
            jax.ShapeDtypeStruct((el, ff, dm), F32),
        ),
        in_specs=[any_spec] * 4,
        out_specs=[any_spec] * 4,
        scratch_shapes=[
            pltpu.VMEM((2, tokens, width), BF16),
            pltpu.VMEM((2, tokens, rows_max), BF16),
            pltpu.VMEM((2, rows_max, width), BF16),
            pltpu.VMEM((2, tokens, width), F32),
            pltpu.VMEM((2, dm, ff), BF16),
            pltpu.VMEM((2, dm, ff), BF16),
            pltpu.VMEM((2, ff, dm), BF16),
            pltpu.VMEM((2, dm, ff), F32),
            pltpu.VMEM((2, dm, ff), F32),
            pltpu.VMEM((2, ff, dm), F32),
            pltpu.VMEM((2, 8, tokens), F32),
            pltpu.VMEM((tile_rows, dm), BF16),
            pltpu.VMEM((tile_rows, dm), BF16),
            pltpu.VMEM((tile_rows, ff), BF16),
            pltpu.VMEM((tile_rows, 2 * ff), BF16),
            pltpu.SMEM((2, 8), jnp.int32),
            pltpu.SMEM((2, 8), jnp.int32),
            pltpu.SemaphoreType.DMA((2,)),
            pltpu.SemaphoreType.DMA((2, 3)),
            pltpu.SemaphoreType.DMA((2, 3)),
            pltpu.SemaphoreType.DMA((2,)),
        ],
        compiler_params=pltpu.CompilerParams(vmem_limit_bytes=66_000_000),
        name="experts",
    )(xd, w_gate, w_up, w_down)


RING = 4
NEAR = (0, -1, 1, 2)
FAR = (2, -1, 1, 0)


class Place:
    def __init__(self):
        self.at = {a: lax.axis_index(a) for a in GROUP_AXES}
        self.size = {a: lax.axis_size(a) for a in GROUP_AXES}

    def step(self, axis, d):
        n = self.size[axis]
        return lax.rem(self.at[axis] + (d + n), n)

    def axes(self, m):
        return ("col", "row") if m == 0 else ("row", "col")

    def block(self, m, d1, d2, other):
        ax1, ax2 = self.axes(m)
        pos = {ax1: self.step(ax1, d1), ax2: self.step(ax2, d2)}
        core = self.step("core", 1) if other else self.at["core"]
        return (pos["row"] * self.size["col"] + pos["col"]) * self.size["core"] + core

    def barrier(self):
        sem = pltpu.get_barrier_semaphore()
        peers = [{a: self.step(a, d)} for a in ("row", "col") for d in (-1, 1)] + [{"core": self.step("core", 1)}]
        for peer in peers:
            pl.semaphore_signal(sem, inc=1, device_id=peer, device_id_type=pl.DeviceIdType.MESH)
        pl.semaphore_wait(sem, len(peers))


def half_lanes(width):
    mid = (width // LANES + 1) // 2 * LANES
    return (pl.ds(0, mid), pl.ds(mid, width - mid))


def gather_kernel(src_hbm, out_hbm, buf, send_sem, recv_sem, load_sem, out_sem):
    here = Place()
    width = src_hbm.shape[2]
    halves = half_lanes(width)
    sent = []

    def move(m, idx, block, peer, lanes=None):
        ref = buf.at[m, block] if lanes is None else buf.at[m, block, :, lanes]
        return pltpu.make_async_remote_copy(src_ref=ref, dst_ref=ref, send_sem=send_sem.at[m, idx], recv_sem=recv_sem.at[m, idx],
                                            device_id=peer, device_id_type=pl.DeviceIdType.MESH)

    def send(m, idx, block, axis, d, lanes=None):
        c = move(m, idx, block, {axis: here.step(axis, d)}, lanes)
        c.start()
        sent.append(c)

    def arrive(m, idx, block, lanes=None):
        move(m, idx, block, {"core": here.at["core"]}, lanes).wait_recv()

    def keep(m, block):
        pltpu.make_async_copy(buf.at[m, block], out_hbm.at[m, block], out_sem.at[m]).start()

    def blk(m, i, d, other=False):
        return here.block(m, NEAR[i], NEAR[d], other)

    def have(m, i, d):
        b = blk(m, i, d)
        send(m, 20 + 4 * i + d, b, "core", 1)
        keep(m, b)

    def spread(m, i):
        b = blk(m, i, 0)
        ax2 = here.axes(m)[1]
        send(m, 4 + 4 * i, b, ax2, 1)
        send(m, 5 + 4 * i, b, ax2, -1)
        have(m, i, 0)

    loads = [pltpu.make_async_copy(src_hbm.at[m], buf.at[m, blk(m, 0, 0)], load_sem.at[m]) for m in range(2)]
    for c in loads:
        c.start()
    here.barrier()
    for m in range(2):
        loads[m].wait()
        ax1 = here.axes(m)[0]
        send(m, 0, blk(m, 0, 0), ax1, 1)
        send(m, 1, blk(m, 0, 0), ax1, -1)
        spread(m, 0)

    def first_axis(m):
        ax1 = here.axes(m)[0]
        arrive(m, 0, blk(m, 1, 0))
        send(m, 2, blk(m, 1, 0), ax1, 1, halves[0])
        spread(m, 1)
        arrive(m, 1, blk(m, 2, 0))
        send(m, 3, blk(m, 2, 0), ax1, -1, halves[1])
        spread(m, 2)

    def first_axis_far(m):
        arrive(m, 2, blk(m, 3, 0), halves[0])
        arrive(m, 3, blk(m, 3, 0), halves[1])
        spread(m, 3)

    def second_axis(m, i):
        ax2 = here.axes(m)[1]
        arrive(m, 4 + 4 * i, blk(m, i, 1))
        send(m, 6 + 4 * i, blk(m, i, 1), ax2, 1, halves[0])
        have(m, i, 1)
        arrive(m, 5 + 4 * i, blk(m, i, 2))
        send(m, 7 + 4 * i, blk(m, i, 2), ax2, -1, halves[1])
        have(m, i, 2)

    def second_axis_far(m, i):
        arrive(m, 6 + 4 * i, blk(m, i, 3), halves[0])
        arrive(m, 7 + 4 * i, blk(m, i, 3), halves[1])
        have(m, i, 3)

    for m in range(2):
        first_axis(m)
    for m in range(2):
        second_axis(m, 0)
    for m in range(2):
        first_axis_far(m)
    for m in range(2):
        second_axis(m, 1)
    for m in range(2):
        second_axis_far(m, 0)
        second_axis(m, 2)
    for m in range(2):
        second_axis_far(m, 1)
        second_axis(m, 3)
    for m in range(2):
        second_axis_far(m, 2)
    for m in range(2):
        second_axis_far(m, 3)
    for m in range(2):
        for i in range(RING):
            for d in range(RING):
                b = blk(m, i, d, True)
                arrive(m, 20 + 4 * i + d, b)
                keep(m, b)
    for c in sent:
        c.wait_send()
    for m in range(2):
        pltpu.make_async_copy(buf.at[m], out_hbm.at[m], out_sem.at[m]).wait()


def gather_tokens(packed, group):
    _, tok_dev, width = packed.shape
    full = (2, group, tok_dev, width)
    sems = pltpu.SemaphoreType.DMA((2, 36))
    return pl.pallas_call(
        gather_kernel,
        out_shape=jax.ShapeDtypeStruct(full, packed.dtype),
        in_specs=[pl.BlockSpec(memory_space=pl.ANY)],
        out_specs=pl.BlockSpec(memory_space=pltpu.HBM),
        scratch_shapes=[pltpu.VMEM(full, packed.dtype), sems, sems, pltpu.SemaphoreType.DMA((2,)), pltpu.SemaphoreType.DMA((2,))],
        compiler_params=pltpu.CompilerParams(collective_id=0, has_side_effects=True, vmem_limit_bytes=32_000_000),
        name="gather_tokens",
    )(packed)


def reduce_kernel(dm, top_k, part_hbm, y_ref, dx_ref, dg_ref, own, pair, full, half, load_sem, pair_send, pair_recv, ring_send, ring_recv):
    here = Place()
    width = part_hbm.shape[3]
    halves = half_lanes(width)
    sent = []

    def load(m, q):
        b = here.block(m, FAR[q // RING], FAR[q % RING], False)
        return pltpu.make_async_copy(part_hbm.at[m, b], own.at[m, q], load_sem.at[m, q])

    def swap(m, q):
        b = here.block(m, FAR[q // RING], FAR[q % RING], True)
        return pltpu.make_async_remote_copy(src_ref=part_hbm.at[m, b], dst_ref=pair.at[m, q], send_sem=pair_send.at[m, q],
                                            recv_sem=pair_recv.at[m, q], device_id={"core": here.step("core", 1)},
                                            device_id_type=pl.DeviceIdType.MESH)

    def ring(m, f, kind, q):
        axis = here.axes(m)[0 if f == RING else 1]
        d = 1 if kind % 2 == 0 else -1
        if kind < 2:
            src, dst = own.at[m, q, :, halves[kind]], half.at[m, f, :, halves[kind]]
        else:
            src, dst = own.at[m, q], full.at[m, f, kind - 2]
        return pltpu.make_async_remote_copy(src_ref=src, dst_ref=dst, send_sem=ring_send.at[m, f, kind], recv_sem=ring_recv.at[m, f, kind],
                                            device_id={axis: here.step(axis, d)}, device_id_type=pl.DeviceIdType.MESH)

    def go(m, f, kind, q):
        c = ring(m, f, kind, q)
        c.start()
        sent.append(c)

    def at(f, d):
        k = FAR.index(d)
        return k * RING + FAR.index(0) if f == RING else f * RING + k

    def add_pair(m, q):
        load(m, q).wait()
        swap(m, q).wait_recv()
        own[m, q] = own[m, q] + pair[m, q]

    def far(f, fresh):
        for m in range(2):
            if fresh:
                add_pair(m, at(f, 2))
        for m in range(2):
            go(m, f, 0, at(f, 2))
            go(m, f, 1, at(f, 2))

    def near(f, fresh):
        for m in range(2):
            for kind, d in ((0, 1), (1, -1)):
                q = at(f, d)
                if fresh:
                    add_pair(m, q)
                ring(m, f, kind, q).wait_recv()
                own[m, q, :, halves[kind]] = own[m, q, :, halves[kind]] + half[m, f, :, halves[kind]]
        for m in range(2):
            go(m, f, 2, at(f, 1))
            go(m, f, 3, at(f, -1))

    def done(f, fresh):
        for m in range(2):
            q = at(f, 0)
            if fresh:
                add_pair(m, q)
            ring(m, f, 2, q).wait_recv()
            ring(m, f, 3, q).wait_recv()
            own[m, q] = own[m, q] + full[m, f, 0] + full[m, f, 1]

    order = [at(0, 2), at(1, 2), at(0, 1), at(0, -1), at(2, 2), at(1, 1), at(1, -1), at(3, 2), at(2, 1), at(2, -1), at(0, 0),
             at(3, 1), at(3, -1), at(1, 0), at(2, 0), at(3, 0)]
    for q in order:
        for m in range(2):
            load(m, q).start()
    here.barrier()
    for q in order:
        for m in range(2):
            c = swap(m, q)
            c.start()
            sent.append(c)
    far(0, True)
    far(1, True)
    near(0, True)
    far(2, True)
    near(1, True)
    far(3, True)
    near(2, True)
    done(0, True)
    far(RING, False)
    near(3, True)
    done(1, True)
    done(2, True)
    near(RING, False)
    done(3, True)
    done(RING, False)
    q = at(RING, 0)
    for m in range(2):
        y_ref[m] = own[m, q, :, :dm].astype(BF16)
        dx_ref[m] = own[m, q, :, dm:2 * dm].astype(BF16)
        dg_ref[m] = own[m, q, :, 2 * dm:2 * dm + top_k]
    for c in sent:
        c.wait_send()


def reduce_tokens(part, dm, top_k):
    _, group, tok_dev, width = part.shape
    chips = RING * RING
    vmem = pl.BlockSpec(memory_space=pltpu.VMEM)
    return pl.pallas_call(
        functools.partial(reduce_kernel, dm, top_k),
        out_shape=(
            jax.ShapeDtypeStruct((2, tok_dev, dm), BF16),
            jax.ShapeDtypeStruct((2, tok_dev, dm), BF16),
            jax.ShapeDtypeStruct((2, tok_dev, top_k), F32),
        ),
        in_specs=[pl.BlockSpec(memory_space=pltpu.HBM)],
        out_specs=(vmem, vmem, vmem),
        scratch_shapes=[
            pltpu.VMEM((2, chips, tok_dev, width), F32),
            pltpu.VMEM((2, chips, tok_dev, width), F32),
            pltpu.VMEM((2, RING + 1, 2, tok_dev, width), F32),
            pltpu.VMEM((2, RING + 1, tok_dev, width), F32),
            pltpu.SemaphoreType.DMA((2, chips)),
            pltpu.SemaphoreType.DMA((2, chips)),
            pltpu.SemaphoreType.DMA((2, chips)),
            pltpu.SemaphoreType.DMA((2, RING + 1, 4)),
            pltpu.SemaphoreType.DMA((2, RING + 1, 4)),
        ],
        compiler_params=pltpu.CompilerParams(collective_id=1, has_side_effects=True, vmem_limit_bytes=40_000_000),
        name="reduce_tokens",
    )(part)


def pack_tokens(x, route_idx, gates, grad_y):
    def piece(v):
        return lax.reduce_precision(v, 8, 7)

    g1 = piece(gates)
    g2 = piece(gates - g1)
    g3 = piece(gates - g1 - g2)

    def pad(v):
        return jnp.pad(v.astype(BF16), ((0, 0), (0, 0), (0, 8 - v.shape[2])))

    ids = route_idx.astype(F32)
    meta = jnp.concatenate([pad(ids), pad(g1), pad(g2), pad(g3)], axis=2)
    meta = jnp.pad(meta, ((0, 0), (0, 0), (0, LANES - meta.shape[2])))
    return jnp.concatenate([x, grad_y, meta], axis=2)


def solution(mesh):
    group = mesh.shape["row"] * mesh.shape["col"] * mesh.shape["core"]
    tok_spec = P(None, ALL_AXES, None)
    w_spec = P(ALL_AXES, None, None)

    def moe_layer(x, route_idx, gates, w_gate, w_up, w_down, grad_y):
        _, tok_dev, dm = x.shape
        top_k = route_idx.shape[2]
        packed = pack_tokens(x, route_idx, gates, grad_y)
        xd = gather_tokens(packed, group).reshape(2, group * tok_dev, packed.shape[2])
        part, g_gate, g_up, g_down = expert_stage(xd, w_gate, w_up, w_down, top_k, group * (tok_dev // 2))
        y, dx, dg = reduce_tokens(part.reshape(2, group, tok_dev, packed.shape[2]), dm, top_k)
        return y, dx, dg, g_gate, g_up, g_down

    return jax.shard_map(moe_layer, mesh=mesh, in_specs=(tok_spec, tok_spec, tok_spec, w_spec, w_spec, w_spec, tok_spec), out_specs=(tok_spec, tok_spec, tok_spec, w_spec, w_spec, w_spec), check_vma=False)
```

```python
import functools

import jax
import jax.numpy as jnp
from jax import lax
from jax.experimental import pallas as pl
from jax.experimental.pallas import tpu as pltpu
from jax.sharding import PartitionSpec as P

GROUP_AXES = ("row", "col", "core")
ALL_AXES = ("rep", "row", "col", "core")
F32 = jnp.float32
BF16 = jnp.bfloat16
LANES = 128
SMALL = 32
VMEM_LIMIT = 66_000_000


def dot_nn(a, b):
    return lax.dot_general(a, b, (((1,), (0,)), ((), ())), preferred_element_type=F32)


def dot_nt(a, b):
    return lax.dot_general(a, b, (((1,), (1,)), ((), ())), preferred_element_type=F32)


def dot_tn(a, b):
    return lax.dot_general(a, b, (((0,), (0,)), ((), ())), preferred_element_type=F32)


def split3(v):
    h1 = v.astype(BF16)
    r1 = v - h1.astype(F32)
    h2 = r1.astype(BF16)
    h3 = (r1 - h2.astype(F32)).astype(BF16)
    return h1, h2, h3


def col_blocks(width, step):
    return [(s, min(step, width - s)) for s in range(0, width, step)]


def expert_kernel(dims, xd_hbm, wg_hbm, wu_hbm, wd_hbm, part_hbm, gg_hbm, gu_hbm, gd_hbm,
                  xd_v, pt_v, gr_v, acc_v, wg_v, wu_v, wd_v, og_v, ou_v, od_v, pos_v,
                  xt_v, qt_v, a_v, duv_v, cnt_s, base_s, sem_x, sem_w, sem_o, sem_p):
    tokens, dm, ff, el, top_k, seg = dims
    n_row, n_col, n_core = lax.axis_size("row"), lax.axis_size("col"), lax.axis_size("core")
    me = (lax.axis_index("row") * n_col + lax.axis_index("col")) * n_core + lax.axis_index("core")
    width = 2 * dm + LANES

    def load_w(e, slot):
        return [pltpu.make_async_copy(h.at[e], v.at[slot], sem_w.at[slot, i])
                for i, (h, v) in enumerate(((wg_hbm, wg_v), (wu_hbm, wu_v), (wd_hbm, wd_v)))]

    def store_g(e, slot):
        return [pltpu.make_async_copy(v.at[slot], h.at[e], sem_o.at[slot, i])
                for i, (h, v) in enumerate(((gg_hbm, og_v), (gu_hbm, ou_v), (gd_hbm, od_v)))]

    loads_x = [pltpu.make_async_copy(xd_hbm.at[m], xd_v.at[m], sem_x.at[m]) for m in range(2)]
    for c in loads_x:
        c.start()
    for s in range(2):
        for c in load_w(s, s):
            c.start()

    row_i = lax.broadcasted_iota(jnp.int32, (tokens, tokens), 0)
    col_i = lax.broadcasted_iota(jnp.int32, (tokens, tokens), 1)
    tri = (row_i < col_i).astype(F32).astype(BF16)
    sub = lax.broadcasted_iota(jnp.int32, (8, tokens), 0)
    eids = jnp.where(sub < el, (me * el + sub), -1).astype(F32)

    def chunks(total):
        return jnp.maximum((total + (seg - 1)) // seg, 1)

    n_chunks = []
    for m in range(2):
        loads_x[m].wait()
        meta_t = xd_v[m, :, 2 * dm:].astype(F32).T
        hits = jnp.zeros((8, tokens), F32)
        for j in range(top_k):
            hits = hits + (meta_t[j:j + 1, :] == eids).astype(F32)
        rank = dot_nn(hits.astype(BF16), tri)
        total = jnp.int32(0)
        for e in range(el):
            cnt = jnp.sum(hits[e:e + 1, :]).astype(jnp.int32)
            cnt_s[m, e] = cnt
            base_s[m, e] = total
            pos_v[m, e:e + 1, :] = jnp.where(hits[e:e + 1, :] > 0, rank[e:e + 1, :] + total.astype(F32), -1.0)
            total = total + (cnt + 15) // 16 * 16
        n_ch = chunks(total)
        n_chunks.append(n_ch)

        def gather(c, carry, m=m):
            off = pl.multiple_of(c * seg, seg)
            rows = (lax.broadcasted_iota(jnp.int32, (seg, tokens), 0) + off).astype(F32)
            pick = rows == pos_v[m, 0:1, :]
            for e in range(1, el):
                pick = pick | (rows == pos_v[m, e:e + 1, :])
            pick_f = pick.astype(F32)
            pt_v[m, :, pl.ds(off, seg)] = pick_f.T.astype(BF16)
            pick_b = pick_f.astype(BF16)
            for s, w in col_blocks(width, 512):
                gr_v[m, pl.ds(off, seg), s:s + w] = dot_nn(pick_b, xd_v[m, :, s:s + w]).astype(BF16)
            return carry

        lax.fori_loop(0, n_ch, gather, 0)

    def tile(e, slot, ra, rb, m_a, n_a, n_b, first):
        rows = ra + rb
        base_a = pl.multiple_of(base_s[m_a, e], 16)
        base_b = pl.multiple_of(base_s[1 - m_a, e], 16)
        it = lax.broadcasted_iota(jnp.int32, (rows, 1), 0)
        valid = ((it < ra) & (it < n_a)) | ((it >= ra) & (it - ra < n_b))

        def read(s, w):
            return jnp.concatenate([gr_v[m_a, pl.ds(base_a, ra), s:s + w],
                                    gr_v[1 - m_a, pl.ds(base_b, rb), s:s + w]], axis=0)

        def write(s, w, val):
            merged = jnp.where(valid, val.astype(F32), read(s, w).astype(F32)).astype(BF16)
            gr_v[m_a, pl.ds(base_a, ra), s:s + w] = merged[:ra]

            @pl.when(n_b > 0)
            def _():
                gr_v[1 - m_a, pl.ds(base_b, rb), s:s + w] = merged[ra:]

        lane = lax.broadcasted_iota(jnp.int32, (rows, LANES), 1)
        meta = jnp.where(valid, read(2 * dm, LANES).astype(F32), 0.0)
        eid = (me * el + e).astype(F32)
        mine = ((meta == eid) & (lane < top_k)).astype(F32)
        sel = pltpu.roll(mine, 8, 1) + pltpu.roll(mine, 16, 1) + pltpu.roll(mine, 24, 1)
        gate = jnp.where(valid, jnp.sum(meta * sel, axis=1, keepdims=True), 0.0)
        for s, w in col_blocks(dm, 256):
            xt_v[:rows, s:s + w] = jnp.where(valid, read(s, w).astype(F32), 0.0).astype(BF16)
            dy = jnp.where(valid, read(dm + s, w).astype(F32), 0.0)
            qt_v[:rows, s:s + w] = (gate * dy).astype(BF16)
        xt = xt_v[:rows, :]
        u = dot_nn(xt, wg_v[slot]).astype(BF16).astype(F32)
        v = dot_nn(xt, wu_v[slot]).astype(BF16).astype(F32)
        r = dot_nt(qt_v[:rows, :], wd_v[slot])
        s_g = jax.nn.sigmoid(u)
        a_v[:rows, :] = (u * s_g * v).astype(BF16)
        duv_v[:rows, :ff] = (r * v * s_g * (1.0 + u * (1.0 - s_g))).astype(BF16)
        duv_v[:rows, ff:] = (r * u * s_g).astype(BF16)
        a = a_v[:rows, :]
        du = duv_v[:rows, :ff]
        dv = duv_v[:rows, ff:]
        dots = jnp.zeros((rows, 1), F32)
        for s, w in col_blocks(dm, 256):
            o = dot_nn(a, wd_v[slot, :, s:s + w]).astype(BF16)
            dy = jnp.where(valid, read(dm + s, w).astype(F32), 0.0)
            dots = dots + jnp.sum(dy * o.astype(F32), axis=1, keepdims=True)
            write(s, w, o)
        for s, w in col_blocks(dm, 256):
            p = dot_nt(du, wg_v[slot, s:s + w, :]) + dot_nt(dv, wu_v[slot, s:s + w, :])
            write(dm + s, w, p.astype(BF16))
        d1, d2, d3 = split3(dots)
        g1, g2, g3 = split3(gate)
        new_meta = jnp.zeros((rows, LANES), F32)
        for at, val in ((e, d1), (8 + e, d2), (16 + e, d3), (32, g1), (33, g2), (34, g3)):
            new_meta = jnp.where(lane == at, val.astype(F32), new_meta)
        write(2 * dm, LANES, new_meta)

        def put(ref, idx, val):
            if first is None:
                ref[idx] = val
            else:
                ref[idx] = jnp.where(first, 0.0, ref[idx]) + val

        duv = duv_v[:rows, :]
        for s, w in col_blocks(dm, 256):
            g_in = dot_tn(xt_v[:rows, s:s + w], duv)
            put(og_v, (slot, slice(s, s + w)), g_in[:, :ff])
            put(ou_v, (slot, slice(s, s + w)), g_in[:, ff:])
        for s, w in col_blocks(dm, 256):
            put(od_v, (slot, slice(None), slice(s, s + w)), dot_tn(a, qt_v[:rows, s:s + w]))

    def expert(e, carry):
        slot = lax.rem(e, 2)
        for c in load_w(e, slot):
            c.wait()

        @pl.when(e >= 2)
        def _():
            for c in store_g(e - 2, slot):
                c.wait()

        n0, n1 = cnt_s[0, e], cnt_s[1, e]
        big0, big1 = n0 > SMALL, n1 > SMALL

        @pl.when(jnp.logical_not(big0 | big1))
        def _():
            tile(e, slot, SMALL, SMALL, 0, n0, n1, None)

        @pl.when(big0 | big1)
        def _():
            both = big0 & big1

            def one(i, inner):
                m_a = jnp.where(both, i, jnp.where(big0, 0, 1))
                n_a = jnp.where(m_a == 0, n0, n1)
                n_b = jnp.where(both, 0, jnp.where(m_a == 0, n1, n0))
                tile(e, slot, seg, SMALL, m_a, n_a, n_b, i == 0)
                return inner

            lax.fori_loop(0, jnp.where(both, 2, 1), one, 0)

        for c in store_g(e, slot):
            c.start()

        @pl.when(e + 2 < el)
        def _():
            for c in load_w(e + 2, slot):
                c.start()

        return carry

    lax.fori_loop(0, el, expert, 0)

    for m in range(2):
        def scatter(c, carry, m=m):
            off = pl.multiple_of(c * seg, seg)
            rows = pl.ds(off, seg)
            first = c == 0
            pt = pt_v[m, :, rows]
            gp = gr_v[m, rows, 2 * dm:].astype(F32)
            gate = gp[:, 32:33] + gp[:, 33:34] + gp[:, 34:35]
            for s, w in col_blocks(dm, 256):
                h1, h2, h3 = split3(gate * gr_v[m, rows, s:s + w].astype(F32))
                add = dot_nn(pt, h1) + dot_nn(pt, h2) + dot_nn(pt, h3)
                acc_v[m, :, s:s + w] = jnp.where(first, 0.0, acc_v[m, :, s:s + w]) + add
            for s, w in col_blocks(dm + LANES, 256):
                lo = dm + s
                add = dot_nn(pt, gr_v[m, rows, lo:lo + w])
                acc_v[m, :, lo:lo + w] = jnp.where(first, 0.0, acc_v[m, :, lo:lo + w]) + add
            return carry

        lax.fori_loop(0, n_chunks[m], scatter, 0)
        lane = lax.broadcasted_iota(jnp.int32, (tokens, LANES), 1)
        ids = jnp.where(lane < top_k, xd_v[m, :, 2 * dm:].astype(F32), -1.0)
        raw = acc_v[m, :, 2 * dm:]
        out = jnp.zeros((tokens, LANES), F32)
        for e in range(el):
            val = raw[:, e:e + 1] + raw[:, 8 + e:9 + e] + raw[:, 16 + e:17 + e]
            out = jnp.where(ids == (me * el + e).astype(F32), val, out)
        acc_v[m, :, 2 * dm:] = out
        pltpu.make_async_copy(acc_v.at[m], part_hbm.at[m], sem_p.at[m]).start()

    for e in range(el - 2, el):
        for c in store_g(e, e % 2):
            c.wait()
    for m in range(2):
        pltpu.make_async_copy(acc_v.at[m], part_hbm.at[m], sem_p.at[m]).wait()


def expert_stage(xd, w_gate, w_up, w_down, top_k, seg):
    _, tokens, width = xd.shape
    el, dm, ff = w_gate.shape
    any_spec = pl.BlockSpec(memory_space=pltpu.HBM)
    rows_max = el * seg
    tile_rows = seg + SMALL
    dims = (tokens, dm, ff, el, top_k, seg)
    return pl.pallas_call(
        functools.partial(expert_kernel, dims),
        out_shape=(
            jax.ShapeDtypeStruct((2, tokens, width), F32),
            jax.ShapeDtypeStruct((el, dm, ff), F32),
            jax.ShapeDtypeStruct((el, dm, ff), F32),
            jax.ShapeDtypeStruct((el, ff, dm), F32),
        ),
        in_specs=[any_spec] * 4,
        out_specs=[any_spec] * 4,
        scratch_shapes=[
            pltpu.VMEM((2, tokens, width), BF16),
            pltpu.VMEM((2, tokens, rows_max), BF16),
            pltpu.VMEM((2, rows_max, width), BF16),
            pltpu.VMEM((2, tokens, width), F32),
            pltpu.VMEM((2, dm, ff), BF16),
            pltpu.VMEM((2, dm, ff), BF16),
            pltpu.VMEM((2, ff, dm), BF16),
            pltpu.VMEM((2, dm, ff), F32),
            pltpu.VMEM((2, dm, ff), F32),
            pltpu.VMEM((2, ff, dm), F32),
            pltpu.VMEM((2, 8, tokens), F32),
            pltpu.VMEM((tile_rows, dm), BF16),
            pltpu.VMEM((tile_rows, dm), BF16),
            pltpu.VMEM((tile_rows, ff), BF16),
            pltpu.VMEM((tile_rows, 2 * ff), BF16),
            pltpu.SMEM((2, 8), jnp.int32),
            pltpu.SMEM((2, 8), jnp.int32),
            pltpu.SemaphoreType.DMA((2,)),
            pltpu.SemaphoreType.DMA((2, 3)),
            pltpu.SemaphoreType.DMA((2, 3)),
            pltpu.SemaphoreType.DMA((2,)),
        ],
        compiler_params=pltpu.CompilerParams(vmem_limit_bytes=VMEM_LIMIT),
        name="experts",
    )(xd, w_gate, w_up, w_down)


RING = 4
NEAR = (0, -1, 1, 2)
FAR = (2, -1, 1, 0)
GROUPS = (slice(0, 1), slice(1, 3), slice(3, 4))
MESH = pl.DeviceIdType.MESH


class Place:
    def __init__(self):
        self.row, self.col, self.core = (lax.axis_index(a) for a in GROUP_AXES)
        self.n_row, self.n_col = lax.axis_size("row"), lax.axis_size("col")
        self.other = 1 - self.core
        self.partner = {"core": self.other}

    def spot(self, first, d1, d2):
        row = lax.rem(self.row + (d1 * first + d2 * (1 - first)) + self.n_row, self.n_row)
        col = lax.rem(self.col + (d1 * (1 - first) + d2 * first) + self.n_col, self.n_col)
        return row, col

    def chip(self, first, d1, d2):
        row, col = self.spot(first, d1, d2)
        return row * self.n_col + col

    def peer(self, axis, d):
        row, col = self.spot(self.core, d, 0) if axis == 1 else self.spot(self.core, 0, d)
        return {"row": row, "col": col}

    def barrier(self):
        sem = pltpu.get_barrier_semaphore()
        peers = [self.peer(axis, d) for axis in (1, 2) for d in (1, -1)] + [self.partner]
        for peer in peers:
            pl.semaphore_signal(sem, inc=1, device_id=peer, device_id_type=MESH)
        pl.semaphore_wait(sem, len(peers))


def half_lanes(width):
    mid = (width // LANES + 1) // 2 * LANES
    return (pl.ds(0, mid), pl.ds(mid, width - mid))


def token_meta(route, gates):
    top_k, tok_dev = route.shape
    zero = jnp.zeros((8 - top_k, tok_dev), F32)
    parts = [route.astype(F32)] + [p.astype(F32) for p in split3(gates)]
    rows = jnp.concatenate([v for p in parts for v in (p, zero)], axis=0).astype(BF16)
    n = rows.shape[0]
    eye = (lax.broadcasted_iota(jnp.int32, (n, LANES), 0) == lax.broadcasted_iota(jnp.int32, (n, LANES), 1)).astype(F32).astype(BF16)
    return dot_tn(rows, eye).astype(BF16)


def gather_kernel(x_hbm, dy_hbm, route_ref, gates_ref, out_hbm, buf, stage, send_sem, recv_sem, load_sem, out_sem):
    here = Place()
    k, other = here.core, here.other
    dm = x_hbm.shape[2]
    halves = half_lanes(2 * dm + LANES)
    sent = []

    def move(idx, src, dst, peer):
        return pltpu.make_async_remote_copy(src_ref=src, dst_ref=dst, send_sem=send_sem.at[idx], recv_sem=recv_sem.at[idx],
                                            device_id=peer, device_id_type=MESH)

    def send(idx, src, dst, peer):
        c = move(idx, src, dst, peer)
        c.start()
        sent.append(c)

    def arrive(idx, dst):
        move(idx, dst, dst, here.partner).wait_recv()

    def keep(mine, g, d):
        first = k if mine else other
        for i in range(g.start, g.stop):
            c = here.chip(first, NEAR[i], NEAR[d])
            pltpu.make_async_copy(buf.at[0 if mine else 1, d, i], out_hbm.at[first, c], out_sem.at[0 if mine else 1]).start()

    def have(gi, d):
        g = GROUPS[gi]
        send(17 + 3 * d + gi, buf.at[0, d, g], buf.at[1, d, g], here.partner)
        keep(True, g, d)

    def spread(gi):
        g = GROUPS[gi]
        send(5 + 4 * gi, buf.at[0, 0, g], buf.at[0, 1, g], here.peer(2, 1))
        send(6 + 4 * gi, buf.at[0, 0, g], buf.at[0, 2, g], here.peer(2, -1))
        have(gi, 0)

    def second(gi):
        g = GROUPS[gi]
        for d, step in ((1, 1), (2, -1)):
            arrive(4 + 4 * gi + d, buf.at[0, d, g])
            lanes = halves[d - 1]
            send(6 + 4 * gi + d, buf.at[0, d, g, :, :, lanes], buf.at[0, 3, g, :, :, lanes], here.peer(2, step))
            have(gi, d)

    def second_far(gi):
        g = GROUPS[gi]
        for d in (1, 2):
            arrive(6 + 4 * gi + d, buf.at[0, 3, g, :, :, halves[d - 1]])
        have(gi, 3)

    mine = buf.at[0, 0, 0, k]
    loads = [pltpu.make_async_copy(h.at[mb], dst.at[:, pl.ds(lo, dm)], load_sem.at[n])
             for n, (h, mb, dst, lo) in enumerate(((x_hbm, other, stage, 0), (dy_hbm, other, stage, dm), (x_hbm, k, mine, 0), (dy_hbm, k, mine, dm)))]
    for c in loads:
        c.start()
    metas = [token_meta(route_ref[:, m, :], gates_ref[:, m, :]) for m in range(2)]
    zero_core = k == 0
    stage[:, 2 * dm:] = jnp.where(zero_core, metas[1].astype(F32), metas[0].astype(F32)).astype(BF16)
    buf[0, 0, 0, k, :, 2 * dm:] = jnp.where(zero_core, metas[0].astype(F32), metas[1].astype(F32)).astype(BF16)
    here.barrier()
    for c in loads:
        c.wait()
    send(0, stage, buf.at[0, 0, 0, k], here.partner)
    arrive(0, buf.at[0, 0, 0, other])
    send(1, buf.at[0, 0, 0], buf.at[0, 0, 1], here.peer(1, 1))
    send(2, buf.at[0, 0, 0], buf.at[0, 0, 2], here.peer(1, -1))
    spread(0)
    arrive(1, buf.at[0, 0, 1])
    send(3, buf.at[0, 0, 1, :, :, halves[0]], buf.at[0, 0, 3, :, :, halves[0]], here.peer(1, 1))
    arrive(2, buf.at[0, 0, 2])
    send(4, buf.at[0, 0, 2, :, :, halves[1]], buf.at[0, 0, 3, :, :, halves[1]], here.peer(1, -1))
    spread(1)
    second(0)
    arrive(3, buf.at[0, 0, 3, :, :, halves[0]])
    arrive(4, buf.at[0, 0, 3, :, :, halves[1]])
    spread(2)
    second(1)
    second_far(0)
    second(2)
    second_far(1)
    second_far(2)
    for gi, d in [(gi, d) for d in range(RING) for gi in range(len(GROUPS))]:
        arrive(17 + 3 * d + gi, buf.at[1, d, GROUPS[gi]])
        keep(False, GROUPS[gi], d)
    for c in sent:
        c.wait_send()
    for n, mb in enumerate((k, other)):
        pltpu.make_async_copy(out_hbm.at[mb], out_hbm.at[mb], out_sem.at[n]).wait()


def gather_tokens(x, grad_y, route_idx, gates, chips):
    _, tok_dev, dm = x.shape
    width = 2 * dm + LANES
    hbm = pl.BlockSpec(memory_space=pltpu.HBM)
    vmem = pl.BlockSpec(memory_space=pltpu.VMEM)
    sems = pltpu.SemaphoreType.DMA((29,))
    return pl.pallas_call(
        gather_kernel,
        out_shape=jax.ShapeDtypeStruct((2, chips, 2, tok_dev, width), BF16),
        in_specs=[hbm, hbm, vmem, vmem],
        out_specs=hbm,
        scratch_shapes=[pltpu.VMEM((2, RING, RING, 2, tok_dev, width), BF16), pltpu.VMEM((tok_dev, width), BF16),
                        sems, sems, pltpu.SemaphoreType.DMA((4,)), pltpu.SemaphoreType.DMA((2,))],
        compiler_params=pltpu.CompilerParams(collective_id=0, has_side_effects=True, vmem_limit_bytes=VMEM_LIMIT),
        name="gather_tokens",
    )(x, grad_y, jnp.transpose(route_idx, (2, 0, 1)), jnp.transpose(gates, (2, 0, 1)))


def reduce_kernel(dm, top_k, part_hbm, y_ref, dx_ref, dg_ref, own, pair, full, half, last, load_sem, pair_send, pair_recv,
                  ring_send, ring_recv, last_sem):
    here = Place()
    k, other = here.core, here.other
    halves = half_lanes(part_hbm.shape[4])
    sent = []

    def load(d, i):
        return pltpu.make_async_copy(part_hbm.at[k, here.chip(k, FAR[i], FAR[d])], own.at[d, i], load_sem.at[d, i])

    def swap(d, i):
        return pltpu.make_async_remote_copy(src_ref=part_hbm.at[other, here.chip(other, FAR[i], FAR[d])], dst_ref=pair.at[d, i],
                                            send_sem=pair_send.at[d, i], recv_sem=pair_recv.at[d, i], device_id=here.partner, device_id_type=MESH)

    def move(f, kind, src, dst, axis):
        return pltpu.make_async_remote_copy(src_ref=src, dst_ref=dst, send_sem=ring_send.at[f, kind], recv_sem=ring_recv.at[f, kind],
                                            device_id=here.peer(axis, 1 if kind % 2 == 0 else -1), device_id_type=MESH)

    def go(f, kind, src, dst, axis):
        c = move(f, kind, src, dst, axis)
        c.start()
        sent.append(c)

    def arrive(f, kind, dst):
        move(f, kind, dst, dst, 1).wait_recv()

    def add_pair(d, gi):
        for i in range(GROUPS[gi].start, GROUPS[gi].stop):
            load(d, i).wait()
            swap(d, i).wait_recv()
            own[d, i] = own[d, i] + pair[d, i]

    def far(f, src, g, axis):
        for kind in range(2):
            go(f, kind, src.at[:, :, :, halves[kind]], half.at[g, :, :, halves[kind]], axis)

    def near(f, ref, g, axis):
        for kind, step in ((0, 1), (1, -1)):
            lanes = halves[kind]
            arrive(f, kind, half.at[g, :, :, lanes])
            d, at = ref(step)
            own[d, at, :, :, lanes] = own[d, at, :, :, lanes] + half[g, :, :, lanes]
        for kind, step in ((2, 1), (3, -1)):
            d, at = ref(step)
            go(f, kind, own.at[d, at], full.at[kind - 2, g], axis)

    def done(f, at, g):
        arrive(f, 2, full.at[0, g])
        arrive(f, 3, full.at[1, g])
        own[3, at] = own[3, at] + full[0, g] + full[1, g]

    def far2(gi):
        add_pair(0, gi)
        far(gi, own.at[0, GROUPS[gi]], GROUPS[gi], 2)

    def near2(gi):
        add_pair(2, gi)
        add_pair(1, gi)
        near(gi, lambda step: (2 if step == 1 else 1, GROUPS[gi]), GROUPS[gi], 2)

    def done2(gi):
        add_pair(3, gi)
        done(gi, GROUPS[gi], GROUPS[gi])

    order = [(0, 0), (0, 1), (0, 2), (2, 0), (1, 0), (0, 3), (2, 1), (2, 2), (1, 1), (1, 2), (3, 0), (2, 3), (1, 3), (3, 1), (3, 2), (3, 3)]
    for q in order:
        load(*q).start()
    here.barrier()
    for q in order:
        c = swap(*q)
        c.start()
        sent.append(c)
    lone = slice(RING, RING + 1)
    far2(0)
    far2(1)
    near2(0)
    far2(2)
    near2(1)
    done2(0)
    far(3, own.at[3, slice(0, 1)], lone, 1)
    near2(2)
    done2(1)
    near(3, lambda step: (3, slice(2, 3) if step == 1 else slice(1, 2)), lone, 1)
    done2(2)
    done(3, slice(3, 4), lone)

    give = pltpu.make_async_remote_copy(src_ref=own.at[3, 3, other], dst_ref=last, send_sem=last_sem.at[0], recv_sem=last_sem.at[1],
                                        device_id=here.partner, device_id_type=MESH)
    give.start()
    sent.append(give)

    def emit(mb, val):
        y_ref[mb] = val[:, :dm].astype(BF16)
        dx_ref[mb] = val[:, dm:2 * dm].astype(BF16)
        dg_ref[mb] = val[:, 2 * dm:2 * dm + top_k]

    emit(k, own[3, 3, k])
    give.wait_recv()
    emit(other, last[...])
    for c in sent:
        c.wait_send()


def reduce_tokens(part, dm, top_k):
    _, chips, cores, tok_dev, width = part.shape
    vmem = pl.BlockSpec(memory_space=pltpu.VMEM)
    block = (cores, tok_dev, width)
    ring_sems = pltpu.SemaphoreType.DMA((4, 4))
    pair_sems = pltpu.SemaphoreType.DMA((RING, RING))
    return pl.pallas_call(
        functools.partial(reduce_kernel, dm, top_k),
        out_shape=(
            jax.ShapeDtypeStruct((2, tok_dev, dm), BF16),
            jax.ShapeDtypeStruct((2, tok_dev, dm), BF16),
            jax.ShapeDtypeStruct((2, tok_dev, top_k), F32),
        ),
        in_specs=[pl.BlockSpec(memory_space=pltpu.HBM)],
        out_specs=(vmem, vmem, vmem),
        scratch_shapes=[
            pltpu.VMEM((RING, RING) + block, F32),
            pltpu.VMEM((RING, RING) + block, F32),
            pltpu.VMEM((2, RING + 1) + block, F32),
            pltpu.VMEM((RING + 1,) + block, F32),
            pltpu.VMEM((tok_dev, width), F32),
            pair_sems, pair_sems, pair_sems, ring_sems, ring_sems,
            pltpu.SemaphoreType.DMA((2,)),
        ],
        compiler_params=pltpu.CompilerParams(collective_id=1, has_side_effects=True, vmem_limit_bytes=VMEM_LIMIT),
        name="reduce_tokens",
    )(part)


def solution(mesh):
    group = mesh.shape["row"] * mesh.shape["col"] * mesh.shape["core"]
    tok_spec = P(None, ALL_AXES, None)
    w_spec = P(ALL_AXES, None, None)

    def moe_layer(x, route_idx, gates, w_gate, w_up, w_down, grad_y):
        _, tok_dev, dm = x.shape
        top_k = route_idx.shape[2]
        width = 2 * dm + LANES
        chips = group // 2
        xd = gather_tokens(x, grad_y, route_idx, gates, chips).reshape(2, group * tok_dev, width)
        part, g_gate, g_up, g_down = expert_stage(xd, w_gate, w_up, w_down, top_k, group * (tok_dev // 2))
        y, dx, dg = reduce_tokens(part.reshape(2, chips, 2, tok_dev, width), dm, top_k)
        return y, dx, dg, g_gate, g_up, g_down

    return jax.shard_map(moe_layer, mesh=mesh, in_specs=(tok_spec, tok_spec, tok_spec, w_spec, w_spec, w_spec, tok_spec), out_specs=(tok_spec, tok_spec, tok_spec, w_spec, w_spec, w_spec), check_vma=False)
```

```python
import functools

import jax
import jax.numpy as jnp
from jax import lax
from jax.experimental import pallas as pl
from jax.experimental.pallas import tpu as pltpu
from jax.sharding import PartitionSpec as P

GROUP_AXES = ("row", "col", "core")
ALL_AXES = ("rep", "row", "col", "core")
F32 = jnp.float32
BF16 = jnp.bfloat16
LANES = 128
SMALL = 32
VMEM_LIMIT = 66_000_000


def dot_nn(a, b):
    return lax.dot_general(a, b, (((1,), (0,)), ((), ())), preferred_element_type=F32)


def dot_nt(a, b):
    return lax.dot_general(a, b, (((1,), (1,)), ((), ())), preferred_element_type=F32)


def dot_tn(a, b):
    return lax.dot_general(a, b, (((0,), (0,)), ((), ())), preferred_element_type=F32)


def split3(v):
    h1 = v.astype(BF16)
    r1 = v - h1.astype(F32)
    h2 = r1.astype(BF16)
    h3 = (r1 - h2.astype(F32)).astype(BF16)
    return h1, h2, h3


def col_blocks(width, step):
    return [(s, min(step, width - s)) for s in range(0, width, step)]


def expert_kernel(dims, xd_hbm, wg_hbm, wu_hbm, wd_hbm, part_hbm, gg_hbm, gu_hbm, gd_hbm,
                  xd_v, pt_v, gr_v, acc_v, wgu_v, wd_v, og_v, ou_v, od_v, pos_v,
                  xt_v, qt_v, a_v, duv_v, cnt_s, base_s, sem_x, sem_w, sem_o, sem_p):
    tokens, dm, ff, el, top_k, seg = dims
    n_row, n_col, n_core = lax.axis_size("row"), lax.axis_size("col"), lax.axis_size("core")
    me = (lax.axis_index("row") * n_col + lax.axis_index("col")) * n_core + lax.axis_index("core")
    width = 2 * dm + LANES

    def load_w(e, slot):
        pairs = ((wg_hbm, wgu_v.at[slot, :, pl.ds(0, ff)]), (wu_hbm, wgu_v.at[slot, :, pl.ds(ff, ff)]), (wd_hbm, wd_v.at[slot]))
        return [pltpu.make_async_copy(h.at[e], v, sem_w.at[slot, i]) for i, (h, v) in enumerate(pairs)]

    def store_g(e, slot):
        return [pltpu.make_async_copy(v.at[slot], h.at[e], sem_o.at[slot, i])
                for i, (h, v) in enumerate(((gg_hbm, og_v), (gu_hbm, ou_v), (gd_hbm, od_v)))]

    loads_x = [pltpu.make_async_copy(xd_hbm.at[m], xd_v.at[m], sem_x.at[m]) for m in range(2)]
    for c in loads_x:
        c.start()

    row_i = lax.broadcasted_iota(jnp.int32, (tokens, tokens), 0)
    col_i = lax.broadcasted_iota(jnp.int32, (tokens, tokens), 1)
    tri = (row_i < col_i).astype(F32).astype(BF16)
    sub = lax.broadcasted_iota(jnp.int32, (8, tokens), 0)
    eids = jnp.where(sub < el, (me * el + sub), -1).astype(F32)

    def chunks(total):
        return jnp.maximum((total + (seg - 1)) // seg, 1)

    n_chunks = []
    for m in range(2):
        loads_x[m].wait()
        for c in load_w(m, m):
            c.start()
        meta_t = xd_v[m, :, 2 * dm:].astype(F32).T
        hits = jnp.zeros((8, tokens), F32)
        for j in range(top_k):
            hits = hits + (meta_t[j:j + 1, :] == eids).astype(F32)
        rank = dot_nn(hits.astype(BF16), tri)
        total = jnp.int32(0)
        for e in range(el):
            cnt = jnp.sum(hits[e:e + 1, :]).astype(jnp.int32)
            cnt_s[m, e] = cnt
            base_s[m, e] = total
            pos_v[m, e:e + 1, :] = jnp.where(hits[e:e + 1, :] > 0, rank[e:e + 1, :] + total.astype(F32), -1.0)
            total = total + (cnt + 15) // 16 * 16
        n_ch = chunks(total)
        n_chunks.append(n_ch)

        def gather(c, carry, m=m):
            off = pl.multiple_of(c * seg, seg)
            rows = (lax.broadcasted_iota(jnp.int32, (seg, tokens), 0) + off).astype(F32)
            pick = rows == pos_v[m, 0:1, :]
            for e in range(1, el):
                pick = pick | (rows == pos_v[m, e:e + 1, :])
            pick_f = pick.astype(F32)
            pt_v[m, :, pl.ds(off, seg)] = pick_f.T.astype(BF16)
            pick_b = pick_f.astype(BF16)
            for s, w in col_blocks(width, 512):
                gr_v[m, pl.ds(off, seg), s:s + w] = dot_nn(pick_b, xd_v[m, :, s:s + w]).astype(BF16)
            return carry

        lax.fori_loop(0, n_ch, gather, 0)

    def tile(e, slot, ra, rb, m_a, n_a, n_b, first):
        rows = ra + rb
        base_a = pl.multiple_of(base_s[m_a, e], 16)
        base_b = pl.multiple_of(base_s[1 - m_a, e], 16)
        it = lax.broadcasted_iota(jnp.int32, (rows, 1), 0)
        valid = ((it < ra) & (it < n_a)) | ((it >= ra) & (it - ra < n_b))

        def read(s, w):
            return jnp.concatenate([gr_v[m_a, pl.ds(base_a, ra), s:s + w],
                                    gr_v[1 - m_a, pl.ds(base_b, rb), s:s + w]], axis=0)

        def write(s, w, val):
            merged = jnp.where(valid, val.astype(F32), read(s, w).astype(F32)).astype(BF16)
            gr_v[m_a, pl.ds(base_a, ra), s:s + w] = merged[:ra]
            gr_v[1 - m_a, pl.ds(base_b, rb), s:s + w] = merged[ra:]

        lane = lax.broadcasted_iota(jnp.int32, (rows, LANES), 1)
        meta = jnp.where(valid, read(2 * dm, LANES).astype(F32), 0.0)
        eid = (me * el + e).astype(F32)
        mine = ((meta == eid) & (lane < top_k)).astype(F32)
        sel = pltpu.roll(mine, 8, 1) + pltpu.roll(mine, 16, 1) + pltpu.roll(mine, 24, 1)
        gate = jnp.where(valid, jnp.sum(meta * sel, axis=1, keepdims=True), 0.0)
        for s, w in col_blocks(dm, 256):
            xt_v[:rows, s:s + w] = jnp.where(valid, read(s, w).astype(F32), 0.0).astype(BF16)
            dy = jnp.where(valid, read(dm + s, w).astype(F32), 0.0)
            qt_v[:rows, s:s + w] = (gate * dy).astype(BF16)
        xt = xt_v[:rows, :]
        uv = dot_nn(xt, wgu_v[slot]).astype(BF16).astype(F32)
        u, v = uv[:, :ff], uv[:, ff:]
        r = dot_nt(qt_v[:rows, :], wd_v[slot])
        s_g = jax.nn.sigmoid(u)
        a_v[:rows, :] = (u * s_g * v).astype(BF16)
        duv_v[:rows, :ff] = (r * v * s_g * (1.0 + u * (1.0 - s_g))).astype(BF16)
        duv_v[:rows, ff:] = (r * u * s_g).astype(BF16)
        a = a_v[:rows, :]
        duv = duv_v[:rows, :]
        dots = jnp.zeros((rows, 1), F32)
        for s, w in col_blocks(dm, 256):
            o = dot_nn(a, wd_v[slot, :, s:s + w]).astype(BF16)
            dy = jnp.where(valid, read(dm + s, w).astype(F32), 0.0)
            dots = dots + jnp.sum(dy * o.astype(F32), axis=1, keepdims=True)
            write(s, w, o)
        for s, w in col_blocks(dm, 256):
            write(dm + s, w, dot_nt(duv, wgu_v[slot, s:s + w, :]).astype(BF16))
        d1, d2, d3 = split3(dots)
        g1, g2, g3 = split3(gate)
        new_meta = jnp.zeros((rows, LANES), F32)
        for at, val in ((e, d1), (8 + e, d2), (16 + e, d3), (32, g1), (33, g2), (34, g3)):
            new_meta = jnp.where(lane == at, val.astype(F32), new_meta)
        write(2 * dm, LANES, new_meta)

        def put(ref, idx, val):
            if first is None:
                ref[idx] = val
            else:
                ref[idx] = jnp.where(first, 0.0, ref[idx]) + val

        for s, w in col_blocks(dm, 256):
            g_in = dot_tn(xt_v[:rows, s:s + w], duv)
            put(og_v, (slot, slice(s, s + w)), g_in[:, :ff])
            put(ou_v, (slot, slice(s, s + w)), g_in[:, ff:])
        for s, w in col_blocks(dm, 256):
            put(od_v, (slot, slice(None), slice(s, s + w)), dot_tn(a, qt_v[:rows, s:s + w]))

    def expert(e, carry):
        slot = lax.rem(e, 2)
        for c in load_w(e, slot):
            c.wait()

        @pl.when(e >= 2)
        def _():
            for c in store_g(e - 2, slot):
                c.wait()

        n0, n1 = cnt_s[0, e], cnt_s[1, e]
        big0, big1 = n0 > SMALL, n1 > SMALL

        @pl.when(jnp.logical_not(big0 | big1))
        def _():
            tile(e, slot, SMALL, SMALL, 0, n0, n1, None)

        @pl.when(big0 | big1)
        def _():
            both = big0 & big1

            def one(i, inner):
                m_a = jnp.where(both, i, jnp.where(big0, 0, 1))
                n_a = jnp.where(m_a == 0, n0, n1)
                n_b = jnp.where(both, 0, jnp.where(m_a == 0, n1, n0))
                tile(e, slot, seg, SMALL, m_a, n_a, n_b, i == 0)
                return inner

            lax.fori_loop(0, jnp.where(both, 2, 1), one, 0)

        for c in store_g(e, slot):
            c.start()

        @pl.when(e + 2 < el)
        def _():
            for c in load_w(e + 2, slot):
                c.start()

        return carry

    lax.fori_loop(0, el, expert, 0)

    for m in range(2):
        def scatter(c, carry, m=m):
            off = pl.multiple_of(c * seg, seg)
            rows = pl.ds(off, seg)
            first = c == 0
            pt = pt_v[m, :, rows]
            gp = gr_v[m, rows, 2 * dm:].astype(F32)
            gate = gp[:, 32:33] + gp[:, 33:34] + gp[:, 34:35]
            for s, w in col_blocks(dm, 256):
                h1, h2, h3 = split3(gate * gr_v[m, rows, s:s + w].astype(F32))
                add = dot_nn(pt, h1) + dot_nn(pt, h2) + dot_nn(pt, h3)
                acc_v[m, :, s:s + w] = jnp.where(first, 0.0, acc_v[m, :, s:s + w]) + add
            for s, w in col_blocks(dm + LANES, 256):
                lo = dm + s
                add = dot_nn(pt, gr_v[m, rows, lo:lo + w])
                acc_v[m, :, lo:lo + w] = jnp.where(first, 0.0, acc_v[m, :, lo:lo + w]) + add
            return carry

        lax.fori_loop(0, n_chunks[m], scatter, 0)
        lane = lax.broadcasted_iota(jnp.int32, (tokens, LANES), 1)
        ids = jnp.where(lane < top_k, xd_v[m, :, 2 * dm:].astype(F32), -1.0)
        raw = acc_v[m, :, 2 * dm:]
        out = jnp.zeros((tokens, LANES), F32)
        for e in range(el):
            val = raw[:, e:e + 1] + raw[:, 8 + e:9 + e] + raw[:, 16 + e:17 + e]
            out = jnp.where(ids == (me * el + e).astype(F32), val, out)
        acc_v[m, :, 2 * dm:] = out
        pltpu.make_async_copy(acc_v.at[m], part_hbm.at[m], sem_p.at[m]).start()

    for e in range(el - 2, el):
        for c in store_g(e, e % 2):
            c.wait()
    for m in range(2):
        pltpu.make_async_copy(acc_v.at[m], part_hbm.at[m], sem_p.at[m]).wait()


def expert_stage(xd, w_gate, w_up, w_down, top_k, seg):
    _, tokens, width = xd.shape
    el, dm, ff = w_gate.shape
    any_spec = pl.BlockSpec(memory_space=pltpu.HBM)
    rows_max = el * seg
    tile_rows = seg + SMALL
    dims = (tokens, dm, ff, el, top_k, seg)
    return pl.pallas_call(
        functools.partial(expert_kernel, dims),
        out_shape=(
            jax.ShapeDtypeStruct((2, tokens, width), F32),
            jax.ShapeDtypeStruct((el, dm, ff), F32),
            jax.ShapeDtypeStruct((el, dm, ff), F32),
            jax.ShapeDtypeStruct((el, ff, dm), F32),
        ),
        in_specs=[any_spec] * 4,
        out_specs=[any_spec] * 4,
        scratch_shapes=[
            pltpu.VMEM((2, tokens, width), BF16),
            pltpu.VMEM((2, tokens, rows_max), BF16),
            pltpu.VMEM((2, rows_max, width), BF16),
            pltpu.VMEM((2, tokens, width), F32),
            pltpu.VMEM((2, dm, 2 * ff), BF16),
            pltpu.VMEM((2, ff, dm), BF16),
            pltpu.VMEM((2, dm, ff), F32),
            pltpu.VMEM((2, dm, ff), F32),
            pltpu.VMEM((2, ff, dm), F32),
            pltpu.VMEM((2, 8, tokens), F32),
            pltpu.VMEM((tile_rows, dm), BF16),
            pltpu.VMEM((tile_rows, dm), BF16),
            pltpu.VMEM((tile_rows, ff), BF16),
            pltpu.VMEM((tile_rows, 2 * ff), BF16),
            pltpu.SMEM((2, 8), jnp.int32),
            pltpu.SMEM((2, 8), jnp.int32),
            pltpu.SemaphoreType.DMA((2,)),
            pltpu.SemaphoreType.DMA((2, 3)),
            pltpu.SemaphoreType.DMA((2, 3)),
            pltpu.SemaphoreType.DMA((2,)),
        ],
        compiler_params=pltpu.CompilerParams(vmem_limit_bytes=VMEM_LIMIT),
        name="experts",
    )(xd, w_gate, w_up, w_down)


RING = 4
NEAR = (0, -1, 1, 2)
FAR = (2, -1, 1, 0)
GROUPS = (slice(0, 1), slice(1, 3), slice(3, 4))
MESH = pl.DeviceIdType.MESH


class Place:
    def __init__(self):
        self.row, self.col, self.core = (lax.axis_index(a) for a in GROUP_AXES)
        self.n_row, self.n_col = lax.axis_size("row"), lax.axis_size("col")
        self.other = 1 - self.core
        self.partner = {"core": self.other}

    def spot(self, first, d1, d2):
        row = lax.rem(self.row + (d1 * first + d2 * (1 - first)) + self.n_row, self.n_row)
        col = lax.rem(self.col + (d1 * (1 - first) + d2 * first) + self.n_col, self.n_col)
        return row, col

    def chip(self, first, d1, d2):
        row, col = self.spot(first, d1, d2)
        return row * self.n_col + col

    def peer(self, axis, d):
        row, col = self.spot(self.core, d, 0) if axis == 1 else self.spot(self.core, 0, d)
        return {"row": row, "col": col}

    def barrier(self):
        sem = pltpu.get_barrier_semaphore()
        peers = [self.peer(axis, d) for axis in (1, 2) for d in (1, -1)] + [self.partner]
        for peer in peers:
            pl.semaphore_signal(sem, inc=1, device_id=peer, device_id_type=MESH)
        pl.semaphore_wait(sem, len(peers))


def half_lanes(width):
    mid = (width // LANES + 1) // 2 * LANES
    return (pl.ds(0, mid), pl.ds(mid, width - mid))


def token_meta(route, gates):
    top_k, tok_dev = route.shape
    zero = jnp.zeros((8 - top_k, tok_dev), F32)
    parts = [route.astype(F32)] + [p.astype(F32) for p in split3(gates)]
    rows = jnp.concatenate([v for p in parts for v in (p, zero)], axis=0).astype(BF16)
    n = rows.shape[0]
    eye = (lax.broadcasted_iota(jnp.int32, (n, LANES), 0) == lax.broadcasted_iota(jnp.int32, (n, LANES), 1)).astype(F32).astype(BF16)
    return dot_tn(rows, eye).astype(BF16)


def gather_kernel(x_hbm, dy_hbm, route_ref, gates_ref, out_hbm, buf, stage, send_sem, recv_sem, load_sem, out_sem):
    here = Place()
    k, other = here.core, here.other
    dm = x_hbm.shape[2]
    halves = half_lanes(2 * dm + LANES)
    sent = []

    def move(idx, src, dst, peer):
        return pltpu.make_async_remote_copy(src_ref=src, dst_ref=dst, send_sem=send_sem.at[idx], recv_sem=recv_sem.at[idx],
                                            device_id=peer, device_id_type=MESH)

    def send(idx, src, dst, peer):
        c = move(idx, src, dst, peer)
        c.start()
        sent.append(c)

    def arrive(idx, dst):
        move(idx, dst, dst, here.partner).wait_recv()

    def keep(mine, g, d):
        first = k if mine else other
        for i in range(g.start, g.stop):
            c = here.chip(first, NEAR[i], NEAR[d])
            pltpu.make_async_copy(buf.at[0 if mine else 1, d, i], out_hbm.at[first, c], out_sem.at[0 if mine else 1]).start()

    def have(gi, d):
        g = GROUPS[gi]
        send(24 + 3 * d + gi, buf.at[0, d, g], buf.at[1, d, g], here.partner)
        keep(True, g, d)

    def both_ways(p, src, left, right, axis):
        for way, dst in ((0, left), (1, right)):
            for n in range(2):
                lanes = halves[way if n == 0 else 1 - way]
                send(6 * p + 2 * way + n, src.at[:, :, :, lanes], dst.at[:, :, :, lanes], here.peer(axis, 1 - 2 * way))

    def relay(p, left, right, far, axis):
        for way, src in ((0, left), (1, right)):
            lanes = halves[way]
            arrive(6 * p + 2 * way, src.at[:, :, :, lanes])
            send(6 * p + 4 + way, src.at[:, :, :, lanes], far.at[:, :, :, lanes], here.peer(axis, 1 - 2 * way))

    def rest(p, left, right):
        for way, src in ((0, left), (1, right)):
            arrive(6 * p + 2 * way + 1, src.at[:, :, :, halves[1 - way]])

    def far_end(p, far):
        for way in range(2):
            arrive(6 * p + 4 + way, far.at[:, :, :, halves[way]])

    first = [buf.at[0, 0, pl.ds(i, 1)] for i in range(RING)]
    second = [[buf.at[0, d, g] for d in range(RING)] for g in GROUPS]

    def spread(gi):
        both_ways(1 + gi, second[gi][0], second[gi][1], second[gi][2], 2)
        have(gi, 0)

    def second_relay(gi):
        relay(1 + gi, second[gi][1], second[gi][2], second[gi][3], 2)

    def second_rest(gi):
        rest(1 + gi, second[gi][1], second[gi][2])
        have(gi, 1)
        have(gi, 2)

    def second_far(gi):
        far_end(1 + gi, second[gi][3])
        have(gi, 3)

    mine = buf.at[0, 0, 0, k]
    loads = [pltpu.make_async_copy(h.at[mb], dst.at[:, pl.ds(lo, dm)], load_sem.at[n])
             for n, (h, mb, dst, lo) in enumerate(((x_hbm, other, stage, 0), (dy_hbm, other, stage, dm), (x_hbm, k, mine, 0), (dy_hbm, k, mine, dm)))]
    for c in loads:
        c.start()
    metas = [token_meta(route_ref[:, m, :], gates_ref[:, m, :]) for m in range(2)]
    zero_core = k == 0
    stage[:, 2 * dm:] = jnp.where(zero_core, metas[1].astype(F32), metas[0].astype(F32)).astype(BF16)
    buf[0, 0, 0, k, :, 2 * dm:] = jnp.where(zero_core, metas[0].astype(F32), metas[1].astype(F32)).astype(BF16)
    here.barrier()
    for c in loads:
        c.wait()
    send(36, stage, buf.at[0, 0, 0, k], here.partner)
    arrive(36, buf.at[0, 0, 0, other])
    both_ways(0, first[0], first[1], first[2], 1)
    spread(0)
    relay(0, first[1], first[2], first[3], 1)
    second_relay(0)
    rest(0, first[1], first[2])
    spread(1)
    second_rest(0)
    far_end(0, first[3])
    spread(2)
    second_relay(1)
    second_far(0)
    second_rest(1)
    second_relay(2)
    second_rest(2)
    second_far(1)
    second_far(2)
    for gi, d in [(gi, d) for d in range(RING) for gi in range(len(GROUPS))]:
        arrive(24 + 3 * d + gi, buf.at[1, d, GROUPS[gi]])
        keep(False, GROUPS[gi], d)
    for c in sent:
        c.wait_send()
    for n, mb in enumerate((k, other)):
        pltpu.make_async_copy(out_hbm.at[mb], out_hbm.at[mb], out_sem.at[n]).wait()


def gather_tokens(x, grad_y, route_idx, gates, chips):
    _, tok_dev, dm = x.shape
    width = 2 * dm + LANES
    hbm = pl.BlockSpec(memory_space=pltpu.HBM)
    vmem = pl.BlockSpec(memory_space=pltpu.VMEM)
    sems = pltpu.SemaphoreType.DMA((37,))
    return pl.pallas_call(
        gather_kernel,
        out_shape=jax.ShapeDtypeStruct((2, chips, 2, tok_dev, width), BF16),
        in_specs=[hbm, hbm, vmem, vmem],
        out_specs=hbm,
        scratch_shapes=[pltpu.VMEM((2, RING, RING, 2, tok_dev, width), BF16), pltpu.VMEM((tok_dev, width), BF16),
                        sems, sems, pltpu.SemaphoreType.DMA((4,)), pltpu.SemaphoreType.DMA((2,))],
        compiler_params=pltpu.CompilerParams(collective_id=0, has_side_effects=True, vmem_limit_bytes=VMEM_LIMIT),
        name="gather_tokens",
    )(x, grad_y, jnp.transpose(route_idx, (2, 0, 1)), jnp.transpose(gates, (2, 0, 1)))


def reduce_kernel(dm, top_k, part_hbm, y_ref, dx_ref, dg_ref, own, pair, full, half, last, load_sem, pair_send, pair_recv,
                  ring_send, ring_recv, last_sem):
    here = Place()
    k, other = here.core, here.other
    halves = half_lanes(part_hbm.shape[4])
    sent = []

    def load(d, i):
        return pltpu.make_async_copy(part_hbm.at[k, here.chip(k, FAR[i], FAR[d])], own.at[d, i], load_sem.at[d, i])

    def swap(d, i):
        return pltpu.make_async_remote_copy(src_ref=part_hbm.at[other, here.chip(other, FAR[i], FAR[d])], dst_ref=pair.at[d, i],
                                            send_sem=pair_send.at[d, i], recv_sem=pair_recv.at[d, i], device_id=here.partner, device_id_type=MESH)

    def move(f, kind, src, dst, axis):
        return pltpu.make_async_remote_copy(src_ref=src, dst_ref=dst, send_sem=ring_send.at[f, kind], recv_sem=ring_recv.at[f, kind],
                                            device_id=here.peer(axis, 1 if kind % 2 == 0 else -1), device_id_type=MESH)

    def go(f, kind, src, dst, axis):
        c = move(f, kind, src, dst, axis)
        c.start()
        sent.append(c)

    def arrive(f, kind, dst):
        move(f, kind, dst, dst, 1).wait_recv()

    def add_pair(d, gi):
        for i in range(GROUPS[gi].start, GROUPS[gi].stop):
            load(d, i).wait()
            swap(d, i).wait_recv()
            own[d, i] = own[d, i] + pair[d, i]

    def far(f, src, g, axis):
        for kind in range(2):
            go(f, kind, src.at[:, :, :, halves[kind]], half.at[g, :, :, halves[kind]], axis)

    def near(f, ref, g, axis):
        for kind, step in ((0, 1), (1, -1)):
            lanes = halves[kind]
            arrive(f, kind, half.at[g, :, :, lanes])
            d, at = ref(step)
            own[d, at, :, :, lanes] = own[d, at, :, :, lanes] + half[g, :, :, lanes]
        for kind, step in ((2, 1), (3, -1)):
            d, at = ref(step)
            go(f, kind, own.at[d, at], full.at[kind - 2, g], axis)

    def done(f, at, g):
        arrive(f, 2, full.at[0, g])
        arrive(f, 3, full.at[1, g])
        own[3, at] = own[3, at] + full[0, g] + full[1, g]

    def far2(gi):
        add_pair(0, gi)
        far(gi, own.at[0, GROUPS[gi]], GROUPS[gi], 2)

    def near2(gi):
        add_pair(2, gi)
        add_pair(1, gi)
        near(gi, lambda step: (2 if step == 1 else 1, GROUPS[gi]), GROUPS[gi], 2)

    def done2(gi):
        add_pair(3, gi)
        done(gi, GROUPS[gi], GROUPS[gi])

    order = [(0, 0), (0, 1), (0, 2), (2, 0), (1, 0), (0, 3), (2, 1), (2, 2), (1, 1), (1, 2), (3, 0), (2, 3), (1, 3), (3, 1), (3, 2), (3, 3)]
    for q in order:
        load(*q).start()
    here.barrier()
    for q in order:
        c = swap(*q)
        c.start()
        sent.append(c)
    lone = slice(RING, RING + 1)
    far2(0)
    far2(1)
    near2(0)
    far2(2)
    near2(1)
    done2(0)
    far(3, own.at[3, slice(0, 1)], lone, 1)
    near2(2)
    done2(1)
    near(3, lambda step: (3, slice(2, 3) if step == 1 else slice(1, 2)), lone, 1)
    done2(2)
    done(3, slice(3, 4), lone)

    give = pltpu.make_async_remote_copy(src_ref=own.at[3, 3, other], dst_ref=last, send_sem=last_sem.at[0], recv_sem=last_sem.at[1],
                                        device_id=here.partner, device_id_type=MESH)
    give.start()
    sent.append(give)

    def emit(mb, val):
        y_ref[mb] = val[:, :dm].astype(BF16)
        dx_ref[mb] = val[:, dm:2 * dm].astype(BF16)
        dg_ref[mb] = val[:, 2 * dm:2 * dm + top_k]

    emit(k, own[3, 3, k])
    give.wait_recv()
    emit(other, last[...])
    for c in sent:
        c.wait_send()


def reduce_tokens(part, dm, top_k):
    _, chips, cores, tok_dev, width = part.shape
    vmem = pl.BlockSpec(memory_space=pltpu.VMEM)
    block = (cores, tok_dev, width)
    ring_sems = pltpu.SemaphoreType.DMA((4, 4))
    pair_sems = pltpu.SemaphoreType.DMA((RING, RING))
    return pl.pallas_call(
        functools.partial(reduce_kernel, dm, top_k),
        out_shape=(
            jax.ShapeDtypeStruct((2, tok_dev, dm), BF16),
            jax.ShapeDtypeStruct((2, tok_dev, dm), BF16),
            jax.ShapeDtypeStruct((2, tok_dev, top_k), F32),
        ),
        in_specs=[pl.BlockSpec(memory_space=pltpu.HBM)],
        out_specs=(vmem, vmem, vmem),
        scratch_shapes=[
            pltpu.VMEM((RING, RING) + block, F32),
            pltpu.VMEM((RING, RING) + block, F32),
            pltpu.VMEM((2, RING + 1) + block, F32),
            pltpu.VMEM((RING + 1,) + block, F32),
            pltpu.VMEM((tok_dev, width), F32),
            pair_sems, pair_sems, pair_sems, ring_sems, ring_sems,
            pltpu.SemaphoreType.DMA((2,)),
        ],
        compiler_params=pltpu.CompilerParams(collective_id=1, has_side_effects=True, vmem_limit_bytes=60_000_000),
        name="reduce_tokens",
    )(part)


def solution(mesh):
    group = mesh.shape["row"] * mesh.shape["col"] * mesh.shape["core"]
    tok_spec = P(None, ALL_AXES, None)
    w_spec = P(ALL_AXES, None, None)

    def moe_layer(x, route_idx, gates, w_gate, w_up, w_down, grad_y):
        _, tok_dev, dm = x.shape
        top_k = route_idx.shape[2]
        width = 2 * dm + LANES
        chips = group // 2
        xd = gather_tokens(x, grad_y, route_idx, gates, chips).reshape(2, group * tok_dev, width)
        part, g_gate, g_up, g_down = expert_stage(xd, w_gate, w_up, w_down, top_k, group * (tok_dev // 2))
        y, dx, dg = reduce_tokens(part.reshape(2, chips, 2, tok_dev, width), dm, top_k)
        return y, dx, dg, g_gate, g_up, g_down

    return jax.shard_map(moe_layer, mesh=mesh, in_specs=(tok_spec, tok_spec, tok_spec, w_spec, w_spec, w_spec, tok_spec), out_specs=(tok_spec, tok_spec, tok_spec, w_spec, w_spec, w_spec), check_vma=False)
```

```python
import functools

import jax
import jax.numpy as jnp
from jax import lax
from jax.experimental import pallas as pl
from jax.experimental.pallas import tpu as pltpu
from jax.sharding import PartitionSpec as P

GROUP_AXES = ("row", "col", "core")
ALL_AXES = ("rep", "row", "col", "core")
F32 = jnp.float32
BF16 = jnp.bfloat16
LANES = 128
SMALL = 32
EXPERT_VMEM = 46_000_000
COMM_VMEM = 30_000_000


def dot_nn(a, b):
    return lax.dot_general(a, b, (((1,), (0,)), ((), ())), preferred_element_type=F32)


def dot_nt(a, b):
    return lax.dot_general(a, b, (((1,), (1,)), ((), ())), preferred_element_type=F32)


def dot_tn(a, b):
    return lax.dot_general(a, b, (((0,), (0,)), ((), ())), preferred_element_type=F32)


def split3(v):
    h1 = v.astype(BF16)
    r1 = v - h1.astype(F32)
    h2 = r1.astype(BF16)
    h3 = (r1 - h2.astype(F32)).astype(BF16)
    return h1, h2, h3


def col_blocks(width, step):
    return [(s, min(step, width - s)) for s in range(0, width, step)]


def expert_kernel(dims, xd_v, wg_hbm, wu_hbm, wd_hbm, acc_v, gg_hbm, gu_hbm, gd_hbm,
                  pt_v, gr_v, wgu_v, wd_v, og_v, ou_v, od_v, pos_v,
                  xt_v, qt_v, a_v, duv_v, cnt_s, base_s, sem_w, sem_o):
    tokens, dm, ff, el, top_k, seg = dims
    n_row, n_col, n_core = lax.axis_size("row"), lax.axis_size("col"), lax.axis_size("core")
    me = (lax.axis_index("row") * n_col + lax.axis_index("col")) * n_core + lax.axis_index("core")
    width = 2 * dm + LANES

    def load_w(e, slot):
        pairs = ((wg_hbm, wgu_v.at[slot, :, pl.ds(0, ff)]), (wu_hbm, wgu_v.at[slot, :, pl.ds(ff, ff)]), (wd_hbm, wd_v.at[slot]))
        return [pltpu.make_async_copy(h.at[e], v, sem_w.at[slot, i]) for i, (h, v) in enumerate(pairs)]

    def store_g(e, slot):
        return [pltpu.make_async_copy(v.at[slot], h.at[e], sem_o.at[slot, i])
                for i, (h, v) in enumerate(((gg_hbm, og_v), (gu_hbm, ou_v), (gd_hbm, od_v)))]

    for m in range(2):
        for c in load_w(m, m):
            c.start()

    row_i = lax.broadcasted_iota(jnp.int32, (tokens, tokens), 0)
    col_i = lax.broadcasted_iota(jnp.int32, (tokens, tokens), 1)
    tri = (row_i < col_i).astype(F32).astype(BF16)
    sub = lax.broadcasted_iota(jnp.int32, (8, tokens), 0)
    eids = jnp.where(sub < el, (me * el + sub), -1).astype(F32)

    def chunks(total):
        return jnp.maximum((total + (seg - 1)) // seg, 1)

    n_chunks = []
    for m in range(2):
        meta_t = xd_v[m, :, 2 * dm:].astype(F32).T
        hits = jnp.zeros((8, tokens), F32)
        for j in range(top_k):
            hits = hits + (meta_t[j:j + 1, :] == eids).astype(F32)
        rank = dot_nn(hits.astype(BF16), tri)
        total = jnp.int32(0)
        for e in range(el):
            cnt = jnp.sum(hits[e:e + 1, :]).astype(jnp.int32)
            cnt_s[m, e] = cnt
            base_s[m, e] = total
            pos_v[m, e:e + 1, :] = jnp.where(hits[e:e + 1, :] > 0, rank[e:e + 1, :] + total.astype(F32), -1.0)
            total = total + (cnt + 15) // 16 * 16
        n_ch = chunks(total)
        n_chunks.append(n_ch)

        def gather(c, carry, m=m):
            off = pl.multiple_of(c * seg, seg)
            rows = (lax.broadcasted_iota(jnp.int32, (seg, tokens), 0) + off).astype(F32)
            pick = rows == pos_v[m, 0:1, :]
            for e in range(1, el):
                pick = pick | (rows == pos_v[m, e:e + 1, :])
            pick_f = pick.astype(F32)
            pt_v[m, :, pl.ds(off, seg)] = pick_f.T.astype(BF16)
            pick_b = pick_f.astype(BF16)
            for s, w in col_blocks(width, 512):
                gr_v[m, pl.ds(off, seg), s:s + w] = dot_nn(pick_b, xd_v[m, :, s:s + w]).astype(BF16)
            return carry

        lax.fori_loop(0, n_ch, gather, 0)

    def tile(e, slot, ra, rb, m_a, n_a, n_b, first):
        rows = ra + rb
        base_a = pl.multiple_of(base_s[m_a, e], 16)
        base_b = pl.multiple_of(base_s[1 - m_a, e], 16)
        it = lax.broadcasted_iota(jnp.int32, (rows, 1), 0)
        valid = ((it < ra) & (it < n_a)) | ((it >= ra) & (it - ra < n_b))

        def read(s, w):
            return jnp.concatenate([gr_v[m_a, pl.ds(base_a, ra), s:s + w],
                                    gr_v[1 - m_a, pl.ds(base_b, rb), s:s + w]], axis=0)

        def write(s, w, val):
            merged = jnp.where(valid, val.astype(F32), read(s, w).astype(F32)).astype(BF16)
            gr_v[m_a, pl.ds(base_a, ra), s:s + w] = merged[:ra]
            gr_v[1 - m_a, pl.ds(base_b, rb), s:s + w] = merged[ra:]

        lane = lax.broadcasted_iota(jnp.int32, (rows, LANES), 1)
        meta = jnp.where(valid, read(2 * dm, LANES).astype(F32), 0.0)
        eid = (me * el + e).astype(F32)
        mine = ((meta == eid) & (lane < top_k)).astype(F32)
        sel = pltpu.roll(mine, 8, 1) + pltpu.roll(mine, 16, 1) + pltpu.roll(mine, 24, 1)
        gate = jnp.where(valid, jnp.sum(meta * sel, axis=1, keepdims=True), 0.0)
        for s, w in col_blocks(dm, 256):
            xt_v[:rows, s:s + w] = jnp.where(valid, read(s, w).astype(F32), 0.0).astype(BF16)
            dy = jnp.where(valid, read(dm + s, w).astype(F32), 0.0)
            qt_v[:rows, s:s + w] = (gate * dy).astype(BF16)
        xt = xt_v[:rows, :]
        uv = dot_nn(xt, wgu_v[slot]).astype(BF16).astype(F32)
        u, v = uv[:, :ff], uv[:, ff:]
        r = dot_nt(qt_v[:rows, :], wd_v[slot])
        s_g = jax.nn.sigmoid(u)
        a_v[:rows, :] = (u * s_g * v).astype(BF16)
        duv_v[:rows, :ff] = (r * v * s_g * (1.0 + u * (1.0 - s_g))).astype(BF16)
        duv_v[:rows, ff:] = (r * u * s_g).astype(BF16)
        a = a_v[:rows, :]
        duv = duv_v[:rows, :]
        dots = jnp.zeros((rows, 1), F32)
        for s, w in col_blocks(dm, 256):
            o = dot_nn(a, wd_v[slot, :, s:s + w]).astype(BF16)
            dy = jnp.where(valid, read(dm + s, w).astype(F32), 0.0)
            dots = dots + jnp.sum(dy * o.astype(F32), axis=1, keepdims=True)
            write(s, w, o)
        for s, w in col_blocks(dm, 256):
            write(dm + s, w, dot_nt(duv, wgu_v[slot, s:s + w, :]).astype(BF16))
        d1, d2, d3 = split3(dots)
        g1, g2, g3 = split3(gate)
        new_meta = jnp.zeros((rows, LANES), F32)
        for at, val in ((e, d1), (8 + e, d2), (16 + e, d3), (32, g1), (33, g2), (34, g3)):
            new_meta = jnp.where(lane == at, val.astype(F32), new_meta)
        write(2 * dm, LANES, new_meta)

        def put(ref, idx, val):
            if first is None:
                ref[idx] = val
            else:
                ref[idx] = jnp.where(first, 0.0, ref[idx]) + val

        for s, w in col_blocks(dm, 256):
            g_in = dot_tn(xt_v[:rows, s:s + w], duv)
            put(og_v, (slot, slice(s, s + w)), g_in[:, :ff])
            put(ou_v, (slot, slice(s, s + w)), g_in[:, ff:])
        for s, w in col_blocks(dm, 256):
            put(od_v, (slot, slice(None), slice(s, s + w)), dot_tn(a, qt_v[:rows, s:s + w]))

    def expert(e, carry):
        slot = lax.rem(e, 2)
        for c in load_w(e, slot):
            c.wait()

        @pl.when(e >= 2)
        def _():
            for c in store_g(e - 2, slot):
                c.wait()

        n0, n1 = cnt_s[0, e], cnt_s[1, e]
        big0, big1 = n0 > SMALL, n1 > SMALL

        @pl.when(jnp.logical_not(big0 | big1))
        def _():
            tile(e, slot, SMALL, SMALL, 0, n0, n1, None)

        @pl.when(big0 | big1)
        def _():
            both = big0 & big1

            def one(i, inner):
                m_a = jnp.where(both, i, jnp.where(big0, 0, 1))
                n_a = jnp.where(m_a == 0, n0, n1)
                n_b = jnp.where(both, 0, jnp.where(m_a == 0, n1, n0))
                tile(e, slot, seg, SMALL, m_a, n_a, n_b, i == 0)
                return inner

            lax.fori_loop(0, jnp.where(both, 2, 1), one, 0)

        for c in store_g(e, slot):
            c.start()

        @pl.when(e + 2 < el)
        def _():
            for c in load_w(e + 2, slot):
                c.start()

        return carry

    lax.fori_loop(0, el, expert, 0)

    for m in range(2):
        def scatter(c, carry, m=m):
            off = pl.multiple_of(c * seg, seg)
            rows = pl.ds(off, seg)
            first = c == 0
            pt = pt_v[m, :, rows]
            gp = gr_v[m, rows, 2 * dm:].astype(F32)
            gate = gp[:, 32:33] + gp[:, 33:34] + gp[:, 34:35]
            for s, w in col_blocks(dm, 256):
                h1, h2, h3 = split3(gate * gr_v[m, rows, s:s + w].astype(F32))
                add = dot_nn(pt, h1) + dot_nn(pt, h2) + dot_nn(pt, h3)
                acc_v[m, :, s:s + w] = jnp.where(first, 0.0, acc_v[m, :, s:s + w]) + add
            for s, w in col_blocks(dm + LANES, 256):
                lo = dm + s
                add = dot_nn(pt, gr_v[m, rows, lo:lo + w])
                acc_v[m, :, lo:lo + w] = jnp.where(first, 0.0, acc_v[m, :, lo:lo + w]) + add
            return carry

        lax.fori_loop(0, n_chunks[m], scatter, 0)
        lane = lax.broadcasted_iota(jnp.int32, (tokens, LANES), 1)
        ids = jnp.where(lane < top_k, xd_v[m, :, 2 * dm:].astype(F32), -1.0)
        raw = acc_v[m, :, 2 * dm:]
        out = jnp.zeros((tokens, LANES), F32)
        for e in range(el):
            val = raw[:, e:e + 1] + raw[:, 8 + e:9 + e] + raw[:, 16 + e:17 + e]
            out = jnp.where(ids == (me * el + e).astype(F32), val, out)
        acc_v[m, :, 2 * dm:] = out

    for e in range(el - 2, el):
        for c in store_g(e, e % 2):
            c.wait()


def expert_stage(xd, w_gate, w_up, w_down, top_k, seg):
    _, tokens, width = xd.shape
    el, dm, ff = w_gate.shape
    any_spec = pl.BlockSpec(memory_space=pltpu.HBM)
    vmem_spec = pl.BlockSpec(memory_space=pltpu.VMEM)
    rows_max = el * seg
    tile_rows = seg + SMALL
    dims = (tokens, dm, ff, el, top_k, seg)
    return pl.pallas_call(
        functools.partial(expert_kernel, dims),
        out_shape=(
            pltpu.VMEM((2, tokens, width), F32),
            pltpu.HBM((el, dm, ff), F32),
            pltpu.HBM((el, dm, ff), F32),
            pltpu.HBM((el, ff, dm), F32),
        ),
        in_specs=[vmem_spec] + [any_spec] * 3,
        out_specs=[vmem_spec] + [any_spec] * 3,
        scratch_shapes=[
            pltpu.VMEM((2, tokens, rows_max), BF16),
            pltpu.VMEM((2, rows_max, width), BF16),
            pltpu.VMEM((2, dm, 2 * ff), BF16),
            pltpu.VMEM((2, ff, dm), BF16),
            pltpu.VMEM((2, dm, ff), F32),
            pltpu.VMEM((2, dm, ff), F32),
            pltpu.VMEM((2, ff, dm), F32),
            pltpu.VMEM((2, 8, tokens), F32),
            pltpu.VMEM((tile_rows, dm), BF16),
            pltpu.VMEM((tile_rows, dm), BF16),
            pltpu.VMEM((tile_rows, ff), BF16),
            pltpu.VMEM((tile_rows, 2 * ff), BF16),
            pltpu.SMEM((2, 8), jnp.int32),
            pltpu.SMEM((2, 8), jnp.int32),
            pltpu.SemaphoreType.DMA((2, 3)),
            pltpu.SemaphoreType.DMA((2, 3)),
        ],
        compiler_params=pltpu.CompilerParams(vmem_limit_bytes=EXPERT_VMEM),
        name="experts",
    )(pltpu.with_memory_space_constraint(xd, pltpu.VMEM), *(pltpu.with_memory_space_constraint(w, pltpu.HBM) for w in (w_gate, w_up, w_down)))


RING = 4
NEAR = (0, -1, 1, 2)
FAR = (2, -1, 1, 0)
GROUPS = (slice(0, 1), slice(1, 3), slice(3, 4))
MESH = pl.DeviceIdType.MESH


class Place:
    def __init__(self):
        self.row, self.col, self.core = (lax.axis_index(a) for a in GROUP_AXES)
        self.n_row, self.n_col = lax.axis_size("row"), lax.axis_size("col")
        self.other = 1 - self.core
        self.partner = {"core": self.other}

    def spot(self, first, d1, d2):
        row = lax.rem(self.row + (d1 * first + d2 * (1 - first)) + self.n_row, self.n_row)
        col = lax.rem(self.col + (d1 * (1 - first) + d2 * first) + self.n_col, self.n_col)
        return row, col

    def peer(self, axis, d):
        row, col = self.spot(self.core, d, 0) if axis == 1 else self.spot(self.core, 0, d)
        return {"row": row, "col": col}

    def barrier(self):
        sem = pltpu.get_barrier_semaphore()
        peers = [self.peer(axis, d) for axis in (1, 2) for d in (1, -1)] + [self.partner]
        for peer in peers:
            pl.semaphore_signal(sem, inc=1, device_id=peer, device_id_type=MESH)
        pl.semaphore_wait(sem, len(peers))


def half_lanes(width):
    mid = (width // LANES + 1) // 2 * LANES
    return (pl.ds(0, mid), pl.ds(mid, width - mid))


def token_meta(route, gates):
    top_k, tok_dev = route.shape
    zero = jnp.zeros((8 - top_k, tok_dev), F32)
    parts = [route.astype(F32)] + [p.astype(F32) for p in split3(gates)]
    rows = jnp.concatenate([v for p in parts for v in (p, zero)], axis=0).astype(BF16)
    n = rows.shape[0]
    eye = (lax.broadcasted_iota(jnp.int32, (n, LANES), 0) == lax.broadcasted_iota(jnp.int32, (n, LANES), 1)).astype(F32).astype(BF16)
    return dot_tn(rows, eye).astype(BF16)


def gather_kernel(x_hbm, dy_hbm, route_ref, gates_ref, buf, stage, send_sem, recv_sem, load_sem):
    here = Place()
    k, other = here.core, here.other
    dm = x_hbm.shape[2]
    halves = half_lanes(2 * dm + LANES)
    sent = []

    def move(idx, src, dst, peer):
        return pltpu.make_async_remote_copy(src_ref=src, dst_ref=dst, send_sem=send_sem.at[idx], recv_sem=recv_sem.at[idx],
                                            device_id=peer, device_id_type=MESH)

    def send(idx, src, dst, peer):
        c = move(idx, src, dst, peer)
        c.start()
        sent.append(c)

    def arrive(idx, dst):
        move(idx, dst, dst, here.partner).wait_recv()

    def have(gi, d):
        g = GROUPS[gi]
        send(24 + 3 * d + gi, buf.at[0, d, g], buf.at[1, d, g], here.partner)

    def both_ways(p, src, left, right, axis):
        for way, dst in ((0, left), (1, right)):
            for n in range(2):
                lanes = halves[way if n == 0 else 1 - way]
                send(6 * p + 2 * way + n, src.at[:, :, :, lanes], dst.at[:, :, :, lanes], here.peer(axis, 1 - 2 * way))

    def relay(p, left, right, far, axis):
        for way, src in ((0, left), (1, right)):
            lanes = halves[way]
            arrive(6 * p + 2 * way, src.at[:, :, :, lanes])
            send(6 * p + 4 + way, src.at[:, :, :, lanes], far.at[:, :, :, lanes], here.peer(axis, 1 - 2 * way))

    def rest(p, left, right):
        for way, src in ((0, left), (1, right)):
            arrive(6 * p + 2 * way + 1, src.at[:, :, :, halves[1 - way]])

    def far_end(p, far):
        for way in range(2):
            arrive(6 * p + 4 + way, far.at[:, :, :, halves[way]])

    first = [buf.at[0, 0, pl.ds(i, 1)] for i in range(RING)]
    second = [[buf.at[0, d, g] for d in range(RING)] for g in GROUPS]

    def spread(gi):
        both_ways(1 + gi, second[gi][0], second[gi][1], second[gi][2], 2)
        have(gi, 0)

    def second_relay(gi):
        relay(1 + gi, second[gi][1], second[gi][2], second[gi][3], 2)

    def second_rest(gi):
        rest(1 + gi, second[gi][1], second[gi][2])
        have(gi, 1)
        have(gi, 2)

    def second_far(gi):
        far_end(1 + gi, second[gi][3])
        have(gi, 3)

    mine = buf.at[0, 0, 0, k]
    loads = [pltpu.make_async_copy(h.at[mb], dst.at[:, pl.ds(lo, dm)], load_sem.at[n])
             for n, (h, mb, dst, lo) in enumerate(((x_hbm, other, stage, 0), (dy_hbm, other, stage, dm), (x_hbm, k, mine, 0), (dy_hbm, k, mine, dm)))]
    for c in loads:
        c.start()
    metas = [token_meta(route_ref[:, m, :], gates_ref[:, m, :]) for m in range(2)]
    zero_core = k == 0
    stage[:, 2 * dm:] = jnp.where(zero_core, metas[1].astype(F32), metas[0].astype(F32)).astype(BF16)
    buf[0, 0, 0, k, :, 2 * dm:] = jnp.where(zero_core, metas[0].astype(F32), metas[1].astype(F32)).astype(BF16)
    here.barrier()
    for c in loads:
        c.wait()
    send(36, stage, buf.at[0, 0, 0, k], here.partner)
    arrive(36, buf.at[0, 0, 0, other])
    both_ways(0, first[0], first[1], first[2], 1)
    spread(0)
    relay(0, first[1], first[2], first[3], 1)
    second_relay(0)
    rest(0, first[1], first[2])
    spread(1)
    second_rest(0)
    far_end(0, first[3])
    spread(2)
    second_relay(1)
    second_far(0)
    second_rest(1)
    second_relay(2)
    second_rest(2)
    second_far(1)
    second_far(2)
    for gi, d in [(gi, d) for d in range(RING) for gi in range(len(GROUPS))]:
        arrive(24 + 3 * d + gi, buf.at[1, d, GROUPS[gi]])
    for c in sent:
        c.wait_send()


def gather_tokens(x, grad_y, route_idx, gates):
    _, tok_dev, dm = x.shape
    width = 2 * dm + LANES
    hbm = pl.BlockSpec(memory_space=pltpu.HBM)
    vmem = pl.BlockSpec(memory_space=pltpu.VMEM)
    sems = pltpu.SemaphoreType.DMA((37,))
    return pl.pallas_call(
        gather_kernel,
        out_shape=pltpu.VMEM((2, RING, RING, 2, tok_dev, width), BF16),
        in_specs=[hbm, hbm, vmem, vmem],
        out_specs=vmem,
        scratch_shapes=[pltpu.VMEM((tok_dev, width), BF16), sems, sems, pltpu.SemaphoreType.DMA((4,))],
        compiler_params=pltpu.CompilerParams(collective_id=0, has_side_effects=True, vmem_limit_bytes=COMM_VMEM),
        name="gather_tokens",
    )(pltpu.with_memory_space_constraint(x, pltpu.HBM), pltpu.with_memory_space_constraint(grad_y, pltpu.HBM), jnp.transpose(route_idx, (2, 0, 1)), jnp.transpose(gates, (2, 0, 1)))


def reduce_kernel(dm, top_k, part_ref, y_ref, dx_ref, dg_ref, own, pair, full, half, last, pair_send, pair_recv,
                  ring_send, ring_recv, last_sem):
    here = Place()
    k, other = here.core, here.other
    halves = half_lanes(part_ref.shape[5])
    sent = []

    def near_at(n):
        return NEAR.index(FAR[n])

    def swap(d, i):
        return pltpu.make_async_remote_copy(src_ref=part_ref.at[1, near_at(d), near_at(i)], dst_ref=pair.at[d, i], send_sem=pair_send.at[d, i],
                                            recv_sem=pair_recv.at[d, i], device_id=here.partner, device_id_type=MESH)

    def move(f, kind, src, dst, axis):
        return pltpu.make_async_remote_copy(src_ref=src, dst_ref=dst, send_sem=ring_send.at[f, kind], recv_sem=ring_recv.at[f, kind],
                                            device_id=here.peer(axis, 1 if kind % 2 == 0 else -1), device_id_type=MESH)

    def go(f, kind, src, dst, axis):
        c = move(f, kind, src, dst, axis)
        c.start()
        sent.append(c)

    def arrive(f, kind, dst):
        move(f, kind, dst, dst, 1).wait_recv()

    def add_pair(d, gi):
        for i in range(GROUPS[gi].start, GROUPS[gi].stop):
            swap(d, i).wait_recv()
            own[d, i] = part_ref[0, near_at(d), near_at(i)] + pair[d, i]

    def far(f, src, g, axis):
        for kind in range(2):
            go(f, kind, src.at[:, :, :, halves[kind]], half.at[g, :, :, halves[kind]], axis)

    def near(f, ref, g, axis):
        for kind, step in ((0, 1), (1, -1)):
            lanes = halves[kind]
            arrive(f, kind, half.at[g, :, :, lanes])
            d, at = ref(step)
            own[d, at, :, :, lanes] = own[d, at, :, :, lanes] + half[g, :, :, lanes]
        for kind, step in ((2, 1), (3, -1)):
            d, at = ref(step)
            go(f, kind, own.at[d, at], full.at[kind - 2, g], axis)

    def done(f, at, g):
        arrive(f, 2, full.at[0, g])
        arrive(f, 3, full.at[1, g])
        own[3, at] = own[3, at] + full[0, g] + full[1, g]

    def far2(gi):
        add_pair(0, gi)
        far(gi, own.at[0, GROUPS[gi]], GROUPS[gi], 2)

    def near2(gi):
        add_pair(2, gi)
        add_pair(1, gi)
        near(gi, lambda step: (2 if step == 1 else 1, GROUPS[gi]), GROUPS[gi], 2)

    def done2(gi):
        add_pair(3, gi)
        done(gi, GROUPS[gi], GROUPS[gi])

    order = [(0, 0), (0, 1), (0, 2), (2, 0), (1, 0), (0, 3), (2, 1), (2, 2), (1, 1), (1, 2), (3, 0), (2, 3), (1, 3), (3, 1), (3, 2), (3, 3)]
    here.barrier()
    for q in order:
        c = swap(*q)
        c.start()
        sent.append(c)
    lone = slice(RING, RING + 1)
    far2(0)
    far2(1)
    near2(0)
    far2(2)
    near2(1)
    done2(0)
    far(3, own.at[3, slice(0, 1)], lone, 1)
    near2(2)
    done2(1)
    near(3, lambda step: (3, slice(2, 3) if step == 1 else slice(1, 2)), lone, 1)
    done2(2)
    done(3, slice(3, 4), lone)

    give = pltpu.make_async_remote_copy(src_ref=own.at[3, 3, other], dst_ref=last, send_sem=last_sem.at[0], recv_sem=last_sem.at[1],
                                        device_id=here.partner, device_id_type=MESH)
    give.start()
    sent.append(give)

    def emit(mb, val):
        y_ref[mb] = val[:, :dm].astype(BF16)
        dx_ref[mb] = val[:, dm:2 * dm].astype(BF16)
        dg_ref[mb] = val[:, 2 * dm:2 * dm + top_k]

    emit(k, own[3, 3, k])
    give.wait_recv()
    emit(other, last[...])
    for c in sent:
        c.wait_send()


def reduce_tokens(part, dm, top_k):
    _, _, _, cores, tok_dev, width = part.shape
    vmem = pl.BlockSpec(memory_space=pltpu.VMEM)
    block = (cores, tok_dev, width)
    ring_sems = pltpu.SemaphoreType.DMA((4, 4))
    pair_sems = pltpu.SemaphoreType.DMA((RING, RING))
    return pl.pallas_call(
        functools.partial(reduce_kernel, dm, top_k),
        out_shape=(
            jax.ShapeDtypeStruct((2, tok_dev, dm), BF16),
            jax.ShapeDtypeStruct((2, tok_dev, dm), BF16),
            jax.ShapeDtypeStruct((2, tok_dev, top_k), F32),
        ),
        in_specs=[vmem],
        out_specs=(vmem, vmem, vmem),
        scratch_shapes=[
            pltpu.VMEM((RING, RING) + block, F32),
            pltpu.VMEM((RING, RING) + block, F32),
            pltpu.VMEM((2, RING + 1) + block, F32),
            pltpu.VMEM((RING + 1,) + block, F32),
            pltpu.VMEM((tok_dev, width), F32),
            pair_sems, pair_sems, ring_sems, ring_sems,
            pltpu.SemaphoreType.DMA((2,)),
        ],
        compiler_params=pltpu.CompilerParams(collective_id=1, has_side_effects=True, vmem_limit_bytes=COMM_VMEM),
        name="reduce_tokens",
    )(pltpu.with_memory_space_constraint(part, pltpu.VMEM))


def solution(mesh):
    group = mesh.shape["row"] * mesh.shape["col"] * mesh.shape["core"]
    tok_spec = P(None, ALL_AXES, None)
    w_spec = P(ALL_AXES, None, None)

    def moe_layer(x, route_idx, gates, w_gate, w_up, w_down, grad_y):
        _, tok_dev, dm = x.shape
        top_k = route_idx.shape[2]
        width = 2 * dm + LANES
        xd = gather_tokens(x, grad_y, route_idx, gates).reshape(2, group * tok_dev, width)
        part, g_gate, g_up, g_down = expert_stage(xd, w_gate, w_up, w_down, top_k, group * (tok_dev // 2))
        y, dx, dg = reduce_tokens(part.reshape(2, RING, RING, 2, tok_dev, width), dm, top_k)
        return y, dx, dg, g_gate, g_up, g_down

    return jax.shard_map(moe_layer, mesh=mesh, in_specs=(tok_spec, tok_spec, tok_spec, w_spec, w_spec, w_spec, tok_spec), out_specs=(tok_spec, tok_spec, tok_spec, w_spec, w_spec, w_spec), check_vma=False)
```

```python
import functools

import jax
import jax.numpy as jnp
from jax import lax
from jax.experimental import pallas as pl
from jax.experimental.pallas import tpu as pltpu
from jax.sharding import PartitionSpec as P

GROUP_AXES = ("row", "col", "core")
ALL_AXES = ("rep", "row", "col", "core")
F32 = jnp.float32
BF16 = jnp.bfloat16
LANES = 128
SMALL = 32
EXPERT_VMEM = 49_500_000
COMM_VMEM = 30_000_000


def dot_nn(a, b):
    return lax.dot_general(a, b, (((1,), (0,)), ((), ())), preferred_element_type=F32)


def dot_nt(a, b):
    return lax.dot_general(a, b, (((1,), (1,)), ((), ())), preferred_element_type=F32)


def dot_tn(a, b):
    return lax.dot_general(a, b, (((0,), (0,)), ((), ())), preferred_element_type=F32)


def split3(v):
    h1 = v.astype(BF16)
    r1 = v - h1.astype(F32)
    h2 = r1.astype(BF16)
    h3 = (r1 - h2.astype(F32)).astype(BF16)
    return h1, h2, h3


def col_blocks(width, step):
    return [(s, min(step, width - s)) for s in range(0, width, step)]


def expert_kernel(dims, xd_v, wg_hbm, wu_hbm, wd_hbm, acc_v, gg_hbm, gu_hbm, gd_hbm,
                  pt_v, gr_v, wgu_v, wd_v, og_v, ou_v, od_v, pos_v,
                  xt_v, qt_v, a_v, duv_v, cnt_s, base_s, sem_w, sem_o):
    tokens, dm, ff, el, top_k, seg = dims
    n_row, n_col, n_core = lax.axis_size("row"), lax.axis_size("col"), lax.axis_size("core")
    me = (lax.axis_index("row") * n_col + lax.axis_index("col")) * n_core + lax.axis_index("core")
    width = 2 * dm + LANES

    def load_w(e):
        pairs = ((wg_hbm, wgu_v.at[e, :, pl.ds(0, ff)]), (wu_hbm, wgu_v.at[e, :, pl.ds(ff, ff)]), (wd_hbm, wd_v.at[e]))
        return [pltpu.make_async_copy(h.at[e], v, sem_w.at[e, i]) for i, (h, v) in enumerate(pairs)]

    def store_g(e, slot):
        return [pltpu.make_async_copy(v.at[slot], h.at[e], sem_o.at[slot, i])
                for i, (h, v) in enumerate(((gg_hbm, og_v), (gu_hbm, ou_v), (gd_hbm, od_v)))]

    for e in range(el):
        for c in load_w(e):
            c.start()

    row_i = lax.broadcasted_iota(jnp.int32, (tokens, tokens), 0)
    col_i = lax.broadcasted_iota(jnp.int32, (tokens, tokens), 1)
    tri = (row_i < col_i).astype(F32).astype(BF16)
    sub = lax.broadcasted_iota(jnp.int32, (8, tokens), 0)
    eids = jnp.where(sub < el, (me * el + sub), -1).astype(F32)

    def chunks(total):
        return jnp.maximum((total + (seg - 1)) // seg, 1)

    n_chunks = []
    for m in range(2):
        meta_t = xd_v[m, :, 2 * dm:].astype(F32).T
        hits = jnp.zeros((8, tokens), F32)
        for j in range(top_k):
            hits = hits + (meta_t[j:j + 1, :] == eids).astype(F32)
        rank = dot_nn(hits.astype(BF16), tri)
        total = jnp.int32(0)
        for e in range(el):
            cnt = jnp.sum(hits[e:e + 1, :]).astype(jnp.int32)
            cnt_s[m, e] = cnt
            base_s[m, e] = total
            pos_v[m, e:e + 1, :] = jnp.where(hits[e:e + 1, :] > 0, rank[e:e + 1, :] + total.astype(F32), -1.0)
            total = total + (cnt + 15) // 16 * 16
        n_ch = chunks(total)
        n_chunks.append(n_ch)

        def gather(c, carry, m=m):
            off = pl.multiple_of(c * seg, seg)
            rows = (lax.broadcasted_iota(jnp.int32, (seg, tokens), 0) + off).astype(F32)
            pick = rows == pos_v[m, 0:1, :]
            for e in range(1, el):
                pick = pick | (rows == pos_v[m, e:e + 1, :])
            pick_f = pick.astype(F32)
            pt_v[m, :, pl.ds(off, seg)] = pick_f.T.astype(BF16)
            pick_b = pick_f.astype(BF16)
            for s, w in col_blocks(width, 512):
                gr_v[m, pl.ds(off, seg), s:s + w] = dot_nn(pick_b, xd_v[m, :, s:s + w]).astype(BF16)
            return carry

        lax.fori_loop(0, n_ch, gather, 0)

    def tile(e, slot, ra, rb, m_a, n_a, n_b, first):
        rows = ra + rb
        base_a = pl.multiple_of(base_s[m_a, e], 16)
        base_b = pl.multiple_of(base_s[1 - m_a, e], 16)
        it = lax.broadcasted_iota(jnp.int32, (rows, 1), 0)
        valid = ((it < ra) & (it < n_a)) | ((it >= ra) & (it - ra < n_b))

        def read(s, w):
            return jnp.concatenate([gr_v[m_a, pl.ds(base_a, ra), s:s + w],
                                    gr_v[1 - m_a, pl.ds(base_b, rb), s:s + w]], axis=0)

        def write(s, w, val):
            merged = jnp.where(valid, val.astype(F32), read(s, w).astype(F32)).astype(BF16)
            gr_v[m_a, pl.ds(base_a, ra), s:s + w] = merged[:ra]
            gr_v[1 - m_a, pl.ds(base_b, rb), s:s + w] = merged[ra:]

        lane = lax.broadcasted_iota(jnp.int32, (rows, LANES), 1)
        meta = jnp.where(valid, read(2 * dm, LANES).astype(F32), 0.0)
        eid = (me * el + e).astype(F32)
        mine = ((meta == eid) & (lane < top_k)).astype(F32)
        sel = pltpu.roll(mine, 8, 1) + pltpu.roll(mine, 16, 1) + pltpu.roll(mine, 24, 1)
        gate = jnp.where(valid, jnp.sum(meta * sel, axis=1, keepdims=True), 0.0)
        for s, w in col_blocks(dm, 256):
            xt_v[:rows, s:s + w] = jnp.where(valid, read(s, w).astype(F32), 0.0).astype(BF16)
            dy = jnp.where(valid, read(dm + s, w).astype(F32), 0.0)
            qt_v[:rows, s:s + w] = (gate * dy).astype(BF16)
        xt = xt_v[:rows, :]
        uv = dot_nn(xt, wgu_v[e]).astype(BF16).astype(F32)
        u, v = uv[:, :ff], uv[:, ff:]
        r = dot_nt(qt_v[:rows, :], wd_v[e])
        s_g = jax.nn.sigmoid(u)
        a_v[:rows, :] = (u * s_g * v).astype(BF16)
        duv_v[:rows, :ff] = (r * v * s_g * (1.0 + u * (1.0 - s_g))).astype(BF16)
        duv_v[:rows, ff:] = (r * u * s_g).astype(BF16)
        a = a_v[:rows, :]
        duv = duv_v[:rows, :]
        dots = jnp.zeros((rows, 1), F32)
        for s, w in col_blocks(dm, 256):
            o = dot_nn(a, wd_v[e, :, s:s + w]).astype(BF16)
            dy = jnp.where(valid, read(dm + s, w).astype(F32), 0.0)
            dots = dots + jnp.sum(dy * o.astype(F32), axis=1, keepdims=True)
            write(s, w, o)
        for s, w in col_blocks(dm, 256):
            write(dm + s, w, dot_nt(duv, wgu_v[e, s:s + w, :]).astype(BF16))
        d1, d2, d3 = split3(dots)
        g1, g2, g3 = split3(gate)
        new_meta = jnp.zeros((rows, LANES), F32)
        for at, val in ((e, d1), (8 + e, d2), (16 + e, d3), (32, g1), (33, g2), (34, g3)):
            new_meta = jnp.where(lane == at, val.astype(F32), new_meta)
        write(2 * dm, LANES, new_meta)

        def put(ref, idx, val):
            if first is None:
                ref[idx] = val
            else:
                ref[idx] = jnp.where(first, 0.0, ref[idx]) + val

        for s, w in col_blocks(dm, 256):
            g_in = dot_tn(xt_v[:rows, s:s + w], duv)
            put(og_v, (slot, slice(s, s + w)), g_in[:, :ff])
            put(ou_v, (slot, slice(s, s + w)), g_in[:, ff:])
        for s, w in col_blocks(dm, 256):
            put(od_v, (slot, slice(None), slice(s, s + w)), dot_tn(a, qt_v[:rows, s:s + w]))

    def expert(e, carry):
        slot = lax.rem(e, 2)
        for c in load_w(e):
            c.wait()

        @pl.when(e >= 2)
        def _():
            for c in store_g(e - 2, slot):
                c.wait()

        n0, n1 = cnt_s[0, e], cnt_s[1, e]
        big0, big1 = n0 > SMALL, n1 > SMALL

        @pl.when(jnp.logical_not(big0 | big1))
        def _():
            tile(e, slot, SMALL, SMALL, 0, n0, n1, None)

        @pl.when(big0 | big1)
        def _():
            both = big0 & big1

            def one(i, inner):
                m_a = jnp.where(both, i, jnp.where(big0, 0, 1))
                n_a = jnp.where(m_a == 0, n0, n1)
                n_b = jnp.where(both, 0, jnp.where(m_a == 0, n1, n0))
                tile(e, slot, seg, SMALL, m_a, n_a, n_b, i == 0)
                return inner

            lax.fori_loop(0, jnp.where(both, 2, 1), one, 0)

        for c in store_g(e, slot):
            c.start()

        return carry

    lax.fori_loop(0, el, expert, 0)

    for m in range(2):
        def scatter(c, carry, m=m):
            off = pl.multiple_of(c * seg, seg)
            rows = pl.ds(off, seg)
            first = c == 0
            pt = pt_v[m, :, rows]
            gp = gr_v[m, rows, 2 * dm:].astype(F32)
            gate = gp[:, 32:33] + gp[:, 33:34] + gp[:, 34:35]
            for s, w in col_blocks(dm, 256):
                h1, h2, h3 = split3(gate * gr_v[m, rows, s:s + w].astype(F32))
                add = dot_nn(pt, h1) + dot_nn(pt, h2) + dot_nn(pt, h3)
                acc_v[m, :, s:s + w] = jnp.where(first, 0.0, acc_v[m, :, s:s + w]) + add
            for s, w in col_blocks(dm + LANES, 256):
                lo = dm + s
                add = dot_nn(pt, gr_v[m, rows, lo:lo + w])
                acc_v[m, :, lo:lo + w] = jnp.where(first, 0.0, acc_v[m, :, lo:lo + w]) + add
            return carry

        lax.fori_loop(0, n_chunks[m], scatter, 0)
        lane = lax.broadcasted_iota(jnp.int32, (tokens, LANES), 1)
        ids = jnp.where(lane < top_k, xd_v[m, :, 2 * dm:].astype(F32), -1.0)
        raw = acc_v[m, :, 2 * dm:]
        out = jnp.zeros((tokens, LANES), F32)
        for e in range(el):
            val = raw[:, e:e + 1] + raw[:, 8 + e:9 + e] + raw[:, 16 + e:17 + e]
            out = jnp.where(ids == (me * el + e).astype(F32), val, out)
        acc_v[m, :, 2 * dm:] = out

    for e in range(el - 2, el):
        for c in store_g(e, e % 2):
            c.wait()


def expert_stage(xd, w_gate, w_up, w_down, top_k, seg):
    _, tokens, width = xd.shape
    el, dm, ff = w_gate.shape
    any_spec = pl.BlockSpec(memory_space=pltpu.HBM)
    vmem_spec = pl.BlockSpec(memory_space=pltpu.VMEM)
    rows_max = el * seg
    tile_rows = seg + SMALL
    dims = (tokens, dm, ff, el, top_k, seg)
    return pl.pallas_call(
        functools.partial(expert_kernel, dims),
        out_shape=(
            pltpu.VMEM((2, tokens, width), F32),
            pltpu.HBM((el, dm, ff), F32),
            pltpu.HBM((el, dm, ff), F32),
            pltpu.HBM((el, ff, dm), F32),
        ),
        in_specs=[vmem_spec] + [any_spec] * 3,
        out_specs=[vmem_spec] + [any_spec] * 3,
        scratch_shapes=[
            pltpu.VMEM((2, tokens, rows_max), BF16),
            pltpu.VMEM((2, rows_max, width), BF16),
            pltpu.VMEM((el, dm, 2 * ff), BF16),
            pltpu.VMEM((el, ff, dm), BF16),
            pltpu.VMEM((2, dm, ff), F32),
            pltpu.VMEM((2, dm, ff), F32),
            pltpu.VMEM((2, ff, dm), F32),
            pltpu.VMEM((2, 8, tokens), F32),
            pltpu.VMEM((tile_rows, dm), BF16),
            pltpu.VMEM((tile_rows, dm), BF16),
            pltpu.VMEM((tile_rows, ff), BF16),
            pltpu.VMEM((tile_rows, 2 * ff), BF16),
            pltpu.SMEM((2, 8), jnp.int32),
            pltpu.SMEM((2, 8), jnp.int32),
            pltpu.SemaphoreType.DMA((el, 3)),
            pltpu.SemaphoreType.DMA((2, 3)),
        ],
        compiler_params=pltpu.CompilerParams(vmem_limit_bytes=EXPERT_VMEM),
        name="experts",
    )(pltpu.with_memory_space_constraint(xd, pltpu.VMEM), *(pltpu.with_memory_space_constraint(w, pltpu.HBM) for w in (w_gate, w_up, w_down)))


RING = 4
NEAR = (0, -1, 1, 2)
FAR = (2, -1, 1, 0)
GROUPS = (slice(0, 1), slice(1, 3), slice(3, 4))
MESH = pl.DeviceIdType.MESH


class Place:
    def __init__(self):
        self.row, self.col, self.core = (lax.axis_index(a) for a in GROUP_AXES)
        self.n_row, self.n_col = lax.axis_size("row"), lax.axis_size("col")
        self.other = 1 - self.core
        self.partner = {"core": self.other}

    def spot(self, first, d1, d2):
        row = lax.rem(self.row + (d1 * first + d2 * (1 - first)) + self.n_row, self.n_row)
        col = lax.rem(self.col + (d1 * (1 - first) + d2 * first) + self.n_col, self.n_col)
        return row, col

    def peer(self, axis, d):
        row, col = self.spot(self.core, d, 0) if axis == 1 else self.spot(self.core, 0, d)
        return {"row": row, "col": col}

    def barrier(self):
        sem = pltpu.get_barrier_semaphore()
        peers = [self.peer(axis, d) for axis in (1, 2) for d in (1, -1)] + [self.partner]
        for peer in peers:
            pl.semaphore_signal(sem, inc=1, device_id=peer, device_id_type=MESH)
        pl.semaphore_wait(sem, len(peers))


STREAMS = range(2)


def half_lanes(start, size):
    mid = (size // LANES + 1) // 2 * LANES
    return ((start, mid), (start + mid, size - mid))


def stream_lanes(width):
    whole = half_lanes(0, width)
    return [pl.ds(*w) for w in whole], [[pl.ds(*h) for h in half_lanes(*w)] for w in whole]


def token_meta(route, gates):
    top_k, tok_dev = route.shape
    zero = jnp.zeros((8 - top_k, tok_dev), F32)
    parts = [route.astype(F32)] + [p.astype(F32) for p in split3(gates)]
    rows = jnp.concatenate([v for p in parts for v in (p, zero)], axis=0).astype(BF16)
    n = rows.shape[0]
    eye = (lax.broadcasted_iota(jnp.int32, (n, LANES), 0) == lax.broadcasted_iota(jnp.int32, (n, LANES), 1)).astype(F32).astype(BF16)
    return dot_tn(rows, eye).astype(BF16)


def gather_kernel(x_hbm, dy_hbm, route_hbm, gates_hbm, buf, stage, route_v, gates_v, send_sem, recv_sem, load_sem):
    here = Place()
    k, other = here.core, here.other
    dm = x_hbm.shape[2]
    lanes_of, halves = stream_lanes(2 * dm + LANES)
    sent = []

    def move(idx, src, dst, peer):
        return pltpu.make_async_remote_copy(src_ref=src, dst_ref=dst, send_sem=send_sem.at[idx], recv_sem=recv_sem.at[idx],
                                            device_id=peer, device_id_type=MESH)

    def send(idx, src, dst, peer):
        c = move(idx, src, dst, peer)
        c.start()
        sent.append(c)

    def arrive(idx, dst):
        move(idx, dst, dst, here.partner).wait_recv()

    def blk(s, d, g, lanes, side=0):
        ref = buf.at[side, d, g] if s == 0 else buf.at[side, g, d]
        return ref.at[:, :, :, lanes]

    def towards(s, axis, way):
        return here.peer(axis if s == 0 else 3 - axis, 1 - 2 * way)

    class Leg:
        def __init__(self, s, p):
            self.s, self.base, self.axis = s, 37 * s + 6 * p, 1 if p == 0 else 2
            self.at = (lambda j, lanes: blk(s, 0, slice(j, j + 1), lanes)) if p == 0 else (lambda j, lanes: blk(s, j, GROUPS[p - 1], lanes))

        def both_ways(self):
            for way in range(2):
                for n in range(2):
                    lanes = halves[self.s][way if n == 0 else 1 - way]
                    send(self.base + 2 * way + n, self.at(0, lanes), self.at(1 + way, lanes), towards(self.s, self.axis, way))

        def relay(self):
            for way in range(2):
                lanes = halves[self.s][way]
                arrive(self.base + 2 * way, self.at(1 + way, lanes))
                send(self.base + 4 + way, self.at(1 + way, lanes), self.at(3, lanes), towards(self.s, self.axis, way))

        def rest(self):
            for way in range(2):
                arrive(self.base + 2 * way + 1, self.at(1 + way, halves[self.s][1 - way]))

        def far_end(self):
            for way in range(2):
                arrive(self.base + 4 + way, self.at(3, halves[self.s][way]))

    legs = [[Leg(s, p) for p in range(4)] for s in STREAMS]

    def have(s, gi, d):
        lanes = lanes_of[s]
        send(37 * s + 24 + 3 * d + gi, blk(s, d, GROUPS[gi], lanes), blk(s, d, GROUPS[gi], lanes, 1), here.partner)

    def spread(s, gi):
        legs[s][1 + gi].both_ways()
        have(s, gi, 0)

    def second_rest(s, gi):
        legs[s][1 + gi].rest()
        have(s, gi, 1)
        have(s, gi, 2)

    def second_far(s, gi):
        legs[s][1 + gi].far_end()
        have(s, gi, 3)

    mine = buf.at[0, 0, 0, k]
    smalls = [pltpu.make_async_copy(route_hbm, route_v, load_sem.at[4]), pltpu.make_async_copy(gates_hbm, gates_v, load_sem.at[5])]
    loads = [pltpu.make_async_copy(h.at[mb], dst.at[:, pl.ds(lo, dm)], load_sem.at[n])
             for n, (h, mb, dst, lo) in enumerate(((x_hbm, other, stage, 0), (dy_hbm, other, stage, dm), (x_hbm, k, mine, 0), (dy_hbm, k, mine, dm)))]
    for c in smalls + loads:
        c.start()
    for c in smalls:
        c.wait()
    metas = [token_meta(route_v[:, m, :], gates_v[:, m, :]) for m in range(2)]
    zero_core = k == 0
    stage[:, 2 * dm:] = jnp.where(zero_core, metas[1].astype(F32), metas[0].astype(F32)).astype(BF16)
    buf[0, 0, 0, k, :, 2 * dm:] = jnp.where(zero_core, metas[0].astype(F32), metas[1].astype(F32)).astype(BF16)
    here.barrier()
    for c in loads:
        c.wait()
    send(36, stage, buf.at[0, 0, 0, k], here.partner)
    arrive(36, buf.at[0, 0, 0, other])
    for s in STREAMS:
        legs[s][0].both_ways()
    for s in STREAMS:
        spread(s, 0)
    for s in STREAMS:
        legs[s][0].relay()
    for s in STREAMS:
        legs[s][1].relay()
    for s in STREAMS:
        legs[s][0].rest()
        spread(s, 1)
    for s in STREAMS:
        second_rest(s, 0)
    for s in STREAMS:
        legs[s][0].far_end()
        spread(s, 2)
    for s in STREAMS:
        legs[s][2].relay()
    for s in STREAMS:
        second_far(s, 0)
    for s in STREAMS:
        second_rest(s, 1)
    for s in STREAMS:
        legs[s][3].relay()
    for s in STREAMS:
        second_rest(s, 2)
    for s in STREAMS:
        second_far(s, 1)
    for s in STREAMS:
        second_far(s, 2)
    for d in range(RING):
        for gi in range(len(GROUPS)):
            for s in STREAMS:
                arrive(37 * s + 24 + 3 * d + gi, blk(s, d, GROUPS[gi], lanes_of[s], 1))
    for c in sent:
        c.wait_send()


def gather_tokens(x, grad_y, route_idx, gates):
    _, tok_dev, dm = x.shape
    top_k = gates.shape[2]
    width = 2 * dm + LANES
    hbm = pl.BlockSpec(memory_space=pltpu.HBM)
    vmem = pl.BlockSpec(memory_space=pltpu.VMEM)
    sems = pltpu.SemaphoreType.DMA((74,))
    args = (x, grad_y, jnp.transpose(route_idx, (2, 0, 1)), jnp.transpose(gates, (2, 0, 1)))
    return pl.pallas_call(
        gather_kernel,
        out_shape=pltpu.VMEM((2, RING, RING, 2, tok_dev, width), BF16),
        in_specs=[hbm] * 4,
        out_specs=vmem,
        scratch_shapes=[pltpu.VMEM((tok_dev, width), BF16), pltpu.VMEM((top_k, 2, tok_dev), jnp.int32), pltpu.VMEM((top_k, 2, tok_dev), F32),
                        sems, sems, pltpu.SemaphoreType.DMA((6,))],
        compiler_params=pltpu.CompilerParams(collective_id=0, has_side_effects=True, vmem_limit_bytes=COMM_VMEM),
        name="gather_tokens",
    )(*(pltpu.with_memory_space_constraint(v, pltpu.HBM) for v in args))


def reduce_kernel(dm, top_k, part_ref, y_ref, dx_ref, dg_ref, own, pair, full, half, last, pair_send, pair_recv,
                  ring_send, ring_recv, last_sem):
    here = Place()
    k, other = here.core, here.other
    lanes_of, halves = stream_lanes(part_ref.shape[5])
    sent = []

    def slot(s, d, i):
        return (d, i) if s == 0 else (i, d)

    def near_slot(s, d, i):
        return slot(s, NEAR.index(FAR[d]), NEAR.index(FAR[i]))

    def swap(s, d, i):
        lanes = lanes_of[s]
        return pltpu.make_async_remote_copy(src_ref=part_ref.at[(1,) + near_slot(s, d, i)].at[:, :, lanes],
                                            dst_ref=pair.at[slot(s, d, i)].at[:, :, lanes], send_sem=pair_send.at[s, d, i],
                                            recv_sem=pair_recv.at[s, d, i], device_id=here.partner, device_id_type=MESH)

    def move(s, f, kind, src, dst, axis):
        peer = here.peer(axis if s == 0 else 3 - axis, 1 if kind % 2 == 0 else -1)
        return pltpu.make_async_remote_copy(src_ref=src, dst_ref=dst, send_sem=ring_send.at[s, f, kind], recv_sem=ring_recv.at[s, f, kind],
                                            device_id=peer, device_id_type=MESH)

    def go(s, f, kind, src, dst, axis):
        c = move(s, f, kind, src, dst, axis)
        c.start()
        sent.append(c)

    def arrive(s, f, kind, dst):
        move(s, f, kind, dst, dst, 1).wait_recv()

    def own_ref(s, d, g, lanes):
        return own.at[slot(s, d, g)].at[:, :, :, lanes]

    def add_own(s, d, g, lanes, *vals):
        ix = slot(s, d, g) + (slice(None), slice(None), lanes)
        total = own[ix]
        for v in vals:
            total = total + v
        own[ix] = total

    def add_pair(s, d, gi):
        lanes = (slice(None), slice(None), lanes_of[s])
        for i in range(GROUPS[gi].start, GROUPS[gi].stop):
            swap(s, d, i).wait_recv()
            own[slot(s, d, i) + lanes] = part_ref[(0,) + near_slot(s, d, i) + lanes] + pair[slot(s, d, i) + lanes]

    def far(s, f, d, at, g, axis):
        for kind in range(2):
            lanes = halves[s][kind]
            go(s, f, kind, own_ref(s, d, at, lanes), half.at[g, :, :, lanes], axis)

    def near(s, f, spot, g, axis):
        for kind, step in ((0, 1), (1, -1)):
            lanes = halves[s][kind]
            arrive(s, f, kind, half.at[g, :, :, lanes])
            add_own(s, *spot(step), lanes, half[g, :, :, lanes])
        lanes = lanes_of[s]
        for kind, step in ((2, 1), (3, -1)):
            go(s, f, kind, own_ref(s, *spot(step), lanes), full.at[kind - 2, g, :, :, lanes], axis)

    def done(s, f, at, g):
        lanes = lanes_of[s]
        for n in range(2):
            arrive(s, f, 2 + n, full.at[n, g, :, :, lanes])
        add_own(s, 3, at, lanes, full[0, g, :, :, lanes], full[1, g, :, :, lanes])

    def far2(gi):
        for s in STREAMS:
            add_pair(s, 0, gi)
            far(s, gi, 0, GROUPS[gi], GROUPS[gi], 2)

    def near2(gi):
        for s in STREAMS:
            add_pair(s, 2, gi)
            add_pair(s, 1, gi)
        for s in STREAMS:
            near(s, gi, lambda step: (2 if step == 1 else 1, GROUPS[gi]), GROUPS[gi], 2)

    def done2(gi):
        for s in STREAMS:
            add_pair(s, 3, gi)
        for s in STREAMS:
            done(s, gi, GROUPS[gi], GROUPS[gi])

    order = [(0, 0), (0, 1), (0, 2), (2, 0), (1, 0), (0, 3), (2, 1), (2, 2), (1, 1), (1, 2), (3, 0), (2, 3), (1, 3), (3, 1), (3, 2), (3, 3)]
    here.barrier()
    for q in order:
        for s in STREAMS:
            c = swap(s, *q)
            c.start()
            sent.append(c)
    lone = slice(RING, RING + 1)
    far2(0)
    far2(1)
    near2(0)
    far2(2)
    near2(1)
    done2(0)
    for s in STREAMS:
        far(s, 3, 3, slice(0, 1), lone, 1)
    near2(2)
    done2(1)
    for s in STREAMS:
        near(s, 3, lambda step: (3, slice(2, 3) if step == 1 else slice(1, 2)), lone, 1)
    done2(2)
    for s in STREAMS:
        done(s, 3, slice(3, 4), lone)

    give = pltpu.make_async_remote_copy(src_ref=own.at[3, 3, other], dst_ref=last, send_sem=last_sem.at[0], recv_sem=last_sem.at[1],
                                        device_id=here.partner, device_id_type=MESH)
    give.start()
    sent.append(give)

    def emit(mb, val):
        y_ref[mb] = val[:, :dm].astype(BF16)
        dx_ref[mb] = val[:, dm:2 * dm].astype(BF16)
        dg_ref[mb] = val[:, 2 * dm:2 * dm + top_k]

    emit(k, own[3, 3, k])
    give.wait_recv()
    emit(other, last[...])
    for c in sent:
        c.wait_send()


def reduce_tokens(part, dm, top_k):
    _, _, _, cores, tok_dev, width = part.shape
    vmem = pl.BlockSpec(memory_space=pltpu.VMEM)
    block = (cores, tok_dev, width)
    ring_sems = pltpu.SemaphoreType.DMA((2, 4, 4))
    pair_sems = pltpu.SemaphoreType.DMA((2, RING, RING))
    return pl.pallas_call(
        functools.partial(reduce_kernel, dm, top_k),
        out_shape=(
            jax.ShapeDtypeStruct((2, tok_dev, dm), BF16),
            jax.ShapeDtypeStruct((2, tok_dev, dm), BF16),
            jax.ShapeDtypeStruct((2, tok_dev, top_k), F32),
        ),
        in_specs=[vmem],
        out_specs=(vmem, vmem, vmem),
        scratch_shapes=[
            pltpu.VMEM((RING, RING) + block, F32),
            pltpu.VMEM((RING, RING) + block, F32),
            pltpu.VMEM((2, RING + 1) + block, F32),
            pltpu.VMEM((RING + 1,) + block, F32),
            pltpu.VMEM((tok_dev, width), F32),
            pair_sems, pair_sems, ring_sems, ring_sems,
            pltpu.SemaphoreType.DMA((2,)),
        ],
        compiler_params=pltpu.CompilerParams(collective_id=1, has_side_effects=True, vmem_limit_bytes=COMM_VMEM),
        name="reduce_tokens",
    )(pltpu.with_memory_space_constraint(part, pltpu.VMEM))


def solution(mesh):
    group = mesh.shape["row"] * mesh.shape["col"] * mesh.shape["core"]
    tok_spec = P(None, ALL_AXES, None)
    w_spec = P(ALL_AXES, None, None)

    def moe_layer(x, route_idx, gates, w_gate, w_up, w_down, grad_y):
        _, tok_dev, dm = x.shape
        top_k = route_idx.shape[2]
        width = 2 * dm + LANES
        xd = gather_tokens(x, grad_y, route_idx, gates).reshape(2, group * tok_dev, width)
        part, g_gate, g_up, g_down = expert_stage(xd, w_gate, w_up, w_down, top_k, group * (tok_dev // 2))
        y, dx, dg = reduce_tokens(part.reshape(2, RING, RING, 2, tok_dev, width), dm, top_k)
        return y, dx, dg, g_gate, g_up, g_down

    return jax.shard_map(moe_layer, mesh=mesh, in_specs=(tok_spec, tok_spec, tok_spec, w_spec, w_spec, w_spec, tok_spec), out_specs=(tok_spec, tok_spec, tok_spec, w_spec, w_spec, w_spec), check_vma=False)
```

```python
import functools

import jax
import jax.numpy as jnp
from jax import lax
from jax.experimental import pallas as pl
from jax.experimental.pallas import tpu as pltpu
from jax.sharding import PartitionSpec as P

GROUP_AXES = ("row", "col", "core")
ALL_AXES = ("rep", "row", "col", "core")
F32 = jnp.float32
BF16 = jnp.bfloat16
LANES = 128
SMALL = 32
EXPERT_VMEM = 49_500_000
COMM_VMEM = 30_000_000


def dot_nn(a, b):
    return lax.dot_general(a, b, (((1,), (0,)), ((), ())), preferred_element_type=F32)


def dot_nt(a, b):
    return lax.dot_general(a, b, (((1,), (1,)), ((), ())), preferred_element_type=F32)


def dot_tn(a, b):
    return lax.dot_general(a, b, (((0,), (0,)), ((), ())), preferred_element_type=F32)


def split3(v):
    h1 = v.astype(BF16)
    r1 = v - h1.astype(F32)
    h2 = r1.astype(BF16)
    h3 = (r1 - h2.astype(F32)).astype(BF16)
    return h1, h2, h3


def col_blocks(width, step):
    return [(s, min(step, width - s)) for s in range(0, width, step)]


def expert_kernel(dims, xd_v, wg_hbm, wu_hbm, wd_hbm, acc_v, gg_hbm, gu_hbm, gd_hbm,
                  pt_v, gr_v, wgu_v, wd_v, og_v, ou_v, od_v, pos_v,
                  xt_v, qt_v, a_v, duv_v, cnt_s, base_s, big_s, sem_w, sem_o):
    tokens, dm, ff, el, top_k, seg = dims
    n_row, n_col, n_core = lax.axis_size("row"), lax.axis_size("col"), lax.axis_size("core")
    me = (lax.axis_index("row") * n_col + lax.axis_index("col")) * n_core + lax.axis_index("core")
    width = 2 * dm + LANES

    def load_w(e):
        pairs = ((wg_hbm, wgu_v.at[e, :, pl.ds(0, ff)]), (wu_hbm, wgu_v.at[e, :, pl.ds(ff, ff)]), (wd_hbm, wd_v.at[e]))
        return [pltpu.make_async_copy(h.at[e], v, sem_w.at[e, i]) for i, (h, v) in enumerate(pairs)]

    def store_g(e, slot):
        return [pltpu.make_async_copy(v.at[slot], h.at[e], sem_o.at[slot, i])
                for i, (h, v) in enumerate(((gg_hbm, og_v), (gu_hbm, ou_v), (gd_hbm, od_v)))]

    for e in range(el):
        for c in load_w(e):
            c.start()

    row_i = lax.broadcasted_iota(jnp.int32, (tokens, tokens), 0)
    col_i = lax.broadcasted_iota(jnp.int32, (tokens, tokens), 1)
    tri = (row_i < col_i).astype(F32).astype(BF16)
    sub = lax.broadcasted_iota(jnp.int32, (8, tokens), 0)
    eids = jnp.where(sub < el, (me * el + sub), -1).astype(F32)

    def chunks(total):
        return jnp.maximum((total + (seg - 1)) // seg, 1)

    n_bigs, n_small = [], []
    for m in range(2):
        meta_t = xd_v[m, :, 2 * dm:].astype(F32).T
        hits = jnp.zeros((8, tokens), F32)
        for j in range(top_k):
            hits = hits + (meta_t[j:j + 1, :] == eids).astype(F32)
        rank = dot_nn(hits.astype(BF16), tri)
        counts = [jnp.sum(hits[e:e + 1, :]).astype(jnp.int32) for e in range(el)]
        n_big = jnp.int32(0)
        for cnt in counts:
            n_big = n_big + (cnt > SMALL).astype(jnp.int32)
        big_at, total = jnp.int32(0), n_big * seg
        for e, cnt in enumerate(counts):
            is_big = cnt > SMALL
            base = jnp.where(is_big, big_at * seg, total)
            cnt_s[m, e] = cnt
            base_s[m, e] = base

            @pl.when(is_big)
            def _(m=m, e=e, big_at=big_at):
                big_s[m, big_at] = jnp.int32(e)

            pos_v[m, e:e + 1, :] = jnp.where(hits[e:e + 1, :] > 0, rank[e:e + 1, :] + base.astype(F32), -1.0)
            big_at = big_at + is_big.astype(jnp.int32)
            total = total + jnp.where(is_big, 0, (cnt + 15) // 16 * 16)
        n_bigs.append(n_big)
        n_small.append(jnp.maximum((total - n_big * seg + (LANES - 1)) // LANES, (n_big == 0).astype(jnp.int32)))
        n_ch = chunks(total)

        def gather(c, carry, m=m):
            off = pl.multiple_of(c * seg, seg)
            rows = (lax.broadcasted_iota(jnp.int32, (seg, tokens), 0) + off).astype(F32)
            pick = rows == pos_v[m, 0:1, :]
            for e in range(1, el):
                pick = pick | (rows == pos_v[m, e:e + 1, :])
            pick_f = pick.astype(F32)
            pt_v[m, :, pl.ds(off, seg)] = pick_f.T.astype(BF16)
            pick_b = pick_f.astype(BF16)
            for s, w in col_blocks(width, 512):
                gr_v[m, pl.ds(off, seg), s:s + w] = dot_nn(pick_b, xd_v[m, :, s:s + w]).astype(BF16)
            return carry

        lax.fori_loop(0, n_ch, gather, 0)

    def tile(e, slot, ra, rb, m_a, n_a, n_b, first):
        rows = ra + rb
        base_a = pl.multiple_of(base_s[m_a, e], 16)
        base_b = pl.multiple_of(base_s[1 - m_a, e], 16)
        it = lax.broadcasted_iota(jnp.int32, (rows, 1), 0)
        valid = ((it < ra) & (it < n_a)) | ((it >= ra) & (it - ra < n_b))

        def read(s, w):
            return jnp.concatenate([gr_v[m_a, pl.ds(base_a, ra), s:s + w],
                                    gr_v[1 - m_a, pl.ds(base_b, rb), s:s + w]], axis=0)

        def write(s, w, val):
            merged = jnp.where(valid, val.astype(F32), read(s, w).astype(F32)).astype(BF16)
            gr_v[m_a, pl.ds(base_a, ra), s:s + w] = merged[:ra]
            gr_v[1 - m_a, pl.ds(base_b, rb), s:s + w] = merged[ra:]

        lane = lax.broadcasted_iota(jnp.int32, (rows, LANES), 1)
        meta = jnp.where(valid, read(2 * dm, LANES).astype(F32), 0.0)
        eid = (me * el + e).astype(F32)
        mine = ((meta == eid) & (lane < top_k)).astype(F32)
        sel = pltpu.roll(mine, 8, 1) + pltpu.roll(mine, 16, 1) + pltpu.roll(mine, 24, 1)
        gate = jnp.where(valid, jnp.sum(meta * sel, axis=1, keepdims=True), 0.0)
        for s, w in col_blocks(dm, 256):
            xt_v[:rows, s:s + w] = jnp.where(valid, read(s, w).astype(F32), 0.0).astype(BF16)
            dy = jnp.where(valid, read(dm + s, w).astype(F32), 0.0)
            qt_v[:rows, s:s + w] = (gate * dy).astype(BF16)
        xt = xt_v[:rows, :]
        uv = dot_nn(xt, wgu_v[e]).astype(BF16).astype(F32)
        u, v = uv[:, :ff], uv[:, ff:]
        r = dot_nt(qt_v[:rows, :], wd_v[e])
        s_g = jax.nn.sigmoid(u)
        a_v[:rows, :] = (u * s_g * v).astype(BF16)
        duv_v[:rows, :ff] = (r * v * s_g * (1.0 + u * (1.0 - s_g))).astype(BF16)
        duv_v[:rows, ff:] = (r * u * s_g).astype(BF16)
        a = a_v[:rows, :]
        duv = duv_v[:rows, :]
        dots = jnp.zeros((rows, 1), F32)
        for s, w in col_blocks(dm, 256):
            o = dot_nn(a, wd_v[e, :, s:s + w]).astype(BF16)
            dy = jnp.where(valid, read(dm + s, w).astype(F32), 0.0)
            dots = dots + jnp.sum(dy * o.astype(F32), axis=1, keepdims=True)
            write(s, w, o)
        for s, w in col_blocks(dm, 256):
            write(dm + s, w, dot_nt(duv, wgu_v[e, s:s + w, :]).astype(BF16))
        d1, d2, d3 = split3(dots)
        g1, g2, g3 = split3(gate)
        new_meta = jnp.zeros((rows, LANES), F32)
        for at, val in ((e, d1), (8 + e, d2), (16 + e, d3), (32, g1), (33, g2), (34, g3)):
            new_meta = jnp.where(lane == at, val.astype(F32), new_meta)
        write(2 * dm, LANES, new_meta)

        def put(ref, idx, val):
            if first is None:
                ref[idx] = val
            else:
                ref[idx] = jnp.where(first, 0.0, ref[idx]) + val

        for s, w in col_blocks(dm, 256):
            g_in = dot_tn(xt_v[:rows, s:s + w], duv)
            put(og_v, (slot, slice(s, s + w)), g_in[:, :ff])
            put(ou_v, (slot, slice(s, s + w)), g_in[:, ff:])
        for s, w in col_blocks(dm, 256):
            put(od_v, (slot, slice(None), slice(s, s + w)), dot_tn(a, qt_v[:rows, s:s + w]))

    def expert(e, carry):
        slot = lax.rem(e, 2)
        for c in load_w(e):
            c.wait()

        @pl.when(e >= 2)
        def _():
            for c in store_g(e - 2, slot):
                c.wait()

        n0, n1 = cnt_s[0, e], cnt_s[1, e]
        big0, big1 = n0 > SMALL, n1 > SMALL

        @pl.when(jnp.logical_not(big0 | big1))
        def _():
            tile(e, slot, SMALL, SMALL, 0, n0, n1, None)

        @pl.when(big0 | big1)
        def _():
            both = big0 & big1

            def one(i, inner):
                m_a = jnp.where(both, i, jnp.where(big0, 0, 1))
                n_a = jnp.where(m_a == 0, n0, n1)
                n_b = jnp.where(both, 0, jnp.where(m_a == 0, n1, n0))
                tile(e, slot, seg, SMALL, m_a, n_a, n_b, i == 0)
                return inner

            lax.fori_loop(0, jnp.where(both, 2, 1), one, 0)

        for c in store_g(e, slot):
            c.start()

        return carry

    lax.fori_loop(0, el, expert, 0)

    for m in range(2):
        lane = lax.broadcasted_iota(jnp.int32, (tokens, LANES), 1)

        def put(s, w, first, add):
            acc_v[m, :, s:s + w] = jnp.where(first, 0.0, acc_v[m, :, s:s + w]) + add

        def back(pt, rows, first):
            for s, w in col_blocks(dm + LANES, 256):
                put(dm + s, w, first, dot_nn(pt, gr_v[m, rows, dm + s:dm + s + w]))

        def one_expert(j, carry):
            rows = pl.ds(pl.multiple_of(j * seg, seg), seg)
            pt = pt_v[m, :, rows]
            meta = xd_v[m, :, 2 * dm:].astype(F32)
            mine = ((meta == (me * el + big_s[m, j]).astype(F32)) & (lane < top_k)).astype(F32)
            sel = pltpu.roll(mine, 8, 1) + pltpu.roll(mine, 16, 1) + pltpu.roll(mine, 24, 1)
            gate = jnp.sum(meta * sel, axis=1, keepdims=True)
            for s, w in col_blocks(dm, 256):
                put(s, w, j == 0, gate * dot_nn(pt, gr_v[m, rows, s:s + w]))
            back(pt, rows, j == 0)
            return carry

        def several(c, carry):
            rows = pl.ds(pl.multiple_of(n_bigs[m] * seg + c * LANES, LANES), LANES)
            first = (c == 0) & (n_bigs[m] == 0)
            pt = pt_v[m, :, rows]
            pt2 = jnp.concatenate([pt, pt], axis=1)
            gp = gr_v[m, rows, 2 * dm:].astype(F32)
            gate = gp[:, 32:33] + gp[:, 33:34] + gp[:, 34:35]
            for s, w in col_blocks(dm, 256):
                h1, h2, h3 = split3(gate * gr_v[m, rows, s:s + w].astype(F32))
                put(s, w, first, dot_nn(pt2, jnp.concatenate([h1, h2], axis=0)) + dot_nn(pt, h3))
            back(pt, rows, first)
            return carry

        lax.fori_loop(0, n_bigs[m], one_expert, 0)
        lax.fori_loop(0, n_small[m], several, 0)
        ids = jnp.where(lane < top_k, xd_v[m, :, 2 * dm:].astype(F32), -1.0)
        raw = acc_v[m, :, 2 * dm:]
        out = jnp.zeros((tokens, LANES), F32)
        for e in range(el):
            val = raw[:, e:e + 1] + raw[:, 8 + e:9 + e] + raw[:, 16 + e:17 + e]
            out = jnp.where(ids == (me * el + e).astype(F32), val, out)
        acc_v[m, :, 2 * dm:] = out

    for e in range(el - 2, el):
        for c in store_g(e, e % 2):
            c.wait()


def expert_stage(xd, w_gate, w_up, w_down, top_k, seg):
    _, tokens, width = xd.shape
    el, dm, ff = w_gate.shape
    any_spec = pl.BlockSpec(memory_space=pltpu.HBM)
    vmem_spec = pl.BlockSpec(memory_space=pltpu.VMEM)
    rows_max = el * seg
    tile_rows = seg + SMALL
    dims = (tokens, dm, ff, el, top_k, seg)
    return pl.pallas_call(
        functools.partial(expert_kernel, dims),
        out_shape=(
            pltpu.VMEM((2, tokens, width), F32),
            pltpu.HBM((el, dm, ff), F32),
            pltpu.HBM((el, dm, ff), F32),
            pltpu.HBM((el, ff, dm), F32),
        ),
        in_specs=[vmem_spec] + [any_spec] * 3,
        out_specs=[vmem_spec] + [any_spec] * 3,
        scratch_shapes=[
            pltpu.VMEM((2, tokens, rows_max), BF16),
            pltpu.VMEM((2, rows_max, width), BF16),
            pltpu.VMEM((el, dm, 2 * ff), BF16),
            pltpu.VMEM((el, ff, dm), BF16),
            pltpu.VMEM((2, dm, ff), F32),
            pltpu.VMEM((2, dm, ff), F32),
            pltpu.VMEM((2, ff, dm), F32),
            pltpu.VMEM((2, 8, tokens), F32),
            pltpu.VMEM((tile_rows, dm), BF16),
            pltpu.VMEM((tile_rows, dm), BF16),
            pltpu.VMEM((tile_rows, ff), BF16),
            pltpu.VMEM((tile_rows, 2 * ff), BF16),
            pltpu.SMEM((2, 8), jnp.int32),
            pltpu.SMEM((2, 8), jnp.int32),
            pltpu.SMEM((2, 8), jnp.int32),
            pltpu.SemaphoreType.DMA((el, 3)),
            pltpu.SemaphoreType.DMA((2, 3)),
        ],
        compiler_params=pltpu.CompilerParams(vmem_limit_bytes=EXPERT_VMEM),
        name="experts",
    )(pltpu.with_memory_space_constraint(xd, pltpu.VMEM), *(pltpu.with_memory_space_constraint(w, pltpu.HBM) for w in (w_gate, w_up, w_down)))


RING = 4
NEAR = (0, -1, 1, 2)
FAR = (2, -1, 1, 0)
GROUPS = (slice(0, 1), slice(1, 3), slice(3, 4))
MESH = pl.DeviceIdType.MESH


class Place:
    def __init__(self):
        self.row, self.col, self.core = (lax.axis_index(a) for a in GROUP_AXES)
        self.n_row, self.n_col = lax.axis_size("row"), lax.axis_size("col")
        self.other = 1 - self.core
        self.partner = {"core": self.other}

    def spot(self, first, d1, d2):
        row = lax.rem(self.row + (d1 * first + d2 * (1 - first)) + self.n_row, self.n_row)
        col = lax.rem(self.col + (d1 * (1 - first) + d2 * first) + self.n_col, self.n_col)
        return row, col

    def peer(self, axis, d):
        row, col = self.spot(self.core, d, 0) if axis == 1 else self.spot(self.core, 0, d)
        return {"row": row, "col": col}

    def barrier(self):
        sem = pltpu.get_barrier_semaphore()
        peers = [self.peer(axis, d) for axis in (1, 2) for d in (1, -1)] + [self.partner]
        for peer in peers:
            pl.semaphore_signal(sem, inc=1, device_id=peer, device_id_type=MESH)
        pl.semaphore_wait(sem, len(peers))


STREAMS = range(2)


def half_lanes(start, size):
    mid = (size // LANES + 1) // 2 * LANES
    return ((start, mid), (start + mid, size - mid))


def stream_lanes(width):
    whole = half_lanes(0, width)
    return [pl.ds(*w) for w in whole], [[pl.ds(*h) for h in half_lanes(*w)] for w in whole]


def token_meta(route, gates):
    top_k, tok_dev = route.shape
    zero = jnp.zeros((8 - top_k, tok_dev), F32)
    parts = [route.astype(F32)] + [p.astype(F32) for p in split3(gates)]
    rows = jnp.concatenate([v for p in parts for v in (p, zero)], axis=0).astype(BF16)
    n = rows.shape[0]
    eye = (lax.broadcasted_iota(jnp.int32, (n, LANES), 0) == lax.broadcasted_iota(jnp.int32, (n, LANES), 1)).astype(F32).astype(BF16)
    return dot_tn(rows, eye).astype(BF16)


def gather_kernel(x_hbm, dy_hbm, route_hbm, gates_hbm, buf, stage, route_v, gates_v, send_sem, recv_sem, load_sem):
    here = Place()
    k, other = here.core, here.other
    dm = x_hbm.shape[2]
    lanes_of, halves = stream_lanes(2 * dm + LANES)
    sent = []

    def move(idx, src, dst, peer):
        return pltpu.make_async_remote_copy(src_ref=src, dst_ref=dst, send_sem=send_sem.at[idx], recv_sem=recv_sem.at[idx],
                                            device_id=peer, device_id_type=MESH)

    def send(idx, src, dst, peer):
        c = move(idx, src, dst, peer)
        c.start()
        sent.append(c)

    def arrive(idx, dst):
        move(idx, dst, dst, here.partner).wait_recv()

    def blk(s, d, g, lanes, side=0):
        ref = buf.at[side, d, g] if s == 0 else buf.at[side, g, d]
        return ref.at[:, :, :, lanes]

    def towards(s, axis, way):
        return here.peer(axis if s == 0 else 3 - axis, 1 - 2 * way)

    class Leg:
        def __init__(self, s, p):
            self.s, self.base, self.axis = s, 37 * s + 6 * p, 1 if p == 0 else 2
            self.at = (lambda j, lanes: blk(s, 0, slice(j, j + 1), lanes)) if p == 0 else (lambda j, lanes: blk(s, j, GROUPS[p - 1], lanes))

        def both_ways(self):
            for way in range(2):
                for n in range(2):
                    lanes = halves[self.s][way if n == 0 else 1 - way]
                    send(self.base + 2 * way + n, self.at(0, lanes), self.at(1 + way, lanes), towards(self.s, self.axis, way))

        def relay(self):
            for way in range(2):
                lanes = halves[self.s][way]
                arrive(self.base + 2 * way, self.at(1 + way, lanes))
                send(self.base + 4 + way, self.at(1 + way, lanes), self.at(3, lanes), towards(self.s, self.axis, way))

        def rest(self):
            for way in range(2):
                arrive(self.base + 2 * way + 1, self.at(1 + way, halves[self.s][1 - way]))

        def far_end(self):
            for way in range(2):
                arrive(self.base + 4 + way, self.at(3, halves[self.s][way]))

    legs = [[Leg(s, p) for p in range(4)] for s in STREAMS]

    def have(s, gi, d):
        lanes = lanes_of[s]
        send(37 * s + 24 + 3 * d + gi, blk(s, d, GROUPS[gi], lanes), blk(s, d, GROUPS[gi], lanes, 1), here.partner)

    def spread(s, gi):
        legs[s][1 + gi].both_ways()
        have(s, gi, 0)

    def second_rest(s, gi):
        legs[s][1 + gi].rest()
        have(s, gi, 1)
        have(s, gi, 2)

    def second_far(s, gi):
        legs[s][1 + gi].far_end()
        have(s, gi, 3)

    mine = buf.at[0, 0, 0, k]
    smalls = [pltpu.make_async_copy(route_hbm, route_v, load_sem.at[4]), pltpu.make_async_copy(gates_hbm, gates_v, load_sem.at[5])]
    loads = [pltpu.make_async_copy(h.at[mb], dst.at[:, pl.ds(lo, dm)], load_sem.at[n])
             for n, (h, mb, dst, lo) in enumerate(((x_hbm, other, stage, 0), (dy_hbm, other, stage, dm), (x_hbm, k, mine, 0), (dy_hbm, k, mine, dm)))]
    for c in smalls + loads:
        c.start()
    for c in smalls:
        c.wait()
    metas = [token_meta(route_v[:, m, :], gates_v[:, m, :]) for m in range(2)]
    zero_core = k == 0
    stage[:, 2 * dm:] = jnp.where(zero_core, metas[1].astype(F32), metas[0].astype(F32)).astype(BF16)
    buf[0, 0, 0, k, :, 2 * dm:] = jnp.where(zero_core, metas[0].astype(F32), metas[1].astype(F32)).astype(BF16)
    here.barrier()
    for c in loads:
        c.wait()
    send(36, stage, buf.at[0, 0, 0, k], here.partner)
    arrive(36, buf.at[0, 0, 0, other])
    for s in STREAMS:
        legs[s][0].both_ways()
    for s in STREAMS:
        spread(s, 0)
    for s in STREAMS:
        legs[s][0].relay()
    for s in STREAMS:
        legs[s][1].relay()
    for s in STREAMS:
        legs[s][0].rest()
        spread(s, 1)
    for s in STREAMS:
        second_rest(s, 0)
    for s in STREAMS:
        legs[s][0].far_end()
        spread(s, 2)
    for s in STREAMS:
        legs[s][2].relay()
    for s in STREAMS:
        second_far(s, 0)
    for s in STREAMS:
        second_rest(s, 1)
    for s in STREAMS:
        legs[s][3].relay()
    for s in STREAMS:
        second_rest(s, 2)
    for s in STREAMS:
        second_far(s, 1)
    for s in STREAMS:
        second_far(s, 2)
    for d in range(RING):
        for gi in range(len(GROUPS)):
            for s in STREAMS:
                arrive(37 * s + 24 + 3 * d + gi, blk(s, d, GROUPS[gi], lanes_of[s], 1))
    for c in sent:
        c.wait_send()


def gather_tokens(x, grad_y, route_idx, gates):
    _, tok_dev, dm = x.shape
    top_k = gates.shape[2]
    width = 2 * dm + LANES
    hbm = pl.BlockSpec(memory_space=pltpu.HBM)
    vmem = pl.BlockSpec(memory_space=pltpu.VMEM)
    sems = pltpu.SemaphoreType.DMA((74,))
    args = (x, grad_y, jnp.transpose(route_idx, (2, 0, 1)), jnp.transpose(gates, (2, 0, 1)))
    return pl.pallas_call(
        gather_kernel,
        out_shape=pltpu.VMEM((2, RING, RING, 2, tok_dev, width), BF16),
        in_specs=[hbm] * 4,
        out_specs=vmem,
        scratch_shapes=[pltpu.VMEM((tok_dev, width), BF16), pltpu.VMEM((top_k, 2, tok_dev), jnp.int32), pltpu.VMEM((top_k, 2, tok_dev), F32),
                        sems, sems, pltpu.SemaphoreType.DMA((6,))],
        compiler_params=pltpu.CompilerParams(collective_id=0, has_side_effects=True, vmem_limit_bytes=COMM_VMEM),
        name="gather_tokens",
    )(*(pltpu.with_memory_space_constraint(v, pltpu.HBM) for v in args))


def reduce_kernel(dm, top_k, part_ref, y_ref, dx_ref, dg_ref, own, pair, full, half, last, pair_send, pair_recv,
                  ring_send, ring_recv, last_sem):
    here = Place()
    k, other = here.core, here.other
    lanes_of, halves = stream_lanes(part_ref.shape[5])
    sent = []

    def slot(s, d, i):
        return (d, i) if s == 0 else (i, d)

    def near_slot(s, d, i):
        return slot(s, NEAR.index(FAR[d]), NEAR.index(FAR[i]))

    def swap(s, d, i):
        lanes = lanes_of[s]
        return pltpu.make_async_remote_copy(src_ref=part_ref.at[(1,) + near_slot(s, d, i)].at[:, :, lanes],
                                            dst_ref=pair.at[slot(s, d, i)].at[:, :, lanes], send_sem=pair_send.at[s, d, i],
                                            recv_sem=pair_recv.at[s, d, i], device_id=here.partner, device_id_type=MESH)

    def move(s, f, kind, src, dst, axis):
        peer = here.peer(axis if s == 0 else 3 - axis, 1 if kind % 2 == 0 else -1)
        return pltpu.make_async_remote_copy(src_ref=src, dst_ref=dst, send_sem=ring_send.at[s, f, kind], recv_sem=ring_recv.at[s, f, kind],
                                            device_id=peer, device_id_type=MESH)

    def go(s, f, kind, src, dst, axis):
        c = move(s, f, kind, src, dst, axis)
        c.start()
        sent.append(c)

    def arrive(s, f, kind, dst):
        move(s, f, kind, dst, dst, 1).wait_recv()

    def own_ref(s, d, g, lanes):
        return own.at[slot(s, d, g)].at[:, :, :, lanes]

    def add_own(s, d, g, lanes, *vals):
        ix = slot(s, d, g) + (slice(None), slice(None), lanes)
        total = own[ix]
        for v in vals:
            total = total + v
        own[ix] = total

    def add_pair(s, d, gi):
        lanes = (slice(None), slice(None), lanes_of[s])
        for i in range(GROUPS[gi].start, GROUPS[gi].stop):
            swap(s, d, i).wait_recv()
            own[slot(s, d, i) + lanes] = part_ref[(0,) + near_slot(s, d, i) + lanes] + pair[slot(s, d, i) + lanes]

    def far(s, f, d, at, g, axis):
        for kind in range(2):
            lanes = halves[s][kind]
            go(s, f, kind, own_ref(s, d, at, lanes), half.at[g, :, :, lanes], axis)

    def near(s, f, spot, g, axis):
        for kind, step in ((0, 1), (1, -1)):
            lanes = halves[s][kind]
            arrive(s, f, kind, half.at[g, :, :, lanes])
            add_own(s, *spot(step), lanes, half[g, :, :, lanes])
        lanes = lanes_of[s]
        for kind, step in ((2, 1), (3, -1)):
            go(s, f, kind, own_ref(s, *spot(step), lanes), full.at[kind - 2, g, :, :, lanes], axis)

    def done(s, f, at, g):
        lanes = lanes_of[s]
        for n in range(2):
            arrive(s, f, 2 + n, full.at[n, g, :, :, lanes])
        add_own(s, 3, at, lanes, full[0, g, :, :, lanes], full[1, g, :, :, lanes])

    def far2(gi):
        for s in STREAMS:
            add_pair(s, 0, gi)
            far(s, gi, 0, GROUPS[gi], GROUPS[gi], 2)

    def near2(gi):
        for s in STREAMS:
            add_pair(s, 2, gi)
            add_pair(s, 1, gi)
        for s in STREAMS:
            near(s, gi, lambda step: (2 if step == 1 else 1, GROUPS[gi]), GROUPS[gi], 2)

    def done2(gi):
        for s in STREAMS:
            add_pair(s, 3, gi)
        for s in STREAMS:
            done(s, gi, GROUPS[gi], GROUPS[gi])

    order = [(0, 0), (0, 1), (0, 2), (2, 0), (1, 0), (0, 3), (2, 1), (2, 2), (1, 1), (1, 2), (3, 0), (2, 3), (1, 3), (3, 1), (3, 2), (3, 3)]
    here.barrier()
    for q in order:
        for s in STREAMS:
            c = swap(s, *q)
            c.start()
            sent.append(c)
    lone = slice(RING, RING + 1)
    far2(0)
    far2(1)
    near2(0)
    far2(2)
    near2(1)
    done2(0)
    for s in STREAMS:
        far(s, 3, 3, slice(0, 1), lone, 1)
    near2(2)
    done2(1)
    for s in STREAMS:
        near(s, 3, lambda step: (3, slice(2, 3) if step == 1 else slice(1, 2)), lone, 1)
    done2(2)
    for s in STREAMS:
        done(s, 3, slice(3, 4), lone)

    give = pltpu.make_async_remote_copy(src_ref=own.at[3, 3, other], dst_ref=last, send_sem=last_sem.at[0], recv_sem=last_sem.at[1],
                                        device_id=here.partner, device_id_type=MESH)
    give.start()
    sent.append(give)

    def emit(mb, val):
        y_ref[mb] = val[:, :dm].astype(BF16)
        dx_ref[mb] = val[:, dm:2 * dm].astype(BF16)
        dg_ref[mb] = val[:, 2 * dm:2 * dm + top_k]

    emit(k, own[3, 3, k])
    give.wait_recv()
    emit(other, last[...])
    for c in sent:
        c.wait_send()


def reduce_tokens(part, dm, top_k):
    _, _, _, cores, tok_dev, width = part.shape
    vmem = pl.BlockSpec(memory_space=pltpu.VMEM)
    block = (cores, tok_dev, width)
    ring_sems = pltpu.SemaphoreType.DMA((2, 4, 4))
    pair_sems = pltpu.SemaphoreType.DMA((2, RING, RING))
    return pl.pallas_call(
        functools.partial(reduce_kernel, dm, top_k),
        out_shape=(
            jax.ShapeDtypeStruct((2, tok_dev, dm), BF16),
            jax.ShapeDtypeStruct((2, tok_dev, dm), BF16),
            jax.ShapeDtypeStruct((2, tok_dev, top_k), F32),
        ),
        in_specs=[vmem],
        out_specs=(vmem, vmem, vmem),
        scratch_shapes=[
            pltpu.VMEM((RING, RING) + block, F32),
            pltpu.VMEM((RING, RING) + block, F32),
            pltpu.VMEM((2, RING + 1) + block, F32),
            pltpu.VMEM((RING + 1,) + block, F32),
            pltpu.VMEM((tok_dev, width), F32),
            pair_sems, pair_sems, ring_sems, ring_sems,
            pltpu.SemaphoreType.DMA((2,)),
        ],
        compiler_params=pltpu.CompilerParams(collective_id=1, has_side_effects=True, vmem_limit_bytes=COMM_VMEM),
        name="reduce_tokens",
    )(pltpu.with_memory_space_constraint(part, pltpu.VMEM))


def solution(mesh):
    group = mesh.shape["row"] * mesh.shape["col"] * mesh.shape["core"]
    tok_spec = P(None, ALL_AXES, None)
    w_spec = P(ALL_AXES, None, None)

    def moe_layer(x, route_idx, gates, w_gate, w_up, w_down, grad_y):
        _, tok_dev, dm = x.shape
        top_k = route_idx.shape[2]
        width = 2 * dm + LANES
        xd = gather_tokens(x, grad_y, route_idx, gates).reshape(2, group * tok_dev, width)
        part, g_gate, g_up, g_down = expert_stage(xd, w_gate, w_up, w_down, top_k, group * (tok_dev // 2))
        y, dx, dg = reduce_tokens(part.reshape(2, RING, RING, 2, tok_dev, width), dm, top_k)
        return y, dx, dg, g_gate, g_up, g_down

    return jax.shard_map(moe_layer, mesh=mesh, in_specs=(tok_spec, tok_spec, tok_spec, w_spec, w_spec, w_spec, tok_spec), out_specs=(tok_spec, tok_spec, tok_spec, w_spec, w_spec, w_spec), check_vma=False)
```

```python
import functools

import jax
import jax.numpy as jnp
from jax import lax
from jax.experimental import pallas as pl
from jax.experimental.pallas import tpu as pltpu
from jax.sharding import PartitionSpec as P

GROUP_AXES = ("row", "col", "core")
ALL_AXES = ("rep", "row", "col", "core")
F32 = jnp.float32
BF16 = jnp.bfloat16
LANES = 128
SMALL = 32
EXPERT_VMEM = 49_500_000
COMM_VMEM = 30_000_000


def dot_nn(a, b):
    return lax.dot_general(a, b, (((1,), (0,)), ((), ())), preferred_element_type=F32)


def dot_nt(a, b):
    return lax.dot_general(a, b, (((1,), (1,)), ((), ())), preferred_element_type=F32)


def dot_tn(a, b):
    return lax.dot_general(a, b, (((0,), (0,)), ((), ())), preferred_element_type=F32)


def split3(v):
    h1 = v.astype(BF16)
    r1 = v - h1.astype(F32)
    h2 = r1.astype(BF16)
    h3 = (r1 - h2.astype(F32)).astype(BF16)
    return h1, h2, h3


def col_blocks(width, step):
    return [(s, min(step, width - s)) for s in range(0, width, step)]


def expert_kernel(dims, xd_v, wg_hbm, wu_hbm, wd_hbm, acc_v, gg_hbm, gu_hbm, gd_hbm,
                  pt_v, gr_v, wgu_v, wd_v, og_v, ou_v, od_v, pos_v,
                  xt_v, qt_v, a_v, duv_v, cnt_s, base_s, big_s, sem_w, sem_o):
    tokens, dm, ff, el, top_k, seg = dims
    n_row, n_col, n_core = lax.axis_size("row"), lax.axis_size("col"), lax.axis_size("core")
    me = (lax.axis_index("row") * n_col + lax.axis_index("col")) * n_core + lax.axis_index("core")
    width = 2 * dm + LANES

    def load_w(e):
        pairs = ((wg_hbm, wgu_v.at[e, :, pl.ds(0, ff)]), (wu_hbm, wgu_v.at[e, :, pl.ds(ff, ff)]), (wd_hbm, wd_v.at[e]))
        return [pltpu.make_async_copy(h.at[e], v, sem_w.at[e, i]) for i, (h, v) in enumerate(pairs)]

    def store_g(e, slot):
        return [pltpu.make_async_copy(v.at[slot], h.at[e], sem_o.at[slot, i])
                for i, (h, v) in enumerate(((gg_hbm, og_v), (gu_hbm, ou_v), (gd_hbm, od_v)))]

    def start_w(lo, hi):
        for e in range(lo, hi):
            for c in load_w(e):
                c.start()

    start_w(0, 1)

    row_i = lax.broadcasted_iota(jnp.int32, (tokens, tokens), 0)
    col_i = lax.broadcasted_iota(jnp.int32, (tokens, tokens), 1)
    tri = (row_i < col_i).astype(F32).astype(BF16)
    sub = lax.broadcasted_iota(jnp.int32, (8, tokens), 0)
    eids = jnp.where(sub < el, (me * el + sub), -1).astype(F32)

    def chunks(total):
        return jnp.maximum((total + (seg - 1)) // seg, 1)

    n_bigs, n_small = [], []
    for m in range(2):
        meta_t = xd_v[m, :, 2 * dm:].astype(F32).T
        hits = jnp.zeros((8, tokens), F32)
        for j in range(top_k):
            hits = hits + (meta_t[j:j + 1, :] == eids).astype(F32)
        rank = dot_nn(hits.astype(BF16), tri)
        counts = [jnp.sum(hits[e:e + 1, :]).astype(jnp.int32) for e in range(el)]
        n_big = jnp.int32(0)
        for cnt in counts:
            n_big = n_big + (cnt > SMALL).astype(jnp.int32)
        big_at, total = jnp.int32(0), n_big * seg
        for e, cnt in enumerate(counts):
            is_big = cnt > SMALL
            base = jnp.where(is_big, big_at * seg, total)
            cnt_s[m, e] = cnt
            base_s[m, e] = base

            @pl.when(is_big)
            def _(m=m, e=e, big_at=big_at):
                big_s[m, big_at] = jnp.int32(e)

            pos_v[m, e:e + 1, :] = jnp.where(hits[e:e + 1, :] > 0, rank[e:e + 1, :] + base.astype(F32), -1.0)
            big_at = big_at + is_big.astype(jnp.int32)
            total = total + jnp.where(is_big, 0, (cnt + 15) // 16 * 16)
        n_bigs.append(n_big)
        n_small.append(jnp.maximum((total - n_big * seg + (LANES - 1)) // LANES, (n_big == 0).astype(jnp.int32)))
        n_ch = chunks(total)

        def gather(c, carry, m=m):
            off = pl.multiple_of(c * seg, seg)
            rows = (lax.broadcasted_iota(jnp.int32, (seg, tokens), 0) + off).astype(F32)
            pick = rows == pos_v[m, 0:1, :]
            for e in range(1, el):
                pick = pick | (rows == pos_v[m, e:e + 1, :])
            pick_f = pick.astype(F32)
            pt_v[m, :, pl.ds(off, seg)] = pick_f.T.astype(BF16)
            pick_b = pick_f.astype(BF16)
            for s, w in col_blocks(width, 512):
                gr_v[m, pl.ds(off, seg), s:s + w] = dot_nn(pick_b, xd_v[m, :, s:s + w]).astype(BF16)
            return carry

        start_w(1 + m, 2 + m)
        lax.fori_loop(0, n_ch, gather, 0)
    start_w(3, el)

    def tile(e, slot, ra, rb, m_a, n_a, n_b, first):
        rows = ra + rb
        base_a = pl.multiple_of(base_s[m_a, e], 16)
        base_b = pl.multiple_of(base_s[1 - m_a, e], 16)
        it = lax.broadcasted_iota(jnp.int32, (rows, 1), 0)
        valid = ((it < ra) & (it < n_a)) | ((it >= ra) & (it - ra < n_b))

        def read(s, w):
            return jnp.concatenate([gr_v[m_a, pl.ds(base_a, ra), s:s + w],
                                    gr_v[1 - m_a, pl.ds(base_b, rb), s:s + w]], axis=0)

        def write(s, w, val):
            merged = jnp.where(valid, val.astype(F32), read(s, w).astype(F32)).astype(BF16)
            gr_v[m_a, pl.ds(base_a, ra), s:s + w] = merged[:ra]
            gr_v[1 - m_a, pl.ds(base_b, rb), s:s + w] = merged[ra:]

        lane = lax.broadcasted_iota(jnp.int32, (rows, LANES), 1)
        meta = jnp.where(valid, read(2 * dm, LANES).astype(F32), 0.0)
        eid = (me * el + e).astype(F32)
        mine = ((meta == eid) & (lane < top_k)).astype(F32)
        sel = pltpu.roll(mine, 8, 1) + pltpu.roll(mine, 16, 1) + pltpu.roll(mine, 24, 1)
        gate = jnp.where(valid, jnp.sum(meta * sel, axis=1, keepdims=True), 0.0)
        for s, w in col_blocks(dm, 256):
            xt_v[:rows, s:s + w] = jnp.where(valid, read(s, w).astype(F32), 0.0).astype(BF16)
            dy = jnp.where(valid, read(dm + s, w).astype(F32), 0.0)
            qt_v[:rows, s:s + w] = (gate * dy).astype(BF16)
        xt = xt_v[:rows, :]
        uv = dot_nn(xt, wgu_v[e]).astype(BF16).astype(F32)
        u, v = uv[:, :ff], uv[:, ff:]
        r = dot_nt(qt_v[:rows, :], wd_v[e])
        s_g = jax.nn.sigmoid(u)
        a_v[:rows, :] = (u * s_g * v).astype(BF16)
        duv_v[:rows, :ff] = (r * v * s_g * (1.0 + u * (1.0 - s_g))).astype(BF16)
        duv_v[:rows, ff:] = (r * u * s_g).astype(BF16)
        a = a_v[:rows, :]
        duv = duv_v[:rows, :]
        dots = jnp.zeros((rows, 1), F32)
        for s, w in col_blocks(dm, 256):
            o = dot_nn(a, wd_v[e, :, s:s + w]).astype(BF16)
            dy = jnp.where(valid, read(dm + s, w).astype(F32), 0.0)
            dots = dots + jnp.sum(dy * o.astype(F32), axis=1, keepdims=True)
            write(s, w, o)
        for s, w in col_blocks(dm, 256):
            write(dm + s, w, dot_nt(duv, wgu_v[e, s:s + w, :]).astype(BF16))
        d1, d2, d3 = split3(dots)
        g1, g2, g3 = split3(gate)
        new_meta = jnp.zeros((rows, LANES), F32)
        for at, val in ((e, d1), (8 + e, d2), (16 + e, d3), (32, g1), (33, g2), (34, g3)):
            new_meta = jnp.where(lane == at, val.astype(F32), new_meta)
        write(2 * dm, LANES, new_meta)

        def put(ref, idx, val):
            if first is None:
                ref[idx] = val
            else:
                ref[idx] = jnp.where(first, 0.0, ref[idx]) + val

        for s, w in col_blocks(dm, 256):
            g_in = dot_tn(xt_v[:rows, s:s + w], duv)
            put(og_v, (slot, slice(s, s + w)), g_in[:, :ff])
            put(ou_v, (slot, slice(s, s + w)), g_in[:, ff:])
        for s, w in col_blocks(dm, 256):
            put(od_v, (slot, slice(None), slice(s, s + w)), dot_tn(a, qt_v[:rows, s:s + w]))

    def expert(e, carry):
        slot = lax.rem(e, 2)
        for c in load_w(e):
            c.wait()

        @pl.when(e >= 2)
        def _():
            for c in store_g(e - 2, slot):
                c.wait()

        n0, n1 = cnt_s[0, e], cnt_s[1, e]
        big0, big1 = n0 > SMALL, n1 > SMALL

        @pl.when(jnp.logical_not(big0 | big1))
        def _():
            tile(e, slot, SMALL, SMALL, 0, n0, n1, None)

        @pl.when(big0 | big1)
        def _():
            both = big0 & big1

            def one(i, inner):
                m_a = jnp.where(both, i, jnp.where(big0, 0, 1))
                n_a = jnp.where(m_a == 0, n0, n1)
                n_b = jnp.where(both, 0, jnp.where(m_a == 0, n1, n0))
                tile(e, slot, seg, SMALL, m_a, n_a, n_b, i == 0)
                return inner

            lax.fori_loop(0, jnp.where(both, 2, 1), one, 0)

        for c in store_g(e, slot):
            c.start()

        return carry

    lax.fori_loop(0, el, expert, 0)

    for m in range(2):
        lane = lax.broadcasted_iota(jnp.int32, (tokens, LANES), 1)

        def put(s, w, first, add):
            acc_v[m, :, s:s + w] = jnp.where(first, 0.0, acc_v[m, :, s:s + w]) + add

        def back(pt, rows, first):
            for s, w in col_blocks(dm + LANES, 256):
                put(dm + s, w, first, dot_nn(pt, gr_v[m, rows, dm + s:dm + s + w]))

        def one_expert(j, carry):
            rows = pl.ds(pl.multiple_of(j * seg, seg), seg)
            pt = pt_v[m, :, rows]
            meta = xd_v[m, :, 2 * dm:].astype(F32)
            mine = ((meta == (me * el + big_s[m, j]).astype(F32)) & (lane < top_k)).astype(F32)
            sel = pltpu.roll(mine, 8, 1) + pltpu.roll(mine, 16, 1) + pltpu.roll(mine, 24, 1)
            gate = jnp.sum(meta * sel, axis=1, keepdims=True)
            for s, w in col_blocks(dm, 256):
                put(s, w, j == 0, gate * dot_nn(pt, gr_v[m, rows, s:s + w]))
            back(pt, rows, j == 0)
            return carry

        def several(c, carry):
            rows = pl.ds(pl.multiple_of(n_bigs[m] * seg + c * LANES, LANES), LANES)
            first = (c == 0) & (n_bigs[m] == 0)
            pt = pt_v[m, :, rows]
            pt2 = jnp.concatenate([pt, pt], axis=1)
            gp = gr_v[m, rows, 2 * dm:].astype(F32)
            gate = gp[:, 32:33] + gp[:, 33:34] + gp[:, 34:35]
            for s, w in col_blocks(dm, 256):
                h1, h2, h3 = split3(gate * gr_v[m, rows, s:s + w].astype(F32))
                put(s, w, first, dot_nn(pt2, jnp.concatenate([h1, h2], axis=0)) + dot_nn(pt, h3))
            back(pt, rows, first)
            return carry

        lax.fori_loop(0, n_bigs[m], one_expert, 0)
        lax.fori_loop(0, n_small[m], several, 0)
        ids = jnp.where(lane < top_k, xd_v[m, :, 2 * dm:].astype(F32), -1.0)
        raw = acc_v[m, :, 2 * dm:]
        out = jnp.zeros((tokens, LANES), F32)
        for e in range(el):
            val = raw[:, e:e + 1] + raw[:, 8 + e:9 + e] + raw[:, 16 + e:17 + e]
            out = jnp.where(ids == (me * el + e).astype(F32), val, out)
        acc_v[m, :, 2 * dm:] = out

    for e in range(el - 2, el):
        for c in store_g(e, e % 2):
            c.wait()


def expert_stage(xd, w_gate, w_up, w_down, top_k, seg):
    _, tokens, width = xd.shape
    el, dm, ff = w_gate.shape
    any_spec = pl.BlockSpec(memory_space=pltpu.HBM)
    vmem_spec = pl.BlockSpec(memory_space=pltpu.VMEM)
    rows_max = el * seg
    tile_rows = seg + SMALL
    dims = (tokens, dm, ff, el, top_k, seg)
    return pl.pallas_call(
        functools.partial(expert_kernel, dims),
        out_shape=(
            pltpu.VMEM((2, tokens, width), F32),
            pltpu.HBM((el, dm, ff), F32),
            pltpu.HBM((el, dm, ff), F32),
            pltpu.HBM((el, ff, dm), F32),
        ),
        in_specs=[vmem_spec] + [any_spec] * 3,
        out_specs=[vmem_spec] + [any_spec] * 3,
        scratch_shapes=[
            pltpu.VMEM((2, tokens, rows_max), BF16),
            pltpu.VMEM((2, rows_max, width), BF16),
            pltpu.VMEM((el, dm, 2 * ff), BF16),
            pltpu.VMEM((el, ff, dm), BF16),
            pltpu.VMEM((2, dm, ff), F32),
            pltpu.VMEM((2, dm, ff), F32),
            pltpu.VMEM((2, ff, dm), F32),
            pltpu.VMEM((2, 8, tokens), F32),
            pltpu.VMEM((tile_rows, dm), BF16),
            pltpu.VMEM((tile_rows, dm), BF16),
            pltpu.VMEM((tile_rows, ff), BF16),
            pltpu.VMEM((tile_rows, 2 * ff), BF16),
            pltpu.SMEM((2, 8), jnp.int32),
            pltpu.SMEM((2, 8), jnp.int32),
            pltpu.SMEM((2, 8), jnp.int32),
            pltpu.SemaphoreType.DMA((el, 3)),
            pltpu.SemaphoreType.DMA((2, 3)),
        ],
        compiler_params=pltpu.CompilerParams(vmem_limit_bytes=EXPERT_VMEM),
        name="experts",
    )(pltpu.with_memory_space_constraint(xd, pltpu.VMEM), *(pltpu.with_memory_space_constraint(w, pltpu.HBM) for w in (w_gate, w_up, w_down)))


RING = 4
NEAR = (0, -1, 1, 2)
FAR = (2, -1, 1, 0)
GROUPS = (slice(0, 1), slice(1, 3), slice(3, 4))
MESH = pl.DeviceIdType.MESH


class Place:
    def __init__(self):
        self.row, self.col, self.core = (lax.axis_index(a) for a in GROUP_AXES)
        self.n_row, self.n_col = lax.axis_size("row"), lax.axis_size("col")
        self.other = 1 - self.core
        self.partner = {"core": self.other}

    def spot(self, first, d1, d2):
        row = lax.rem(self.row + (d1 * first + d2 * (1 - first)) + self.n_row, self.n_row)
        col = lax.rem(self.col + (d1 * (1 - first) + d2 * first) + self.n_col, self.n_col)
        return row, col

    def peer(self, axis, d):
        row, col = self.spot(self.core, d, 0) if axis == 1 else self.spot(self.core, 0, d)
        return {"row": row, "col": col}

    def barrier(self):
        sem = pltpu.get_barrier_semaphore()
        peers = [self.peer(axis, d) for axis in (1, 2) for d in (1, -1)] + [self.partner]
        for peer in peers:
            pl.semaphore_signal(sem, inc=1, device_id=peer, device_id_type=MESH)
        pl.semaphore_wait(sem, len(peers))


STREAMS = range(2)


def half_lanes(start, size):
    mid = (size // LANES + 1) // 2 * LANES
    return ((start, mid), (start + mid, size - mid))


def stream_lanes(width):
    whole = half_lanes(0, width)
    return [pl.ds(*w) for w in whole], [[pl.ds(*h) for h in half_lanes(*w)] for w in whole]


def token_meta(route, gates):
    top_k, tok_dev = route.shape
    zero = jnp.zeros((8 - top_k, tok_dev), F32)
    parts = [route.astype(F32)] + [p.astype(F32) for p in split3(gates)]
    rows = jnp.concatenate([v for p in parts for v in (p, zero)], axis=0).astype(BF16)
    n = rows.shape[0]
    eye = (lax.broadcasted_iota(jnp.int32, (n, LANES), 0) == lax.broadcasted_iota(jnp.int32, (n, LANES), 1)).astype(F32).astype(BF16)
    return dot_tn(rows, eye).astype(BF16)


def gather_kernel(x_hbm, dy_hbm, route_hbm, gates_hbm, buf, stage, route_v, gates_v, send_sem, recv_sem, load_sem):
    here = Place()
    k, other = here.core, here.other
    dm = x_hbm.shape[2]
    lanes_of, halves = stream_lanes(2 * dm + LANES)
    sent = []

    def move(idx, src, dst, peer):
        return pltpu.make_async_remote_copy(src_ref=src, dst_ref=dst, send_sem=send_sem.at[idx], recv_sem=recv_sem.at[idx],
                                            device_id=peer, device_id_type=MESH)

    def send(idx, src, dst, peer):
        c = move(idx, src, dst, peer)
        c.start()
        sent.append(c)

    def arrive(idx, dst):
        move(idx, dst, dst, here.partner).wait_recv()

    def blk(s, d, g, lanes, side=0):
        ref = buf.at[side, d, g] if s == 0 else buf.at[side, g, d]
        return ref.at[:, :, :, lanes]

    def towards(s, axis, way):
        return here.peer(axis if s == 0 else 3 - axis, 1 - 2 * way)

    class Leg:
        def __init__(self, s, p):
            self.s, self.base, self.axis = s, 37 * s + 6 * p, 1 if p == 0 else 2
            self.at = (lambda j, lanes: blk(s, 0, slice(j, j + 1), lanes)) if p == 0 else (lambda j, lanes: blk(s, j, GROUPS[p - 1], lanes))

        def both_ways(self):
            for way in range(2):
                for n in range(2):
                    lanes = halves[self.s][way if n == 0 else 1 - way]
                    send(self.base + 2 * way + n, self.at(0, lanes), self.at(1 + way, lanes), towards(self.s, self.axis, way))

        def relay(self):
            for way in range(2):
                lanes = halves[self.s][way]
                arrive(self.base + 2 * way, self.at(1 + way, lanes))
                send(self.base + 4 + way, self.at(1 + way, lanes), self.at(3, lanes), towards(self.s, self.axis, way))

        def rest(self):
            for way in range(2):
                arrive(self.base + 2 * way + 1, self.at(1 + way, halves[self.s][1 - way]))

        def far_end(self):
            for way in range(2):
                arrive(self.base + 4 + way, self.at(3, halves[self.s][way]))

    legs = [[Leg(s, p) for p in range(4)] for s in STREAMS]

    def have(s, gi, d):
        lanes = lanes_of[s]
        send(37 * s + 24 + 3 * d + gi, blk(s, d, GROUPS[gi], lanes), blk(s, d, GROUPS[gi], lanes, 1), here.partner)

    def spread(s, gi):
        legs[s][1 + gi].both_ways()
        have(s, gi, 0)

    def second_rest(s, gi):
        legs[s][1 + gi].rest()
        have(s, gi, 1)
        have(s, gi, 2)

    def second_far(s, gi):
        legs[s][1 + gi].far_end()
        have(s, gi, 3)

    mine = buf.at[0, 0, 0, k]
    smalls = [pltpu.make_async_copy(route_hbm, route_v, load_sem.at[4]), pltpu.make_async_copy(gates_hbm, gates_v, load_sem.at[5])]
    loads = [pltpu.make_async_copy(h.at[mb], dst.at[:, pl.ds(lo, dm)], load_sem.at[n])
             for n, (h, mb, dst, lo) in enumerate(((x_hbm, other, stage, 0), (dy_hbm, other, stage, dm), (x_hbm, k, mine, 0), (dy_hbm, k, mine, dm)))]
    for c in smalls + loads:
        c.start()
    for c in smalls:
        c.wait()
    metas = [token_meta(route_v[:, m, :], gates_v[:, m, :]) for m in range(2)]
    zero_core = k == 0
    stage[:, 2 * dm:] = jnp.where(zero_core, metas[1].astype(F32), metas[0].astype(F32)).astype(BF16)
    buf[0, 0, 0, k, :, 2 * dm:] = jnp.where(zero_core, metas[0].astype(F32), metas[1].astype(F32)).astype(BF16)
    here.barrier()
    for c in loads:
        c.wait()
    send(36, stage, buf.at[0, 0, 0, k], here.partner)
    arrive(36, buf.at[0, 0, 0, other])
    for s in STREAMS:
        legs[s][0].both_ways()
    for s in STREAMS:
        spread(s, 0)
    for s in STREAMS:
        legs[s][0].relay()
    for s in STREAMS:
        legs[s][1].relay()
    for s in STREAMS:
        legs[s][0].rest()
        spread(s, 1)
    for s in STREAMS:
        second_rest(s, 0)
    for s in STREAMS:
        legs[s][0].far_end()
        spread(s, 2)
    for s in STREAMS:
        legs[s][2].relay()
    for s in STREAMS:
        second_far(s, 0)
    for s in STREAMS:
        second_rest(s, 1)
    for s in STREAMS:
        legs[s][3].relay()
    for s in STREAMS:
        second_rest(s, 2)
    for s in STREAMS:
        second_far(s, 1)
    for s in STREAMS:
        second_far(s, 2)
    for d in range(RING):
        for gi in range(len(GROUPS)):
            for s in STREAMS:
                arrive(37 * s + 24 + 3 * d + gi, blk(s, d, GROUPS[gi], lanes_of[s], 1))
    for c in sent:
        c.wait_send()


def gather_tokens(x, grad_y, route_idx, gates):
    _, tok_dev, dm = x.shape
    top_k = gates.shape[2]
    width = 2 * dm + LANES
    hbm = pl.BlockSpec(memory_space=pltpu.HBM)
    vmem = pl.BlockSpec(memory_space=pltpu.VMEM)
    sems = pltpu.SemaphoreType.DMA((74,))
    args = (x, grad_y, jnp.transpose(route_idx, (2, 0, 1)), jnp.transpose(gates, (2, 0, 1)))
    return pl.pallas_call(
        gather_kernel,
        out_shape=pltpu.VMEM((2, RING, RING, 2, tok_dev, width), BF16),
        in_specs=[hbm] * 4,
        out_specs=vmem,
        scratch_shapes=[pltpu.VMEM((tok_dev, width), BF16), pltpu.VMEM((top_k, 2, tok_dev), jnp.int32), pltpu.VMEM((top_k, 2, tok_dev), F32),
                        sems, sems, pltpu.SemaphoreType.DMA((6,))],
        compiler_params=pltpu.CompilerParams(collective_id=0, has_side_effects=True, vmem_limit_bytes=COMM_VMEM),
        name="gather_tokens",
    )(*(pltpu.with_memory_space_constraint(v, pltpu.HBM) for v in args))


def reduce_kernel(part_ref, out_ref, own, pair, full, half, pair_send, pair_recv,
                  ring_send, ring_recv, last_sem):
    here = Place()
    k, other = here.core, here.other
    lanes_of, halves = stream_lanes(part_ref.shape[5])
    sent = []

    def slot(s, d, i):
        return (d, i) if s == 0 else (i, d)

    def near_slot(s, d, i):
        return slot(s, NEAR.index(FAR[d]), NEAR.index(FAR[i]))

    def swap(s, d, i):
        lanes = lanes_of[s]
        return pltpu.make_async_remote_copy(src_ref=part_ref.at[(1,) + near_slot(s, d, i)].at[:, :, lanes],
                                            dst_ref=pair.at[slot(s, d, i)].at[:, :, lanes], send_sem=pair_send.at[s, d, i],
                                            recv_sem=pair_recv.at[s, d, i], device_id=here.partner, device_id_type=MESH)

    def move(s, f, kind, src, dst, axis):
        peer = here.peer(axis if s == 0 else 3 - axis, 1 if kind % 2 == 0 else -1)
        return pltpu.make_async_remote_copy(src_ref=src, dst_ref=dst, send_sem=ring_send.at[s, f, kind], recv_sem=ring_recv.at[s, f, kind],
                                            device_id=peer, device_id_type=MESH)

    def go(s, f, kind, src, dst, axis):
        c = move(s, f, kind, src, dst, axis)
        c.start()
        sent.append(c)

    def arrive(s, f, kind, dst):
        move(s, f, kind, dst, dst, 1).wait_recv()

    def own_ref(s, d, g, lanes):
        return own.at[slot(s, d, g)].at[:, :, :, lanes]

    def add_own(s, d, g, lanes, *vals):
        ix = slot(s, d, g) + (slice(None), slice(None), lanes)
        total = own[ix]
        for v in vals:
            total = total + v
        own[ix] = total

    def add_pair(s, d, gi):
        lanes = (slice(None), slice(None), lanes_of[s])
        for i in range(GROUPS[gi].start, GROUPS[gi].stop):
            swap(s, d, i).wait_recv()
            own[slot(s, d, i) + lanes] = part_ref[(0,) + near_slot(s, d, i) + lanes] + pair[slot(s, d, i) + lanes]

    def far(s, f, d, at, g, axis):
        for kind in range(2):
            lanes = halves[s][kind]
            go(s, f, kind, own_ref(s, d, at, lanes), half.at[g, :, :, lanes], axis)

    def near(s, f, spot, g, axis):
        for kind, step in ((0, 1), (1, -1)):
            lanes = halves[s][kind]
            arrive(s, f, kind, half.at[g, :, :, lanes])
            add_own(s, *spot(step), lanes, half[g, :, :, lanes])
        lanes = lanes_of[s]
        for kind, step in ((2, 1), (3, -1)):
            go(s, f, kind, own_ref(s, *spot(step), lanes), full.at[kind - 2, g, :, :, lanes], axis)

    def done(s, f, at, g):
        lanes = lanes_of[s]
        for n in range(2):
            arrive(s, f, 2 + n, full.at[n, g, :, :, lanes])
        add_own(s, 3, at, lanes, full[0, g, :, :, lanes], full[1, g, :, :, lanes])

    def far2(gi):
        for s in STREAMS:
            add_pair(s, 0, gi)
            far(s, gi, 0, GROUPS[gi], GROUPS[gi], 2)

    def near2(gi):
        for s in STREAMS:
            add_pair(s, 2, gi)
            add_pair(s, 1, gi)
        for s in STREAMS:
            near(s, gi, lambda step: (2 if step == 1 else 1, GROUPS[gi]), GROUPS[gi], 2)

    def done2(gi):
        for s in STREAMS:
            add_pair(s, 3, gi)
        for s in STREAMS:
            done(s, gi, GROUPS[gi], GROUPS[gi])

    order = [(0, 0), (0, 1), (0, 2), (2, 0), (1, 0), (0, 3), (2, 1), (2, 2), (1, 1), (1, 2), (3, 0), (2, 3), (1, 3), (3, 1), (3, 2), (3, 3)]
    here.barrier()
    for q in order:
        for s in STREAMS:
            c = swap(s, *q)
            c.start()
            sent.append(c)
    lone = slice(RING, RING + 1)
    far2(0)
    far2(1)
    near2(0)
    far2(2)
    near2(1)
    done2(0)
    for s in STREAMS:
        far(s, 3, 3, slice(0, 1), lone, 1)
    near2(2)
    done2(1)
    for s in STREAMS:
        near(s, 3, lambda step: (3, slice(2, 3) if step == 1 else slice(1, 2)), lone, 1)
    done2(2)
    for s in STREAMS:
        done(s, 3, slice(3, 4), lone)

    give = pltpu.make_async_remote_copy(src_ref=own.at[3, 3, other], dst_ref=out_ref.at[k], send_sem=last_sem.at[0], recv_sem=last_sem.at[1],
                                        device_id=here.partner, device_id_type=MESH)
    give.start()
    sent.append(give)
    out_ref[k] = own[3, 3, k]
    pltpu.make_async_remote_copy(src_ref=own.at[3, 3, k], dst_ref=out_ref.at[other], send_sem=last_sem.at[0], recv_sem=last_sem.at[1],
                                 device_id=here.partner, device_id_type=MESH).wait_recv()
    for c in sent:
        c.wait_send()


def finish_kernel(dm, top_k, in_ref, y_ref, dx_ref, dg_ref):
    for m in range(2):
        y_ref[m] = in_ref[m, :, :dm].astype(BF16)
        dx_ref[m] = in_ref[m, :, dm:2 * dm].astype(BF16)
        dg_ref[:, m, :] = in_ref[m, :, 2 * dm:].T[:top_k, :]


def finish(mine, dm, top_k):
    _, tok_dev, _ = mine.shape
    vmem = pl.BlockSpec(memory_space=pltpu.VMEM)
    out = jax.ShapeDtypeStruct((2, tok_dev, dm), BF16)
    y, dx, dg = pl.pallas_call(
        functools.partial(finish_kernel, dm, top_k),
        out_shape=(out, out, jax.ShapeDtypeStruct((top_k, 2, tok_dev), F32)),
        in_specs=[vmem],
        out_specs=(vmem, vmem, vmem),
        name="finish",
    )(pltpu.with_memory_space_constraint(mine, pltpu.VMEM))
    return y, dx, jnp.transpose(dg, (1, 2, 0))


def reduce_tokens(part):
    _, _, _, cores, tok_dev, width = part.shape
    vmem = pl.BlockSpec(memory_space=pltpu.VMEM)
    block = (cores, tok_dev, width)
    ring_sems = pltpu.SemaphoreType.DMA((2, 4, 4))
    pair_sems = pltpu.SemaphoreType.DMA((2, RING, RING))
    return pl.pallas_call(
        reduce_kernel,
        out_shape=pltpu.VMEM((2, tok_dev, width), F32),
        in_specs=[vmem],
        out_specs=vmem,
        scratch_shapes=[
            pltpu.VMEM((RING, RING) + block, F32),
            pltpu.VMEM((RING, RING) + block, F32),
            pltpu.VMEM((2, RING + 1) + block, F32),
            pltpu.VMEM((RING + 1,) + block, F32),
            pair_sems, pair_sems, ring_sems, ring_sems,
            pltpu.SemaphoreType.DMA((2,)),
        ],
        compiler_params=pltpu.CompilerParams(collective_id=1, has_side_effects=True, vmem_limit_bytes=COMM_VMEM),
        name="reduce_tokens",
    )(pltpu.with_memory_space_constraint(part, pltpu.VMEM))


def solution(mesh):
    group = mesh.shape["row"] * mesh.shape["col"] * mesh.shape["core"]
    tok_spec = P(None, ALL_AXES, None)
    w_spec = P(ALL_AXES, None, None)

    def moe_layer(x, route_idx, gates, w_gate, w_up, w_down, grad_y):
        _, tok_dev, dm = x.shape
        top_k = route_idx.shape[2]
        width = 2 * dm + LANES
        xd = gather_tokens(x, grad_y, route_idx, gates).reshape(2, group * tok_dev, width)
        part, g_gate, g_up, g_down = expert_stage(xd, w_gate, w_up, w_down, top_k, group * (tok_dev // 2))
        y, dx, dg = finish(reduce_tokens(part.reshape(2, RING, RING, 2, tok_dev, width)), dm, top_k)
        return y, dx, dg, g_gate, g_up, g_down

    return jax.shard_map(moe_layer, mesh=mesh, in_specs=(tok_spec, tok_spec, tok_spec, w_spec, w_spec, w_spec, tok_spec), out_specs=(tok_spec, tok_spec, tok_spec, w_spec, w_spec, w_spec), check_vma=False)
```

```python
import functools

import jax
import jax.numpy as jnp
from jax import lax
from jax.experimental import pallas as pl
from jax.experimental.pallas import tpu as pltpu
from jax.sharding import PartitionSpec as P

GROUP_AXES = ("row", "col", "core")
ALL_AXES = ("rep", "row", "col", "core")
F32 = jnp.float32
BF16 = jnp.bfloat16
LANES = 128
SMALL = 32
EXPERT_VMEM = 49_500_000
COMM_VMEM = 30_000_000


def dot_nn(a, b):
    return lax.dot_general(a, b, (((1,), (0,)), ((), ())), preferred_element_type=F32)


def dot_nt(a, b):
    return lax.dot_general(a, b, (((1,), (1,)), ((), ())), preferred_element_type=F32)


def dot_tn(a, b):
    return lax.dot_general(a, b, (((0,), (0,)), ((), ())), preferred_element_type=F32)


def split3(v):
    h1 = v.astype(BF16)
    r1 = v - h1.astype(F32)
    h2 = r1.astype(BF16)
    h3 = (r1 - h2.astype(F32)).astype(BF16)
    return h1, h2, h3


def col_blocks(width, step):
    return [(s, min(step, width - s)) for s in range(0, width, step)]


def expert_kernel(dims, xd_v, wg_hbm, wu_hbm, wd_hbm, acc_v, gg_hbm, gu_hbm, gd_hbm,
                  pt_v, gr_v, wgu_v, wd_v, og_v, ou_v, od_v, pos_v,
                  xt_v, qt_v, a_v, duv_v, cnt_s, base_s, big_s, sem_w, sem_o):
    tokens, dm, ff, el, top_k, seg = dims
    n_row, n_col, n_core = lax.axis_size("row"), lax.axis_size("col"), lax.axis_size("core")
    me = (lax.axis_index("row") * n_col + lax.axis_index("col")) * n_core + lax.axis_index("core")
    width = 2 * dm + LANES

    def load_w(e):
        pairs = ((wg_hbm, wgu_v.at[e, :, pl.ds(0, ff)]), (wu_hbm, wgu_v.at[e, :, pl.ds(ff, ff)]), (wd_hbm, wd_v.at[e]))
        return [pltpu.make_async_copy(h.at[e], v, sem_w.at[e, i]) for i, (h, v) in enumerate(pairs)]

    def store_g(e, slot):
        return [pltpu.make_async_copy(v.at[slot], h.at[e], sem_o.at[slot, i])
                for i, (h, v) in enumerate(((gg_hbm, og_v), (gu_hbm, ou_v), (gd_hbm, od_v)))]

    def start_w(lo, hi):
        for e in range(lo, hi):
            for c in load_w(e):
                c.start()

    start_w(0, 1)

    row_i = lax.broadcasted_iota(jnp.int32, (tokens, tokens), 0)
    col_i = lax.broadcasted_iota(jnp.int32, (tokens, tokens), 1)
    tri = (row_i < col_i).astype(F32).astype(BF16)
    sub = lax.broadcasted_iota(jnp.int32, (8, tokens), 0)
    eids = jnp.where(sub < el, (me * el + sub), -1).astype(F32)

    def chunks(total):
        return jnp.maximum((total + (seg - 1)) // seg, 1)

    n_bigs, n_small = [], []
    for m in range(2):
        meta_t = xd_v[m, :, 2 * dm:].astype(F32).T
        hits = jnp.zeros((8, tokens), F32)
        for j in range(top_k):
            hits = hits + (meta_t[j:j + 1, :] == eids).astype(F32)
        rank = dot_nn(hits.astype(BF16), tri)
        counts = [jnp.sum(hits[e:e + 1, :]).astype(jnp.int32) for e in range(el)]
        n_big = jnp.int32(0)
        for cnt in counts:
            n_big = n_big + (cnt > SMALL).astype(jnp.int32)
        big_at, total = jnp.int32(0), n_big * seg
        for e, cnt in enumerate(counts):
            is_big = cnt > SMALL
            base = jnp.where(is_big, big_at * seg, total)
            cnt_s[m, e] = cnt
            base_s[m, e] = base

            @pl.when(is_big)
            def _(m=m, e=e, big_at=big_at):
                big_s[m, big_at] = jnp.int32(e)

            pos_v[m, e:e + 1, :] = jnp.where(hits[e:e + 1, :] > 0, rank[e:e + 1, :] + base.astype(F32), -1.0)
            big_at = big_at + is_big.astype(jnp.int32)
            total = total + jnp.where(is_big, 0, (cnt + 15) // 16 * 16)
        n_bigs.append(n_big)
        n_small.append(jnp.maximum((total - n_big * seg + (LANES - 1)) // LANES, (n_big == 0).astype(jnp.int32)))
        n_ch = chunks(total)

        def gather(c, carry, m=m):
            off = pl.multiple_of(c * seg, seg)
            rows = (lax.broadcasted_iota(jnp.int32, (seg, tokens), 0) + off).astype(F32)
            pick = rows == pos_v[m, 0:1, :]
            for e in range(1, el):
                pick = pick | (rows == pos_v[m, e:e + 1, :])
            pick_f = pick.astype(F32)
            pt_v[m, :, pl.ds(off, seg)] = pick_f.T.astype(BF16)
            pick_b = pick_f.astype(BF16)
            for s, w in col_blocks(width, 512):
                gr_v[m, pl.ds(off, seg), s:s + w] = dot_nn(pick_b, xd_v[m, :, s:s + w]).astype(BF16)
            return carry

        start_w(1 + m, 2 + m)
        lax.fori_loop(0, n_ch, gather, 0)
    start_w(3, el)

    def tile(e, slot, ra, rb, m_a, n_a, n_b, first):
        rows = ra + rb
        base_a = pl.multiple_of(base_s[m_a, e], 16)
        base_b = pl.multiple_of(base_s[1 - m_a, e], 16)
        it = lax.broadcasted_iota(jnp.int32, (rows, 1), 0)
        valid = ((it < ra) & (it < n_a)) | ((it >= ra) & (it - ra < n_b))

        def read(s, w):
            return jnp.concatenate([gr_v[m_a, pl.ds(base_a, ra), s:s + w],
                                    gr_v[1 - m_a, pl.ds(base_b, rb), s:s + w]], axis=0)

        def write(s, w, val):
            merged = jnp.where(valid, val.astype(F32), read(s, w).astype(F32)).astype(BF16)
            gr_v[m_a, pl.ds(base_a, ra), s:s + w] = merged[:ra]
            gr_v[1 - m_a, pl.ds(base_b, rb), s:s + w] = merged[ra:]

        lane = lax.broadcasted_iota(jnp.int32, (rows, LANES), 1)
        meta = jnp.where(valid, read(2 * dm, LANES).astype(F32), 0.0)
        eid = (me * el + e).astype(F32)
        mine = ((meta == eid) & (lane < top_k)).astype(F32)
        sel = pltpu.roll(mine, 8, 1) + pltpu.roll(mine, 16, 1) + pltpu.roll(mine, 24, 1)
        gate = jnp.where(valid, jnp.sum(meta * sel, axis=1, keepdims=True), 0.0)
        for s, w in col_blocks(dm, 256):
            xt_v[:rows, s:s + w] = jnp.where(valid, read(s, w).astype(F32), 0.0).astype(BF16)
            dy = jnp.where(valid, read(dm + s, w).astype(F32), 0.0)
            qt_v[:rows, s:s + w] = (gate * dy).astype(BF16)
        xt = xt_v[:rows, :]
        uv = dot_nn(xt, wgu_v[e]).astype(BF16).astype(F32)
        u, v = uv[:, :ff], uv[:, ff:]
        r = dot_nt(qt_v[:rows, :], wd_v[e])
        s_g = jax.nn.sigmoid(u)
        a_v[:rows, :] = (u * s_g * v).astype(BF16)
        duv_v[:rows, :ff] = (r * v * s_g * (1.0 + u * (1.0 - s_g))).astype(BF16)
        duv_v[:rows, ff:] = (r * u * s_g).astype(BF16)
        a = a_v[:rows, :]
        duv = duv_v[:rows, :]
        dots = jnp.zeros((rows, 1), F32)
        for s, w in col_blocks(dm, 256):
            o = dot_nn(a, wd_v[e, :, s:s + w]).astype(BF16)
            dy = jnp.where(valid, read(dm + s, w).astype(F32), 0.0)
            dots = dots + jnp.sum(dy * o.astype(F32), axis=1, keepdims=True)
            write(s, w, o)
        for s, w in col_blocks(dm, 256):
            write(dm + s, w, dot_nt(duv, wgu_v[e, s:s + w, :]).astype(BF16))
        d1, d2, d3 = split3(dots)
        g1, g2, g3 = split3(gate)
        new_meta = jnp.zeros((rows, LANES), F32)
        for at, val in ((e, d1), (8 + e, d2), (16 + e, d3), (32, g1), (33, g2), (34, g3)):
            new_meta = jnp.where(lane == at, val.astype(F32), new_meta)
        write(2 * dm, LANES, new_meta)

        def put(ref, idx, val):
            if first is None:
                ref[idx] = val
            else:
                ref[idx] = jnp.where(first, 0.0, ref[idx]) + val

        for s, w in col_blocks(dm, 256):
            g_in = dot_tn(xt_v[:rows, s:s + w], duv)
            put(og_v, (slot, slice(s, s + w)), g_in[:, :ff])
            put(ou_v, (slot, slice(s, s + w)), g_in[:, ff:])
        for s, w in col_blocks(dm, 256):
            put(od_v, (slot, slice(None), slice(s, s + w)), dot_tn(a, qt_v[:rows, s:s + w]))

    def expert(e, carry):
        slot = lax.rem(e, 2)
        for c in load_w(e):
            c.wait()

        @pl.when(e >= 2)
        def _():
            for c in store_g(e - 2, slot):
                c.wait()

        n0, n1 = cnt_s[0, e], cnt_s[1, e]
        big0, big1 = n0 > SMALL, n1 > SMALL

        @pl.when(jnp.logical_not(big0 | big1))
        def _():
            tile(e, slot, SMALL, SMALL, 0, n0, n1, None)

        @pl.when(big0 | big1)
        def _():
            both = big0 & big1

            def one(i, inner):
                m_a = jnp.where(both, i, jnp.where(big0, 0, 1))
                n_a = jnp.where(m_a == 0, n0, n1)
                n_b = jnp.where(both, 0, jnp.where(m_a == 0, n1, n0))
                tile(e, slot, seg, SMALL, m_a, n_a, n_b, i == 0)
                return inner

            lax.fori_loop(0, jnp.where(both, 2, 1), one, 0)

        for c in store_g(e, slot):
            c.start()

        return carry

    lax.fori_loop(0, el, expert, 0)

    for m in range(2):
        lane = lax.broadcasted_iota(jnp.int32, (tokens, LANES), 1)

        def put(s, w, first, add):
            acc_v[m, :, s:s + w] = jnp.where(first, 0.0, acc_v[m, :, s:s + w]) + add

        def back(pt, rows, first):
            for s, w in col_blocks(dm + LANES, 256):
                put(dm + s, w, first, dot_nn(pt, gr_v[m, rows, dm + s:dm + s + w]))

        def one_expert(j, carry):
            rows = pl.ds(pl.multiple_of(j * seg, seg), seg)
            pt = pt_v[m, :, rows]
            meta = xd_v[m, :, 2 * dm:].astype(F32)
            mine = ((meta == (me * el + big_s[m, j]).astype(F32)) & (lane < top_k)).astype(F32)
            sel = pltpu.roll(mine, 8, 1) + pltpu.roll(mine, 16, 1) + pltpu.roll(mine, 24, 1)
            gate = jnp.sum(meta * sel, axis=1, keepdims=True)
            for s, w in col_blocks(dm, 256):
                put(s, w, j == 0, gate * dot_nn(pt, gr_v[m, rows, s:s + w]))
            back(pt, rows, j == 0)
            return carry

        def several(c, carry):
            rows = pl.ds(pl.multiple_of(n_bigs[m] * seg + c * LANES, LANES), LANES)
            first = (c == 0) & (n_bigs[m] == 0)
            pt = pt_v[m, :, rows]
            pt2 = jnp.concatenate([pt, pt], axis=1)
            gp = gr_v[m, rows, 2 * dm:].astype(F32)
            gate = gp[:, 32:33] + gp[:, 33:34] + gp[:, 34:35]
            for s, w in col_blocks(dm, 256):
                h1, h2, h3 = split3(gate * gr_v[m, rows, s:s + w].astype(F32))
                put(s, w, first, dot_nn(pt2, jnp.concatenate([h1, h2], axis=0)) + dot_nn(pt, h3))
            back(pt, rows, first)
            return carry

        lax.fori_loop(0, n_bigs[m], one_expert, 0)
        lax.fori_loop(0, n_small[m], several, 0)
        ids = jnp.where(lane < top_k, xd_v[m, :, 2 * dm:].astype(F32), -1.0)
        raw = acc_v[m, :, 2 * dm:]
        raw = raw + pltpu.roll(raw, LANES - 8, 1) + pltpu.roll(raw, LANES - 16, 1)
        out = jnp.zeros((tokens, LANES), F32)
        for e in range(el):
            out = jnp.where(ids == (me * el + e).astype(F32), raw[:, e:e + 1], out)
        acc_v[m, :, 2 * dm:] = out

    for e in range(el - 2, el):
        for c in store_g(e, e % 2):
            c.wait()


def expert_stage(xd, w_gate, w_up, w_down, top_k, seg):
    _, tokens, width = xd.shape
    el, dm, ff = w_gate.shape
    any_spec = pl.BlockSpec(memory_space=pltpu.HBM)
    vmem_spec = pl.BlockSpec(memory_space=pltpu.VMEM)
    rows_max = el * seg
    tile_rows = seg + SMALL
    dims = (tokens, dm, ff, el, top_k, seg)
    return pl.pallas_call(
        functools.partial(expert_kernel, dims),
        out_shape=(
            pltpu.VMEM((2, tokens, width), F32),
            pltpu.HBM((el, dm, ff), F32),
            pltpu.HBM((el, dm, ff), F32),
            pltpu.HBM((el, ff, dm), F32),
        ),
        in_specs=[vmem_spec] + [any_spec] * 3,
        out_specs=[vmem_spec] + [any_spec] * 3,
        scratch_shapes=[
            pltpu.VMEM((2, tokens, rows_max), BF16),
            pltpu.VMEM((2, rows_max, width), BF16),
            pltpu.VMEM((el, dm, 2 * ff), BF16),
            pltpu.VMEM((el, ff, dm), BF16),
            pltpu.VMEM((2, dm, ff), F32),
            pltpu.VMEM((2, dm, ff), F32),
            pltpu.VMEM((2, ff, dm), F32),
            pltpu.VMEM((2, 8, tokens), F32),
            pltpu.VMEM((tile_rows, dm), BF16),
            pltpu.VMEM((tile_rows, dm), BF16),
            pltpu.VMEM((tile_rows, ff), BF16),
            pltpu.VMEM((tile_rows, 2 * ff), BF16),
            pltpu.SMEM((2, 8), jnp.int32),
            pltpu.SMEM((2, 8), jnp.int32),
            pltpu.SMEM((2, 8), jnp.int32),
            pltpu.SemaphoreType.DMA((el, 3)),
            pltpu.SemaphoreType.DMA((2, 3)),
        ],
        compiler_params=pltpu.CompilerParams(vmem_limit_bytes=EXPERT_VMEM),
        name="experts",
    )(pltpu.with_memory_space_constraint(xd, pltpu.VMEM), *(pltpu.with_memory_space_constraint(w, pltpu.HBM) for w in (w_gate, w_up, w_down)))


RING = 4
NEAR = (0, -1, 1, 2)
FAR = (2, -1, 1, 0)
GROUPS = (slice(0, 1), slice(1, 3), slice(3, 4))
MESH = pl.DeviceIdType.MESH


class Place:
    def __init__(self):
        self.row, self.col, self.core = (lax.axis_index(a) for a in GROUP_AXES)
        self.n_row, self.n_col = lax.axis_size("row"), lax.axis_size("col")
        self.other = 1 - self.core
        self.partner = {"core": self.other}

    def spot(self, first, d1, d2):
        row = lax.rem(self.row + (d1 * first + d2 * (1 - first)) + self.n_row, self.n_row)
        col = lax.rem(self.col + (d1 * (1 - first) + d2 * first) + self.n_col, self.n_col)
        return row, col

    def peer(self, axis, d):
        row, col = self.spot(self.core, d, 0) if axis == 1 else self.spot(self.core, 0, d)
        return {"row": row, "col": col}

    def barrier(self):
        sem = pltpu.get_barrier_semaphore()
        peers = [self.peer(axis, d) for axis in (1, 2) for d in (1, -1)] + [self.partner]
        for peer in peers:
            pl.semaphore_signal(sem, inc=1, device_id=peer, device_id_type=MESH)
        pl.semaphore_wait(sem, len(peers))


STREAMS = range(2)


def half_lanes(start, size):
    mid = (size // LANES + 1) // 2 * LANES
    return ((start, mid), (start + mid, size - mid))


def stream_lanes(width):
    whole = half_lanes(0, width)
    return [pl.ds(*w) for w in whole], [[pl.ds(*h) for h in half_lanes(*w)] for w in whole]


def token_meta(route, gates):
    top_k, tok_dev = route.shape
    zero = jnp.zeros((8 - top_k, tok_dev), F32)
    parts = [route.astype(F32)] + [p.astype(F32) for p in split3(gates)]
    rows = jnp.concatenate([v for p in parts for v in (p, zero)], axis=0).astype(BF16)
    n = rows.shape[0]
    eye = (lax.broadcasted_iota(jnp.int32, (n, LANES), 0) == lax.broadcasted_iota(jnp.int32, (n, LANES), 1)).astype(F32).astype(BF16)
    return dot_tn(rows, eye).astype(BF16)


def gather_kernel(x_hbm, dy_hbm, route_hbm, gates_hbm, buf, stage, route_v, gates_v, send_sem, recv_sem, load_sem):
    here = Place()
    k, other = here.core, here.other
    dm = x_hbm.shape[2]
    lanes_of, halves = stream_lanes(2 * dm + LANES)
    sent = []

    def move(idx, src, dst, peer):
        return pltpu.make_async_remote_copy(src_ref=src, dst_ref=dst, send_sem=send_sem.at[idx], recv_sem=recv_sem.at[idx],
                                            device_id=peer, device_id_type=MESH)

    def send(idx, src, dst, peer):
        c = move(idx, src, dst, peer)
        c.start()
        sent.append(c)

    def arrive(idx, dst):
        move(idx, dst, dst, here.partner).wait_recv()

    def blk(s, d, g, lanes, side=0):
        ref = buf.at[side, d, g] if s == 0 else buf.at[side, g, d]
        return ref.at[:, :, :, lanes]

    def towards(s, axis, way):
        return here.peer(axis if s == 0 else 3 - axis, 1 - 2 * way)

    class Leg:
        def __init__(self, s, p):
            self.s, self.p, self.base, self.axis = s, p, 37 * s + 6 * p, 1 if p == 0 else 2
            self.at = (lambda j, lanes: blk(s, 0, slice(j, j + 1), lanes)) if p == 0 else (lambda j, lanes: blk(s, j, GROUPS[p - 1], lanes))

        def step(self, way, n):
            lanes = halves[self.s][way if n == 0 else 1 - way]
            src, dst = self.at(0, lanes), self.at(1 + way, lanes)
            idx = self.base + 2 * way + n
            if self.p > 1:
                return [(idx, src, dst)]
            more = 74 + 8 * self.s + 4 * self.p + 2 * way + n
            return [(i, src.at[:, pl.ds(c, 1)], dst.at[:, pl.ds(c, 1)]) for i, c in ((idx, k), (more, other))]

        def both_ways(self, turn=0):
            for way in range(2):
                for n in range(2):
                    idx, src, dst = self.step(way, n)[turn]
                    send(idx, src, dst, towards(self.s, self.axis, way))

        def relay(self):
            for way in range(2):
                lanes = halves[self.s][way]
                for idx, _, dst in self.step(way, 0):
                    arrive(idx, dst)
                send(self.base + 4 + way, self.at(1 + way, lanes), self.at(3, lanes), towards(self.s, self.axis, way))

        def rest(self):
            for way in range(2):
                for idx, _, dst in self.step(way, 1):
                    arrive(idx, dst)

        def far_end(self):
            for way in range(2):
                arrive(self.base + 4 + way, self.at(3, halves[self.s][way]))

    legs = [[Leg(s, p) for p in range(4)] for s in STREAMS]

    def have(s, gi, d):
        lanes = lanes_of[s]
        send(37 * s + 24 + 3 * d + gi, blk(s, d, GROUPS[gi], lanes), blk(s, d, GROUPS[gi], lanes, 1), here.partner)

    def spread(s, gi):
        legs[s][1 + gi].both_ways()
        have(s, gi, 0)

    def own_rows(turn):
        for p in range(2):
            for s in STREAMS:
                legs[s][p].both_ways(turn)

    def second_rest(s, gi):
        legs[s][1 + gi].rest()
        have(s, gi, 1)
        have(s, gi, 2)

    def second_far(s, gi):
        legs[s][1 + gi].far_end()
        have(s, gi, 3)

    mine = buf.at[0, 0, 0, k]
    smalls = [pltpu.make_async_copy(route_hbm, route_v, load_sem.at[4]), pltpu.make_async_copy(gates_hbm, gates_v, load_sem.at[5])]
    loads = [pltpu.make_async_copy(h.at[mb], dst.at[:, pl.ds(lo, dm)], load_sem.at[n])
             for n, (h, mb, dst, lo) in enumerate(((x_hbm, other, stage, 0), (dy_hbm, other, stage, dm), (x_hbm, k, mine, 0), (dy_hbm, k, mine, dm)))]
    for c in smalls + loads:
        c.start()
    for c in smalls:
        c.wait()
    metas = [token_meta(route_v[:, m, :], gates_v[:, m, :]) for m in range(2)]
    zero_core = k == 0
    stage[:, 2 * dm:] = jnp.where(zero_core, metas[1].astype(F32), metas[0].astype(F32)).astype(BF16)
    buf[0, 0, 0, k, :, 2 * dm:] = jnp.where(zero_core, metas[0].astype(F32), metas[1].astype(F32)).astype(BF16)
    here.barrier()
    for c in loads:
        c.wait()
    send(36, stage, buf.at[0, 0, 0, k], here.partner)
    own_rows(0)
    arrive(36, buf.at[0, 0, 0, other])
    own_rows(1)
    for s in STREAMS:
        have(s, 0, 0)
    for s in STREAMS:
        legs[s][0].relay()
    for s in STREAMS:
        legs[s][1].relay()
    for s in STREAMS:
        legs[s][0].rest()
        spread(s, 1)
    for s in STREAMS:
        second_rest(s, 0)
    for s in STREAMS:
        legs[s][0].far_end()
        spread(s, 2)
    for s in STREAMS:
        legs[s][2].relay()
    for s in STREAMS:
        second_far(s, 0)
    for s in STREAMS:
        second_rest(s, 1)
    for s in STREAMS:
        legs[s][3].relay()
    for s in STREAMS:
        second_rest(s, 2)
    for s in STREAMS:
        second_far(s, 1)
    for s in STREAMS:
        second_far(s, 2)
    for d in range(RING):
        for gi in range(len(GROUPS)):
            for s in STREAMS:
                arrive(37 * s + 24 + 3 * d + gi, blk(s, d, GROUPS[gi], lanes_of[s], 1))
    for c in sent:
        c.wait_send()


def gather_tokens(x, grad_y, route_idx, gates):
    _, tok_dev, dm = x.shape
    top_k = gates.shape[2]
    width = 2 * dm + LANES
    hbm = pl.BlockSpec(memory_space=pltpu.HBM)
    vmem = pl.BlockSpec(memory_space=pltpu.VMEM)
    sems = pltpu.SemaphoreType.DMA((90,))
    args = (x, grad_y, jnp.transpose(route_idx, (2, 0, 1)), jnp.transpose(gates, (2, 0, 1)))
    return pl.pallas_call(
        gather_kernel,
        out_shape=pltpu.VMEM((2, RING, RING, 2, tok_dev, width), BF16),
        in_specs=[hbm] * 4,
        out_specs=vmem,
        scratch_shapes=[pltpu.VMEM((tok_dev, width), BF16), pltpu.VMEM((top_k, 2, tok_dev), jnp.int32), pltpu.VMEM((top_k, 2, tok_dev), F32),
                        sems, sems, pltpu.SemaphoreType.DMA((6,))],
        compiler_params=pltpu.CompilerParams(collective_id=0, has_side_effects=True, vmem_limit_bytes=COMM_VMEM),
        name="gather_tokens",
    )(*(pltpu.with_memory_space_constraint(v, pltpu.HBM) for v in args))


def reduce_kernel(part_ref, out_ref, own, pair, full, half, pair_send, pair_recv,
                  ring_send, ring_recv, last_sem):
    here = Place()
    k, other = here.core, here.other
    lanes_of, halves = stream_lanes(part_ref.shape[5])
    sent = []

    def slot(s, d, i):
        return (d, i) if s == 0 else (i, d)

    def near_slot(s, d, i):
        return slot(s, NEAR.index(FAR[d]), NEAR.index(FAR[i]))

    def swap(s, d, i):
        lanes = lanes_of[s]
        return pltpu.make_async_remote_copy(src_ref=part_ref.at[(1,) + near_slot(s, d, i)].at[:, :, lanes],
                                            dst_ref=pair.at[slot(s, d, i)].at[:, :, lanes], send_sem=pair_send.at[s, d, i],
                                            recv_sem=pair_recv.at[s, d, i], device_id=here.partner, device_id_type=MESH)

    def move(s, f, kind, src, dst, axis):
        peer = here.peer(axis if s == 0 else 3 - axis, 1 if kind % 2 == 0 else -1)
        return pltpu.make_async_remote_copy(src_ref=src, dst_ref=dst, send_sem=ring_send.at[s, f, kind], recv_sem=ring_recv.at[s, f, kind],
                                            device_id=peer, device_id_type=MESH)

    def go(s, f, kind, src, dst, axis):
        c = move(s, f, kind, src, dst, axis)
        c.start()
        sent.append(c)

    def arrive(s, f, kind, dst):
        move(s, f, kind, dst, dst, 1).wait_recv()

    def own_ref(s, d, g, lanes):
        return own.at[slot(s, d, g)].at[:, :, :, lanes]

    def add_own(s, d, g, lanes, *vals):
        ix = slot(s, d, g) + (slice(None), slice(None), lanes)
        total = own[ix]
        for v in vals:
            total = total + v
        own[ix] = total

    def add_pair(s, d, gi):
        lanes = (slice(None), slice(None), lanes_of[s])
        for i in range(GROUPS[gi].start, GROUPS[gi].stop):
            swap(s, d, i).wait_recv()
            own[slot(s, d, i) + lanes] = part_ref[(0,) + near_slot(s, d, i) + lanes] + pair[slot(s, d, i) + lanes]

    def far(s, f, d, at, g, axis):
        for kind in range(2):
            lanes = halves[s][kind]
            go(s, f, kind, own_ref(s, d, at, lanes), half.at[g, :, :, lanes], axis)

    def near(s, f, spot, g, axis):
        for kind, step in ((0, 1), (1, -1)):
            lanes = halves[s][kind]
            arrive(s, f, kind, half.at[g, :, :, lanes])
            add_own(s, *spot(step), lanes, half[g, :, :, lanes])
        lanes = lanes_of[s]
        for kind, step in ((2, 1), (3, -1)):
            go(s, f, kind, own_ref(s, *spot(step), lanes), full.at[kind - 2, g, :, :, lanes], axis)

    def done(s, f, at, g):
        lanes = lanes_of[s]
        for n in range(2):
            arrive(s, f, 2 + n, full.at[n, g, :, :, lanes])
        add_own(s, 3, at, lanes, full[0, g, :, :, lanes], full[1, g, :, :, lanes])

    def far2(gi):
        for s in STREAMS:
            add_pair(s, 0, gi)
            far(s, gi, 0, GROUPS[gi], GROUPS[gi], 2)

    def near2(gi):
        for s in STREAMS:
            add_pair(s, 2, gi)
            add_pair(s, 1, gi)
        for s in STREAMS:
            near(s, gi, lambda step: (2 if step == 1 else 1, GROUPS[gi]), GROUPS[gi], 2)

    def done2(gi):
        for s in STREAMS:
            add_pair(s, 3, gi)
        for s in STREAMS:
            done(s, gi, GROUPS[gi], GROUPS[gi])

    order = [(0, 0), (0, 1), (0, 2), (2, 0), (1, 0), (0, 3), (2, 1), (2, 2), (1, 1), (1, 2), (3, 0), (2, 3), (1, 3), (3, 1), (3, 2), (3, 3)]
    here.barrier()
    for q in order:
        for s in STREAMS:
            c = swap(s, *q)
            c.start()
            sent.append(c)
    lone = slice(RING, RING + 1)
    far2(0)
    far2(1)
    near2(0)
    far2(2)
    near2(1)
    done2(0)
    for s in STREAMS:
        far(s, 3, 3, slice(0, 1), lone, 1)
    near2(2)
    done2(1)
    for s in STREAMS:
        near(s, 3, lambda step: (3, slice(2, 3) if step == 1 else slice(1, 2)), lone, 1)
    done2(2)
    for s in STREAMS:
        done(s, 3, slice(3, 4), lone)

    give = pltpu.make_async_remote_copy(src_ref=own.at[3, 3, other], dst_ref=out_ref.at[k], send_sem=last_sem.at[0], recv_sem=last_sem.at[1],
                                        device_id=here.partner, device_id_type=MESH)
    give.start()
    sent.append(give)
    out_ref[k] = own[3, 3, k]
    pltpu.make_async_remote_copy(src_ref=own.at[3, 3, k], dst_ref=out_ref.at[other], send_sem=last_sem.at[0], recv_sem=last_sem.at[1],
                                 device_id=here.partner, device_id_type=MESH).wait_recv()
    for c in sent:
        c.wait_send()


def finish_kernel(dm, top_k, in_ref, y_ref, dx_ref, dg_ref):
    for m in range(2):
        y_ref[m] = in_ref[m, :, :dm].astype(BF16)
        dx_ref[m] = in_ref[m, :, dm:2 * dm].astype(BF16)
        dg_ref[:, m, :] = in_ref[m, :, 2 * dm:].T[:top_k, :]


def finish(mine, dm, top_k):
    _, tok_dev, _ = mine.shape
    vmem = pl.BlockSpec(memory_space=pltpu.VMEM)
    out = jax.ShapeDtypeStruct((2, tok_dev, dm), BF16)
    y, dx, dg = pl.pallas_call(
        functools.partial(finish_kernel, dm, top_k),
        out_shape=(out, out, jax.ShapeDtypeStruct((top_k, 2, tok_dev), F32)),
        in_specs=[vmem],
        out_specs=(vmem, vmem, vmem),
        name="finish",
    )(pltpu.with_memory_space_constraint(mine, pltpu.VMEM))
    return y, dx, jnp.transpose(dg, (1, 2, 0))


def reduce_tokens(part):
    _, _, _, cores, tok_dev, width = part.shape
    vmem = pl.BlockSpec(memory_space=pltpu.VMEM)
    block = (cores, tok_dev, width)
    ring_sems = pltpu.SemaphoreType.DMA((2, 4, 4))
    pair_sems = pltpu.SemaphoreType.DMA((2, RING, RING))
    return pl.pallas_call(
        reduce_kernel,
        out_shape=pltpu.VMEM((2, tok_dev, width), F32),
        in_specs=[vmem],
        out_specs=vmem,
        scratch_shapes=[
            pltpu.VMEM((RING, RING) + block, F32),
            pltpu.VMEM((RING, RING) + block, F32),
            pltpu.VMEM((2, RING + 1) + block, F32),
            pltpu.VMEM((RING + 1,) + block, F32),
            pair_sems, pair_sems, ring_sems, ring_sems,
            pltpu.SemaphoreType.DMA((2,)),
        ],
        compiler_params=pltpu.CompilerParams(collective_id=1, has_side_effects=True, vmem_limit_bytes=COMM_VMEM),
        name="reduce_tokens",
    )(pltpu.with_memory_space_constraint(part, pltpu.VMEM))


def solution(mesh):
    group = mesh.shape["row"] * mesh.shape["col"] * mesh.shape["core"]
    tok_spec = P(None, ALL_AXES, None)
    w_spec = P(ALL_AXES, None, None)

    def moe_layer(x, route_idx, gates, w_gate, w_up, w_down, grad_y):
        _, tok_dev, dm = x.shape
        top_k = route_idx.shape[2]
        width = 2 * dm + LANES
        xd = gather_tokens(x, grad_y, route_idx, gates).reshape(2, group * tok_dev, width)
        part, g_gate, g_up, g_down = expert_stage(xd, w_gate, w_up, w_down, top_k, group * (tok_dev // 2))
        y, dx, dg = finish(reduce_tokens(part.reshape(2, RING, RING, 2, tok_dev, width)), dm, top_k)
        return y, dx, dg, g_gate, g_up, g_down

    return jax.shard_map(moe_layer, mesh=mesh, in_specs=(tok_spec, tok_spec, tok_spec, w_spec, w_spec, w_spec, tok_spec), out_specs=(tok_spec, tok_spec, tok_spec, w_spec, w_spec, w_spec), check_vma=False)
```

```python
import functools

import jax
import jax.numpy as jnp
from jax import lax
from jax.experimental import pallas as pl
from jax.experimental.pallas import tpu as pltpu
from jax.sharding import PartitionSpec as P

GROUP_AXES = ("row", "col", "core")
ALL_AXES = ("rep", "row", "col", "core")
F32 = jnp.float32
BF16 = jnp.bfloat16
LANES = 128
SMALL = 32
EXPERT_VMEM = 49_500_000
COMM_VMEM = 30_000_000


def dot_nn(a, b):
    return lax.dot_general(a, b, (((1,), (0,)), ((), ())), preferred_element_type=F32)


def dot_nt(a, b):
    return lax.dot_general(a, b, (((1,), (1,)), ((), ())), preferred_element_type=F32)


def dot_tn(a, b):
    return lax.dot_general(a, b, (((0,), (0,)), ((), ())), preferred_element_type=F32)


def split3(v):
    h1 = v.astype(BF16)
    r1 = v - h1.astype(F32)
    h2 = r1.astype(BF16)
    h3 = (r1 - h2.astype(F32)).astype(BF16)
    return h1, h2, h3


def col_blocks(width, step):
    return [(s, min(step, width - s)) for s in range(0, width, step)]


def expert_kernel(dims, xd_v, wg_hbm, wu_hbm, wd_hbm, acc_v, gg_hbm, gu_hbm, gd_hbm,
                  pt_v, gr_v, wgu_v, wd_v, og_v, ou_v, od_v, pos_v,
                  xt_v, qt_v, a_v, duv_v, cnt_s, base_s, big_s, sem_w, sem_o):
    tokens, dm, ff, el, top_k, seg = dims
    n_row, n_col, n_core = lax.axis_size("row"), lax.axis_size("col"), lax.axis_size("core")
    me = (lax.axis_index("row") * n_col + lax.axis_index("col")) * n_core + lax.axis_index("core")
    width = 2 * dm + LANES

    def load_w(e):
        pairs = ((wg_hbm, wgu_v.at[e, :, pl.ds(0, ff)]), (wu_hbm, wgu_v.at[e, :, pl.ds(ff, ff)]), (wd_hbm, wd_v.at[e]))
        return [pltpu.make_async_copy(h.at[e], v, sem_w.at[e, i]) for i, (h, v) in enumerate(pairs)]

    def store_g(e, slot):
        return [pltpu.make_async_copy(v.at[slot], h.at[e], sem_o.at[slot, i])
                for i, (h, v) in enumerate(((gg_hbm, og_v), (gu_hbm, ou_v), (gd_hbm, od_v)))]

    def start_w(lo, hi):
        for e in range(lo, hi):
            for c in load_w(e):
                c.start()

    start_w(0, 1)

    row_i = lax.broadcasted_iota(jnp.int32, (tokens, tokens), 0)
    col_i = lax.broadcasted_iota(jnp.int32, (tokens, tokens), 1)
    tri = (row_i < col_i).astype(F32).astype(BF16)
    sub = lax.broadcasted_iota(jnp.int32, (8, tokens), 0)
    eids = jnp.where(sub < el, (me * el + sub), -1).astype(F32)

    def chunks(total):
        return jnp.maximum((total + (seg - 1)) // seg, 1)

    n_bigs, n_small = [], []
    for m in range(2):
        meta_t = xd_v[m, :, 2 * dm:].astype(F32).T
        hits = jnp.zeros((8, tokens), F32)
        for j in range(top_k):
            hits = hits + (meta_t[j:j + 1, :] == eids).astype(F32)
        rank = dot_nn(hits.astype(BF16), tri)
        counts = [jnp.sum(hits[e:e + 1, :]).astype(jnp.int32) for e in range(el)]
        n_big = jnp.int32(0)
        for cnt in counts:
            n_big = n_big + (cnt > SMALL).astype(jnp.int32)
        big_at, total = jnp.int32(0), n_big * seg
        for e, cnt in enumerate(counts):
            is_big = cnt > SMALL
            base = jnp.where(is_big, big_at * seg, total)
            cnt_s[m, e] = cnt
            base_s[m, e] = base

            @pl.when(is_big)
            def _(m=m, e=e, big_at=big_at):
                big_s[m, big_at] = jnp.int32(e)

            pos_v[m, e:e + 1, :] = jnp.where(hits[e:e + 1, :] > 0, rank[e:e + 1, :] + base.astype(F32), -1.0)
            big_at = big_at + is_big.astype(jnp.int32)
            total = total + jnp.where(is_big, 0, (cnt + 15) // 16 * 16)
        n_bigs.append(n_big)
        n_small.append(jnp.maximum((total - n_big * seg + (LANES - 1)) // LANES, (n_big == 0).astype(jnp.int32)))
        n_ch = chunks(total)

        def gather(c, carry, m=m):
            off = pl.multiple_of(c * seg, seg)
            rows = (lax.broadcasted_iota(jnp.int32, (seg, tokens), 0) + off).astype(F32)
            pick = rows == pos_v[m, 0:1, :]
            for e in range(1, el):
                pick = pick | (rows == pos_v[m, e:e + 1, :])
            pick_f = pick.astype(F32)
            pt_v[m, :, pl.ds(off, seg)] = pick_f.T.astype(BF16)
            pick_b = pick_f.astype(BF16)
            for s, w in col_blocks(width, 512):
                gr_v[m, pl.ds(off, seg), s:s + w] = dot_nn(pick_b, xd_v[m, :, s:s + w]).astype(BF16)
            return carry

        start_w(1 + m, 2 + m)
        lax.fori_loop(0, n_ch, gather, 0)
    start_w(3, el)

    def tile(e, slot, ra, rb, m_a, n_a, n_b, first):
        rows = ra + rb
        base_a = pl.multiple_of(base_s[m_a, e], 16)
        base_b = pl.multiple_of(base_s[1 - m_a, e], 16)
        it = lax.broadcasted_iota(jnp.int32, (rows, 1), 0)
        valid = ((it < ra) & (it < n_a)) | ((it >= ra) & (it - ra < n_b))

        def read(s, w):
            return jnp.concatenate([gr_v[m_a, pl.ds(base_a, ra), s:s + w],
                                    gr_v[1 - m_a, pl.ds(base_b, rb), s:s + w]], axis=0)

        def write(s, w, val):
            merged = jnp.where(valid, val.astype(F32), read(s, w).astype(F32)).astype(BF16)
            gr_v[m_a, pl.ds(base_a, ra), s:s + w] = merged[:ra]
            gr_v[1 - m_a, pl.ds(base_b, rb), s:s + w] = merged[ra:]

        lane = lax.broadcasted_iota(jnp.int32, (rows, LANES), 1)
        meta = jnp.where(valid, read(2 * dm, LANES).astype(F32), 0.0)
        eid = (me * el + e).astype(F32)
        mine = ((meta == eid) & (lane < top_k)).astype(F32)
        sel = pltpu.roll(mine, 8, 1) + pltpu.roll(mine, 16, 1) + pltpu.roll(mine, 24, 1)
        gate = jnp.where(valid, jnp.sum(meta * sel, axis=1, keepdims=True), 0.0)
        for s, w in col_blocks(dm, 256):
            xt_v[:rows, s:s + w] = jnp.where(valid, read(s, w).astype(F32), 0.0).astype(BF16)
            dy = jnp.where(valid, read(dm + s, w).astype(F32), 0.0)
            qt_v[:rows, s:s + w] = (gate * dy).astype(BF16)
        xt = xt_v[:rows, :]
        uv = dot_nn(xt, wgu_v[e]).astype(BF16).astype(F32)
        u, v = uv[:, :ff], uv[:, ff:]
        r = dot_nt(qt_v[:rows, :], wd_v[e])
        s_g = jax.nn.sigmoid(u)
        a_v[:rows, :] = (u * s_g * v).astype(BF16)
        duv_v[:rows, :ff] = (r * v * s_g * (1.0 + u * (1.0 - s_g))).astype(BF16)
        duv_v[:rows, ff:] = (r * u * s_g).astype(BF16)
        a = a_v[:rows, :]
        duv = duv_v[:rows, :]
        dots = jnp.zeros((rows, 1), F32)
        for s, w in col_blocks(dm, 256):
            o = dot_nn(a, wd_v[e, :, s:s + w]).astype(BF16)
            dy = jnp.where(valid, read(dm + s, w).astype(F32), 0.0)
            dots = dots + jnp.sum(dy * o.astype(F32), axis=1, keepdims=True)
            write(s, w, o)
        for s, w in col_blocks(dm, 256):
            write(dm + s, w, dot_nt(duv, wgu_v[e, s:s + w, :]).astype(BF16))
        d1, d2, d3 = split3(dots)
        g1, g2, g3 = split3(gate)
        new_meta = jnp.zeros((rows, LANES), F32)
        for at, val in ((e, d1), (8 + e, d2), (16 + e, d3), (32, g1), (33, g2), (34, g3)):
            new_meta = jnp.where(lane == at, val.astype(F32), new_meta)
        write(2 * dm, LANES, new_meta)

        def put(ref, idx, val):
            if first is None:
                ref[idx] = val
            else:
                ref[idx] = jnp.where(first, 0.0, ref[idx]) + val

        for s, w in col_blocks(dm, 256):
            g_in = dot_tn(xt_v[:rows, s:s + w], duv)
            put(og_v, (slot, slice(s, s + w)), g_in[:, :ff])
            put(ou_v, (slot, slice(s, s + w)), g_in[:, ff:])
        for s, w in col_blocks(dm, 256):
            put(od_v, (slot, slice(None), slice(s, s + w)), dot_tn(a, qt_v[:rows, s:s + w]))

    def expert(e, carry):
        slot = lax.rem(e, 2)
        for c in load_w(e):
            c.wait()

        @pl.when(e >= 2)
        def _():
            for c in store_g(e - 2, slot):
                c.wait()

        n0, n1 = cnt_s[0, e], cnt_s[1, e]
        big0, big1 = n0 > SMALL, n1 > SMALL

        @pl.when(jnp.logical_not(big0 | big1))
        def _():
            tile(e, slot, SMALL, SMALL, 0, n0, n1, None)

        @pl.when(big0 | big1)
        def _():
            both = big0 & big1

            def one(i, inner):
                m_a = jnp.where(both, i, jnp.where(big0, 0, 1))
                n_a = jnp.where(m_a == 0, n0, n1)
                n_b = jnp.where(both, 0, jnp.where(m_a == 0, n1, n0))
                tile(e, slot, seg, SMALL, m_a, n_a, n_b, i == 0)
                return inner

            lax.fori_loop(0, jnp.where(both, 2, 1), one, 0)

        for c in store_g(e, slot):
            c.start()

        return carry

    lax.fori_loop(0, el, expert, 0)

    for m in range(2):
        lane = lax.broadcasted_iota(jnp.int32, (tokens, LANES), 1)

        def put(s, w, first, add):
            acc_v[m, :, s:s + w] = jnp.where(first, 0.0, acc_v[m, :, s:s + w]) + add

        def back(pt, rows, first):
            for s, w in col_blocks(dm + LANES, 256):
                put(dm + s, w, first, dot_nn(pt, gr_v[m, rows, dm + s:dm + s + w]))

        def one_expert(j, carry):
            rows = pl.ds(pl.multiple_of(j * seg, seg), seg)
            pt = pt_v[m, :, rows]
            meta = xd_v[m, :, 2 * dm:].astype(F32)
            mine = ((meta == (me * el + big_s[m, j]).astype(F32)) & (lane < top_k)).astype(F32)
            sel = pltpu.roll(mine, 8, 1) + pltpu.roll(mine, 16, 1) + pltpu.roll(mine, 24, 1)
            gate = jnp.sum(meta * sel, axis=1, keepdims=True)
            for s, w in col_blocks(dm, 256):
                put(s, w, j == 0, gate * dot_nn(pt, gr_v[m, rows, s:s + w]))
            back(pt, rows, j == 0)
            return carry

        def several(c, carry):
            rows = pl.ds(pl.multiple_of(n_bigs[m] * seg + c * LANES, LANES), LANES)
            first = (c == 0) & (n_bigs[m] == 0)
            pt = pt_v[m, :, rows]
            pt2 = jnp.concatenate([pt, pt], axis=1)
            gp = gr_v[m, rows, 2 * dm:].astype(F32)
            gate = gp[:, 32:33] + gp[:, 33:34] + gp[:, 34:35]
            for s, w in col_blocks(dm, 256):
                h1, h2, h3 = split3(gate * gr_v[m, rows, s:s + w].astype(F32))
                put(s, w, first, dot_nn(pt2, jnp.concatenate([h1, h2], axis=0)) + dot_nn(pt, h3))
            back(pt, rows, first)
            return carry

        lax.fori_loop(0, n_bigs[m], one_expert, 0)
        lax.fori_loop(0, n_small[m], several, 0)
        ids = jnp.where(lane < top_k, xd_v[m, :, 2 * dm:].astype(F32), -1.0)
        raw = acc_v[m, :, 2 * dm:]
        raw = raw + pltpu.roll(raw, LANES - 8, 1) + pltpu.roll(raw, LANES - 16, 1)
        out = jnp.zeros((tokens, LANES), F32)
        for e in range(el):
            out = jnp.where(ids == (me * el + e).astype(F32), raw[:, e:e + 1], out)
        acc_v[m, :, 2 * dm:] = out

    for e in range(el - 2, el):
        for c in store_g(e, e % 2):
            c.wait()


def expert_stage(xd, w_gate, w_up, w_down, top_k, seg):
    _, tokens, width = xd.shape
    el, dm, ff = w_gate.shape
    any_spec = pl.BlockSpec(memory_space=pltpu.HBM)
    vmem_spec = pl.BlockSpec(memory_space=pltpu.VMEM)
    rows_max = el * seg
    tile_rows = seg + SMALL
    dims = (tokens, dm, ff, el, top_k, seg)
    return pl.pallas_call(
        functools.partial(expert_kernel, dims),
        out_shape=(
            pltpu.VMEM((2, tokens, width), F32),
            pltpu.HBM((el, dm, ff), F32),
            pltpu.HBM((el, dm, ff), F32),
            pltpu.HBM((el, ff, dm), F32),
        ),
        in_specs=[vmem_spec] + [any_spec] * 3,
        out_specs=[vmem_spec] + [any_spec] * 3,
        scratch_shapes=[
            pltpu.VMEM((2, tokens, rows_max), BF16),
            pltpu.VMEM((2, rows_max, width), BF16),
            pltpu.VMEM((el, dm, 2 * ff), BF16),
            pltpu.VMEM((el, ff, dm), BF16),
            pltpu.VMEM((2, dm, ff), F32),
            pltpu.VMEM((2, dm, ff), F32),
            pltpu.VMEM((2, ff, dm), F32),
            pltpu.VMEM((2, 8, tokens), F32),
            pltpu.VMEM((tile_rows, dm), BF16),
            pltpu.VMEM((tile_rows, dm), BF16),
            pltpu.VMEM((tile_rows, ff), BF16),
            pltpu.VMEM((tile_rows, 2 * ff), BF16),
            pltpu.SMEM((2, 8), jnp.int32),
            pltpu.SMEM((2, 8), jnp.int32),
            pltpu.SMEM((2, 8), jnp.int32),
            pltpu.SemaphoreType.DMA((el, 3)),
            pltpu.SemaphoreType.DMA((2, 3)),
        ],
        compiler_params=pltpu.CompilerParams(vmem_limit_bytes=EXPERT_VMEM),
        name="experts",
    )(pltpu.with_memory_space_constraint(xd, pltpu.VMEM), *(pltpu.with_memory_space_constraint(w, pltpu.HBM) for w in (w_gate, w_up, w_down)))


RING = 4
NEAR = (0, -1, 1, 2)
FAR = (2, -1, 1, 0)
GROUPS = (slice(0, 1), slice(1, 3), slice(3, 4))
MESH = pl.DeviceIdType.MESH


class Place:
    def __init__(self):
        self.row, self.col, self.core = (lax.axis_index(a) for a in GROUP_AXES)
        self.n_row, self.n_col = lax.axis_size("row"), lax.axis_size("col")
        self.other = 1 - self.core
        self.partner = {"core": self.other}

    def spot(self, first, d1, d2):
        row = lax.rem(self.row + (d1 * first + d2 * (1 - first)) + self.n_row, self.n_row)
        col = lax.rem(self.col + (d1 * (1 - first) + d2 * first) + self.n_col, self.n_col)
        return row, col

    def peer(self, axis, d):
        row, col = self.spot(self.core, d, 0) if axis == 1 else self.spot(self.core, 0, d)
        return {"row": row, "col": col}

    def barrier(self):
        sem = pltpu.get_barrier_semaphore()
        peers = [self.peer(axis, d) for axis in (1, 2) for d in (1, -1)] + [self.partner]
        for peer in peers:
            pl.semaphore_signal(sem, inc=1, device_id=peer, device_id_type=MESH)
        pl.semaphore_wait(sem, len(peers))


STREAMS = range(2)


def half_lanes(start, size):
    mid = (size // LANES + 1) // 2 * LANES
    return ((start, mid), (start + mid, size - mid))


def stream_lanes(width):
    whole = half_lanes(0, width)
    return [pl.ds(*w) for w in whole], [[pl.ds(*h) for h in half_lanes(*w)] for w in whole]


def token_meta(route, gates):
    top_k, tok_dev = route.shape
    zero = jnp.zeros((8 - top_k, tok_dev), F32)
    parts = [route.astype(F32)] + [p.astype(F32) for p in split3(gates)]
    rows = jnp.concatenate([v for p in parts for v in (p, zero)], axis=0).astype(BF16)
    n = rows.shape[0]
    eye = (lax.broadcasted_iota(jnp.int32, (n, LANES), 0) == lax.broadcasted_iota(jnp.int32, (n, LANES), 1)).astype(F32).astype(BF16)
    return dot_tn(rows, eye).astype(BF16)


def gather_kernel(x_hbm, dy_hbm, route_hbm, gates_hbm, buf, stage, route_v, gates_v, send_sem, recv_sem, load_sem):
    here = Place()
    k, other = here.core, here.other
    dm = x_hbm.shape[2]
    lanes_of, halves = stream_lanes(2 * dm + LANES)
    sent = []

    def move(idx, src, dst, peer):
        return pltpu.make_async_remote_copy(src_ref=src, dst_ref=dst, send_sem=send_sem.at[idx], recv_sem=recv_sem.at[idx],
                                            device_id=peer, device_id_type=MESH)

    def send(idx, src, dst, peer):
        c = move(idx, src, dst, peer)
        c.start()
        sent.append(c)

    def arrive(idx, dst):
        move(idx, dst, dst, here.partner).wait_recv()

    def blk(s, d, g, lanes, side=0):
        ref = buf.at[side, d, g] if s == 0 else buf.at[side, g, d]
        return ref.at[:, :, :, lanes]

    def towards(s, axis, way):
        return here.peer(axis if s == 0 else 3 - axis, 1 - 2 * way)

    class Leg:
        def __init__(self, s, p):
            self.s, self.base, self.axis = s, 37 * s + 6 * p, 1 if p == 0 else 2
            self.at = (lambda j, lanes: blk(s, 0, slice(j, j + 1), lanes)) if p == 0 else (lambda j, lanes: blk(s, j, GROUPS[p - 1], lanes))

        def both_ways(self):
            for way in range(2):
                for n in range(2):
                    lanes = halves[self.s][way if n == 0 else 1 - way]
                    send(self.base + 2 * way + n, self.at(0, lanes), self.at(1 + way, lanes), towards(self.s, self.axis, way))

        def relay(self):
            for way in range(2):
                lanes = halves[self.s][way]
                arrive(self.base + 2 * way, self.at(1 + way, lanes))
                send(self.base + 4 + way, self.at(1 + way, lanes), self.at(3, lanes), towards(self.s, self.axis, way))

        def rest(self):
            for way in range(2):
                arrive(self.base + 2 * way + 1, self.at(1 + way, halves[self.s][1 - way]))

        def far_end(self):
            for way in range(2):
                arrive(self.base + 4 + way, self.at(3, halves[self.s][way]))

    legs = [[Leg(s, p) for p in range(4)] for s in STREAMS]

    def have(s, gi, d):
        lanes = lanes_of[s]
        send(37 * s + 24 + 3 * d + gi, blk(s, d, GROUPS[gi], lanes), blk(s, d, GROUPS[gi], lanes, 1), here.partner)

    def spread(s, gi):
        legs[s][1 + gi].both_ways()
        have(s, gi, 0)

    def second_rest(s, gi):
        legs[s][1 + gi].rest()
        have(s, gi, 1)
        have(s, gi, 2)

    def second_far(s, gi):
        legs[s][1 + gi].far_end()
        have(s, gi, 3)

    mine = buf.at[0, 0, 0, k]
    smalls = [pltpu.make_async_copy(route_hbm, route_v, load_sem.at[4]), pltpu.make_async_copy(gates_hbm, gates_v, load_sem.at[5])]
    loads = [pltpu.make_async_copy(h.at[mb], dst.at[:, pl.ds(lo, dm)], load_sem.at[n])
             for n, (h, mb, dst, lo) in enumerate(((x_hbm, other, stage, 0), (dy_hbm, other, stage, dm), (x_hbm, k, mine, 0), (dy_hbm, k, mine, dm)))]
    for c in smalls + loads:
        c.start()
    for c in smalls:
        c.wait()
    metas = [token_meta(route_v[:, m, :], gates_v[:, m, :]) for m in range(2)]
    zero_core = k == 0
    stage[:, 2 * dm:] = jnp.where(zero_core, metas[1].astype(F32), metas[0].astype(F32)).astype(BF16)
    buf[0, 0, 0, k, :, 2 * dm:] = jnp.where(zero_core, metas[0].astype(F32), metas[1].astype(F32)).astype(BF16)
    here.barrier()
    for c in loads:
        c.wait()
    send(36, stage, buf.at[0, 0, 0, k], here.partner)
    arrive(36, buf.at[0, 0, 0, other])
    for s in STREAMS:
        legs[s][0].both_ways()
    for s in STREAMS:
        spread(s, 0)
    for s in STREAMS:
        legs[s][0].relay()
    for s in STREAMS:
        legs[s][1].relay()
    for s in STREAMS:
        legs[s][0].rest()
        spread(s, 1)
    for s in STREAMS:
        second_rest(s, 0)
    for s in STREAMS:
        legs[s][0].far_end()
        spread(s, 2)
    for s in STREAMS:
        legs[s][2].relay()
    for s in STREAMS:
        second_far(s, 0)
    for s in STREAMS:
        second_rest(s, 1)
    for s in STREAMS:
        legs[s][3].relay()
    for s in STREAMS:
        second_rest(s, 2)
    for s in STREAMS:
        second_far(s, 1)
    for s in STREAMS:
        second_far(s, 2)
    for d in range(RING):
        for gi in range(len(GROUPS)):
            for s in STREAMS:
                arrive(37 * s + 24 + 3 * d + gi, blk(s, d, GROUPS[gi], lanes_of[s], 1))
    for c in sent:
        c.wait_send()


def gather_tokens(x, grad_y, route_idx, gates):
    _, tok_dev, dm = x.shape
    top_k = gates.shape[2]
    width = 2 * dm + LANES
    hbm = pl.BlockSpec(memory_space=pltpu.HBM)
    vmem = pl.BlockSpec(memory_space=pltpu.VMEM)
    sems = pltpu.SemaphoreType.DMA((74,))
    args = (x, grad_y, jnp.transpose(route_idx, (2, 0, 1)), jnp.transpose(gates, (2, 0, 1)))
    return pl.pallas_call(
        gather_kernel,
        out_shape=pltpu.VMEM((2, RING, RING, 2, tok_dev, width), BF16),
        in_specs=[hbm] * 4,
        out_specs=vmem,
        scratch_shapes=[pltpu.VMEM((tok_dev, width), BF16), pltpu.VMEM((top_k, 2, tok_dev), jnp.int32), pltpu.VMEM((top_k, 2, tok_dev), F32),
                        sems, sems, pltpu.SemaphoreType.DMA((6,))],
        compiler_params=pltpu.CompilerParams(collective_id=0, has_side_effects=True, vmem_limit_bytes=COMM_VMEM),
        name="gather_tokens",
    )(*(pltpu.with_memory_space_constraint(v, pltpu.HBM) for v in args))


def reduce_kernel(part_ref, out_ref, own, pair, full, half, pair_send, pair_recv,
                  ring_send, ring_recv, last_sem):
    here = Place()
    k, other = here.core, here.other
    lanes_of, halves = stream_lanes(part_ref.shape[5])
    sent = []

    def slot(s, d, i):
        return (d, i) if s == 0 else (i, d)

    def near_slot(s, d, i):
        return slot(s, NEAR.index(FAR[d]), NEAR.index(FAR[i]))

    def swap(s, d, i):
        lanes = lanes_of[s]
        return pltpu.make_async_remote_copy(src_ref=part_ref.at[(1,) + near_slot(s, d, i)].at[:, :, lanes],
                                            dst_ref=pair.at[slot(s, d, i)].at[:, :, lanes], send_sem=pair_send.at[s, d, i],
                                            recv_sem=pair_recv.at[s, d, i], device_id=here.partner, device_id_type=MESH)

    def move(s, f, kind, src, dst, axis):
        peer = here.peer(axis if s == 0 else 3 - axis, 1 if kind % 2 == 0 else -1)
        return pltpu.make_async_remote_copy(src_ref=src, dst_ref=dst, send_sem=ring_send.at[s, f, kind], recv_sem=ring_recv.at[s, f, kind],
                                            device_id=peer, device_id_type=MESH)

    def go(s, f, kind, src, dst, axis):
        c = move(s, f, kind, src, dst, axis)
        c.start()
        sent.append(c)

    def arrive(s, f, kind, dst):
        move(s, f, kind, dst, dst, 1).wait_recv()

    def own_ref(s, d, g, lanes):
        return own.at[slot(s, d, g)].at[:, :, :, lanes]

    def add_own(s, d, g, lanes, *vals):
        ix = slot(s, d, g) + (slice(None), slice(None), lanes)
        total = own[ix]
        for v in vals:
            total = total + v
        own[ix] = total

    def add_pair(s, d, gi):
        lanes = (slice(None), slice(None), lanes_of[s])
        for i in range(GROUPS[gi].start, GROUPS[gi].stop):
            swap(s, d, i).wait_recv()
            own[slot(s, d, i) + lanes] = part_ref[(0,) + near_slot(s, d, i) + lanes] + pair[slot(s, d, i) + lanes]

    def far(s, f, d, at, g, axis):
        for kind in range(2):
            lanes = halves[s][kind]
            go(s, f, kind, own_ref(s, d, at, lanes), half.at[g, :, :, lanes], axis)

    def near(s, f, spot, g, axis):
        for kind, step in ((0, 1), (1, -1)):
            lanes = halves[s][kind]
            arrive(s, f, kind, half.at[g, :, :, lanes])
            add_own(s, *spot(step), lanes, half[g, :, :, lanes])
        lanes = lanes_of[s]
        for kind, step in ((2, 1), (3, -1)):
            go(s, f, kind, own_ref(s, *spot(step), lanes), full.at[kind - 2, g, :, :, lanes], axis)

    def done(s, f, at, g):
        lanes = lanes_of[s]
        for n in range(2):
            arrive(s, f, 2 + n, full.at[n, g, :, :, lanes])
        add_own(s, 3, at, lanes, full[0, g, :, :, lanes], full[1, g, :, :, lanes])

    def far2(gi):
        for s in STREAMS:
            add_pair(s, 0, gi)
            far(s, gi, 0, GROUPS[gi], GROUPS[gi], 2)

    def near2(gi):
        for s in STREAMS:
            add_pair(s, 2, gi)
            add_pair(s, 1, gi)
        for s in STREAMS:
            near(s, gi, lambda step: (2 if step == 1 else 1, GROUPS[gi]), GROUPS[gi], 2)

    def done2(gi):
        for s in STREAMS:
            add_pair(s, 3, gi)
        for s in STREAMS:
            done(s, gi, GROUPS[gi], GROUPS[gi])

    order = [(0, 0), (0, 1), (0, 2), (2, 0), (1, 0), (0, 3), (2, 1), (2, 2), (1, 1), (1, 2), (3, 0), (2, 3), (1, 3), (3, 1), (3, 2), (3, 3)]
    here.barrier()
    for q in order:
        for s in STREAMS:
            c = swap(s, *q)
            c.start()
            sent.append(c)
    lone = slice(RING, RING + 1)
    far2(0)
    far2(1)
    near2(0)
    far2(2)
    near2(1)
    done2(0)
    for s in STREAMS:
        far(s, 3, 3, slice(0, 1), lone, 1)
    near2(2)
    done2(1)
    for s in STREAMS:
        near(s, 3, lambda step: (3, slice(2, 3) if step == 1 else slice(1, 2)), lone, 1)
    done2(2)

    def give(s, c):
        lanes = lanes_of[s]
        return pltpu.make_async_remote_copy(src_ref=own.at[3, 3, c].at[:, lanes], dst_ref=out_ref.at[k].at[:, lanes],
                                            send_sem=last_sem.at[0, s], recv_sem=last_sem.at[1, s], device_id=here.partner, device_id_type=MESH)

    for s in STREAMS:
        done(s, 3, slice(3, 4), lone)
        copy = give(s, other)
        copy.start()
        sent.append(copy)
    out_ref[k] = own[3, 3, k]
    for s in STREAMS:
        give(s, other).wait_recv()
    for c in sent:
        c.wait_send()


def finish_kernel(dm, top_k, in_ref, y_ref, dx_ref, dg_ref):
    for m in range(2):
        y_ref[m] = in_ref[m, :, :dm].astype(BF16)
        dx_ref[m] = in_ref[m, :, dm:2 * dm].astype(BF16)
        dg_ref[:, m, :] = in_ref[m, :, 2 * dm:].T[:top_k, :]


def finish(mine, dm, top_k):
    _, tok_dev, _ = mine.shape
    vmem = pl.BlockSpec(memory_space=pltpu.VMEM)
    out = jax.ShapeDtypeStruct((2, tok_dev, dm), BF16)
    y, dx, dg = pl.pallas_call(
        functools.partial(finish_kernel, dm, top_k),
        out_shape=(out, out, jax.ShapeDtypeStruct((top_k, 2, tok_dev), F32)),
        in_specs=[vmem],
        out_specs=(vmem, vmem, vmem),
        name="finish",
    )(pltpu.with_memory_space_constraint(mine, pltpu.VMEM))
    return y, dx, jnp.transpose(dg, (1, 2, 0))


def reduce_tokens(part):
    _, _, _, cores, tok_dev, width = part.shape
    vmem = pl.BlockSpec(memory_space=pltpu.VMEM)
    block = (cores, tok_dev, width)
    ring_sems = pltpu.SemaphoreType.DMA((2, 4, 4))
    pair_sems = pltpu.SemaphoreType.DMA((2, RING, RING))
    return pl.pallas_call(
        reduce_kernel,
        out_shape=pltpu.VMEM((2, tok_dev, width), F32),
        in_specs=[vmem],
        out_specs=vmem,
        scratch_shapes=[
            pltpu.VMEM((RING, RING) + block, F32),
            pltpu.VMEM((RING, RING) + block, F32),
            pltpu.VMEM((2, RING + 1) + block, F32),
            pltpu.VMEM((RING + 1,) + block, F32),
            pair_sems, pair_sems, ring_sems, ring_sems,
            pltpu.SemaphoreType.DMA((2, 2)),
        ],
        compiler_params=pltpu.CompilerParams(collective_id=1, has_side_effects=True, vmem_limit_bytes=COMM_VMEM),
        name="reduce_tokens",
    )(pltpu.with_memory_space_constraint(part, pltpu.VMEM))


def solution(mesh):
    group = mesh.shape["row"] * mesh.shape["col"] * mesh.shape["core"]
    tok_spec = P(None, ALL_AXES, None)
    w_spec = P(ALL_AXES, None, None)

    def moe_layer(x, route_idx, gates, w_gate, w_up, w_down, grad_y):
        _, tok_dev, dm = x.shape
        top_k = route_idx.shape[2]
        width = 2 * dm + LANES
        xd = gather_tokens(x, grad_y, route_idx, gates).reshape(2, group * tok_dev, width)
        part, g_gate, g_up, g_down = expert_stage(xd, w_gate, w_up, w_down, top_k, group * (tok_dev // 2))
        y, dx, dg = finish(reduce_tokens(part.reshape(2, RING, RING, 2, tok_dev, width)), dm, top_k)
        return y, dx, dg, g_gate, g_up, g_down

    return jax.shard_map(moe_layer, mesh=mesh, in_specs=(tok_spec, tok_spec, tok_spec, w_spec, w_spec, w_spec, tok_spec), out_specs=(tok_spec, tok_spec, tok_spec, w_spec, w_spec, w_spec), check_vma=False)
```
